32 devices in a mesh: frames: 8 (over z, x), heads: 4 (over y, core).
Axes of the slice: x: 2, y: 2, z: 4, core: 2. Of those that a mesh axis runs over, the one named last changes fastest.
Arguments:
- queries: bfloat16 [8192, 2560], P('frames', 'heads'), may hold values from -6 to 6, as said below
- keys: bfloat16 [8192, 2560], P('frames', 'heads'), may hold values from -6 to 6, as said below
- values: bfloat16 [8192, 2560], P('frames', 'heads'), may hold values from -6 to 6
- block_ids: int32 [64, 4], replicated, may hold values from 0 to 63, as said below
- counts: int32 [64], P('frames'), may hold values from 1 to 4
- w_out: bfloat16 [2560, 5120], P('heads'), may hold values from -0.125 to 0.125
Outputs:
- projected: bfloat16 [8192, 5120], P('frames', 'heads')
The draws below stay inside these ranges and needn't reach their ends.
Inputs may be any that keep to these rules, and one draw needn't show every extreme that they name: `block_ids`: block j is held by index j // 8 of frames. Counted with repeats, the entries of the 8 query blocks of one index of frames name at most 4 blocks held by any one index, and exactly 4 held by some index. Entries of a row may repeat. `queries`: drawn in float32 and rounded once. `keys`: drawn in float32 and rounded once.
All inputs are finite; a program needn't handle non-finite values.
Results may differ from the reference program's by a relative error of at most 0.0052.
Values may be sent and summed in bfloat16 or wider, within the bound.
A program may use at most 192 MiB of HBM per device.

```python
import jax
import jax.numpy as jnp
from jax import lax

D = 5120
HEADS = 20
DH = 128
TILE = 128
SEL = 4
BLK_DEV = 8
NB = 64
TOKENS = 8192
CAP = 4
N_FRAMES = 8


def pair_draw(key, which_one):
    base = jax.random.fold_in(key, 7)
    key_query, key_key = jax.random.split(base, 2)
    full_shape = (TOKENS, HEADS * DH)
    query_part = jnp.clip(1.5 * jax.random.normal(key_query, full_shape, jnp.float32), -6.0, 6.0)
    key_part = jnp.clip(1.5 * jax.random.normal(key_key, full_shape, jnp.float32), -6.0, 6.0)
    if which_one == 0:
        return query_part
    return key_part


def draw_queries(key, part):
    return pair_draw(key, 0).astype(jnp.bfloat16)


def draw_keys(key, part):
    return pair_draw(key, 1).astype(jnp.bfloat16)


def draw_block_ids(key, part):
    requests = BLK_DEV * SEL

    def one_device(device_key):
        key_star, key_order, key_shuffle, key_local = jax.random.split(device_key, 4)
        owners = jnp.tile(jnp.arange(N_FRAMES, dtype=jnp.int32), CAP)
        star = jax.random.randint(key_star, (), 0, N_FRAMES, dtype=jnp.int32)
        order = jax.random.permutation(key_order, N_FRAMES * CAP).astype(jnp.int32)
        priority = order + jnp.where(owners == star, 0, N_FRAMES * CAP).astype(jnp.int32)
        picked = owners[jnp.argsort(priority, stable=True)][:requests]
        shuffled = picked[jax.random.permutation(key_shuffle, requests)]
        local_block = jax.random.randint(key_local, (requests,), 0, BLK_DEV, dtype=jnp.int32)
        return shuffled * BLK_DEV + local_block
    device_keys = jax.vmap(lambda device: jax.random.fold_in(key, 100 + device))(jnp.arange(N_FRAMES))
    return jax.vmap(one_device)(device_keys).reshape(NB, SEL).astype(jnp.int32)


def place_ends(array, key, least, top_value):
    spot = [jax.random.randint(jax.random.fold_in(key, axis), (), 0, length) for axis, length in enumerate(array.shape)]
    main_axis = array.shape.index(max(array.shape))
    beside = spot[:main_axis] + [(spot[main_axis] + 1) % array.shape[main_axis]] + spot[main_axis + 1:]
    return array.at[tuple(spot)].set(least).at[tuple(beside)].set(top_value)


def level_of(own_key, shape, cuts, least, top_value):
    def one(axis_at, shards_of):
        draws = jax.random.uniform(jax.random.fold_in(jax.random.fold_in(own_key, 6), axis_at), (shards_of,), jnp.float32, least / len(cuts), top_value / len(cuts))
        return jnp.repeat(jnp.exp(draws), shape[axis_at] // shards_of).reshape((-1,) + (1,) * (len(shape) - axis_at - 1))

    loudness = one(*cuts[0])
    for cut in cuts[1:]:
        loudness = loudness * one(*cut)
    return loudness


def normal_values(key, extent, scale, reach, cuts=(), kind=jnp.bfloat16):
    loudness = level_of(key, extent, cuts, -0.22, 0.18) if cuts else 1.0
    array = jax.random.normal(key, extent, jnp.float32) * scale * loudness
    return jnp.minimum(jnp.maximum(array, -reach), reach).astype(kind)


def setup_inputs(seed: int = 0) -> dict:
    arg_keys = jax.random.split(jax.random.key(seed), 7)
    queries = draw_queries(jax.random.fold_in(arg_keys[6], 71), 0)
    keys = draw_keys(jax.random.fold_in(arg_keys[6], 71), 0)
    values = normal_values(arg_keys[2], (TOKENS, HEADS * DH), 1.0, 6.0, ((0, 8), (1, 4)))
    block_ids = draw_block_ids(jax.random.fold_in(arg_keys[6], 71), 0)
    counts = place_ends(jax.random.randint(arg_keys[4], (NB,), 1, SEL + 1), jax.random.fold_in(arg_keys[4], 1), 1, SEL).astype(jnp.int32)
    w_out = normal_values(arg_keys[5], (HEADS * DH, D), (HEADS * DH) ** -0.5, 0.125, ((0, 4),))
    return {"queries": queries, "keys": keys, "values": values, "block_ids": block_ids, "counts": counts, "w_out": w_out}


def reference(queries, keys, values, block_ids, counts, w_out):
    full_width = HEADS * DH
    inv_root = 1.0 / (DH ** 0.5)
    query_tiles = queries.reshape(NB, TILE, full_width)
    key_tiles = keys.reshape(NB, TILE, full_width)
    value_tiles = values.reshape(NB, TILE, full_width)

    def one_block(block_index):
        chosen = block_ids[block_index]
        keyset_k = jnp.concatenate([key_tiles[block_index][None], key_tiles[chosen]], 0)
        keyset_v = jnp.concatenate([value_tiles[block_index][None], value_tiles[chosen]], 0)
        keyset_k = keyset_k.reshape((SEL + 1) * TILE, HEADS, DH).astype(jnp.float32)
        keyset_v = keyset_v.reshape((SEL + 1) * TILE, HEADS, DH).astype(jnp.float32)
        query_tile = query_tiles[block_index].reshape(TILE, HEADS, DH).astype(jnp.float32)
        scores = jnp.einsum("qhd,khd->hqk", query_tile, keyset_k) * inv_root
        allowed = jnp.concatenate([jnp.ones((1,), bool), jnp.arange(SEL) < counts[block_index]])
        key_allowed = jnp.repeat(allowed, TILE)
        scores = jnp.where(key_allowed[None, None, :], scores, -jnp.inf)
        row_max = jnp.max(scores, axis=-1, keepdims=True)
        probs = jnp.exp(scores - row_max)
        denom_sum = jnp.sum(probs, axis=-1)
        weights = lax.optimization_barrier(probs.astype(jnp.bfloat16)).astype(jnp.float32)
        mixed = jnp.einsum("hqk,khd->qhd", weights, keyset_v)
        mixed = mixed / jnp.transpose(denom_sum)[:, :, None]
        return mixed.astype(jnp.bfloat16).reshape(TILE, full_width)

    attn = lax.map(one_block, jnp.arange(NB)).reshape(TOKENS, full_width)
    return jnp.dot(attn, w_out, preferred_element_type=jnp.float32).astype(jnp.bfloat16)
```

```python
import functools
import math

import jax
import jax.numpy as jnp
from jax import lax
from jax.experimental import pallas as pl
from jax.experimental.pallas import tpu as pltpu
from jax.sharding import PartitionSpec as P

DH = 128
TILE = 128
MESH = pl.DeviceIdType.MESH
F32 = jnp.float32
PAIR = 2
LINE = 4
PARTS = 2
UNROLL = 2
EARLY = 3
SUBLANES = 8
LOG2E = math.log2(math.e)
LOWEST = -1e38
SMALLEST = 1e-37
VMEM_BYTES = 67043328
NT_DIMS = (((1,), (1,)), ((), ()))


def head_columns(h):
    return slice(h * DH, (h + 1) * DH)


class direct_exchange:
    def __init__(self, dims, pick_ref, k_ref, v_ref, recv, send, kv_send, kv_recv):
        self.frames, _, _, _, self.capacity, self.heads, self.slots = dims
        self.pick_ref, self.k_ref, self.v_ref, self.recv = pick_ref, k_ref, v_ref, recv
        self.send, self.kv_send, self.kv_recv = send, kv_send, kv_recv
        self.me_f, self.me_p = lax.axis_index("frames"), lax.axis_index("heads")

    def copy(self, h, target, origin):
        return pltpu.make_async_remote_copy(
            src_ref=self.send.at[h % self.slots, target],
            dst_ref=self.recv[h].at[pl.ds(origin * self.capacity, self.capacity)],
            send_sem=self.kv_send.at[h, target],
            recv_sem=self.kv_recv.at[h, origin],
            device_id=(target, self.me_p),
            device_id_type=MESH,
        )

    def others(self, action):
        @pl.loop(1, self.frames)
        def _(step):
            action(lax.rem(self.me_f + step, self.frames))

    def pick(self, target, c):
        return self.pick_ref[(target * self.frames + self.me_f) * self.capacity + c]

    def build(self, h):
        if h >= self.slots:
            self.others(lambda target: self.copy(h - self.slots, target, self.me_f).wait_send())

        def fill(target):
            for c in range(self.capacity):
                index = self.pick(target, c)
                self.send[h % self.slots, target, c, 0] = self.k_ref[index, :, head_columns(h)]
                self.send[h % self.slots, target, c, 1] = self.v_ref[index, :, head_columns(h)]

        self.others(fill)
        for c in range(self.capacity):
            index = self.pick(self.me_f, c)
            self.recv[h][self.me_f * self.capacity + c, 0] = self.k_ref[index, :, head_columns(h)]
            self.recv[h][self.me_f * self.capacity + c, 1] = self.v_ref[index, :, head_columns(h)]

    def start(self, h):
        self.others(lambda target: self.copy(h, target, self.me_f).start())

    def prepare(self):
        self.build(0)

    def begin(self):
        self.start(0)

    def follow(self):
        if self.heads > 1:
            self.build(1)
            self.start(1)

    def receive(self, h, midway):
        if h + 2 < self.heads:
            self.build(h + 2)
        midway()
        self.others(lambda origin: self.copy(h, origin, origin).wait_recv())
        if h + 2 < self.heads:
            self.start(h + 2)

    def drain(self):
        for h in range(max(0, self.heads - self.slots), self.heads):
            self.others(lambda target: self.copy(h, target, self.me_f).wait_send())


def layer_kernel(
    dims, pick_ref, slot_ref, count_ref, q_ref, k_ref, v_ref, w_ref, out_ref,
    rows, attn, acc, w_send, w_recv, a_send, a_recv, own_sem, *kv_refs,
):
    frames, peers, blocks, select, capacity, heads, slots = dims
    recv, kv_refs = kv_refs[:heads], kv_refs[heads:]
    me_f, me_p = lax.axis_index("frames"), lax.axis_index("heads")
    depth = heads * DH
    features = rows.shape[2]

    barrier = pltpu.get_barrier_semaphore()

    @pl.loop(1, frames)
    def _(step):
        pl.semaphore_signal(
            barrier, inc=1, device_id=(lax.rem(me_f + step, frames), me_p), device_id_type=MESH
        )

    @pl.loop(1, peers)
    def _(step):
        pl.semaphore_signal(
            barrier, inc=1, device_id=(me_f, lax.rem(me_p + step, peers)), device_id_type=MESH
        )

    def columns_of(peer):
        return pl.ds(pl.multiple_of(peer * features, features), features)

    own_rows = pltpu.make_async_copy(w_ref.at[:, columns_of(me_p)], rows.at[me_p], own_sem)
    own_rows.start()

    exchange = direct_exchange(dims, pick_ref, k_ref, v_ref, recv, *kv_refs)

    def w_copy(target, origin):
        return pltpu.make_async_remote_copy(
            src_ref=w_ref.at[:, columns_of(target)],
            dst_ref=rows.at[origin],
            send_sem=w_send.at[target],
            recv_sem=w_recv.at[origin],
            device_id=(me_f, target),
            device_id_type=MESH,
        )

    part_blocks = blocks // PARTS
    part_rows = part_blocks * TILE

    def a_copy(h, part, target, origin):
        held = attn.at[h, origin, pl.ds(part * part_rows, part_rows)]
        return pltpu.make_async_remote_copy(
            src_ref=held,
            dst_ref=held,
            send_sem=a_send.at[h, part, target, origin],
            recv_sem=a_recv.at[h, part, origin],
            device_id=(me_f, target),
            device_id_type=MESH,
        )

    twin = me_p + 1 - 2 * lax.rem(me_p, 2)

    def over_alike(action):
        @pl.loop(1, peers // 2)
        def _(step):
            action(lax.rem(me_p + 2 * step, peers))

    def over_twins(action):
        @pl.loop(0, peers // 2)
        def _(step):
            action(lax.rem(twin + 2 * step, peers))

    def share(h, part):
        over_alike(lambda target: a_copy(h, part, target, me_p).start())
        a_copy(h, part, twin, me_p).start()

    def finish(h):
        if h == 0:
            own_rows.wait()
            over_peers(lambda origin: w_copy(origin, origin).wait_recv())
        for part in range(PARTS):

            def relay(origin):
                a_copy(h, part, origin, origin).wait_recv()
                a_copy(h, part, twin, origin).start()

            over_alike(relay)
        for part in range(PARTS):
            over_twins(lambda origin: a_copy(h, part, origin, origin).wait_recv())
            project(h, part)

    def drain_attn(h, part):
        over_alike(lambda target: a_copy(h, part, target, me_p).wait_send())
        a_copy(h, part, twin, me_p).wait_send()
        over_alike(lambda origin: a_copy(h, part, twin, origin).wait_send())

    def over_peers(action):
        @pl.loop(1, peers)
        def _(step):
            action(lax.rem(me_p + step, peers))

    def attend(h, part):
        @pl.loop(part * part_blocks, (part + 1) * part_blocks, unroll=UNROLL)
        def _(b):
            q = q_ref[b, :, head_columns(h)]
            picks = [slot_ref[b * select + s] for s in range(select)]
            keyset = jnp.concatenate(
                [k_ref[b, :, head_columns(h)]] + [recv[h][i, 0] for i in picks], axis=0
            )
            valueset = jnp.concatenate(
                [v_ref[b, :, head_columns(h)]] + [recv[h][i, 1] for i in picks], axis=0
            )
            scores = lax.dot_general(q, keyset, NT_DIMS, preferred_element_type=F32)
            scores = scores * (1.0 / DH**0.5)
            position = lax.broadcasted_iota(jnp.int32, scores.shape, 1)
            scores = jnp.where(position < (count_ref[b] + 1) * TILE, scores, -jnp.inf)
            top = jnp.max(scores, axis=1, keepdims=True)
            probs = jnp.exp(scores - top)
            denom = jnp.sum(probs, axis=1, keepdims=True)
            mixed = jnp.dot(probs.astype(jnp.bfloat16), valueset, preferred_element_type=F32)
            attn[h, me_p, pl.ds(pl.multiple_of(b * TILE, TILE), TILE), :] = (mixed / denom).astype(
                jnp.bfloat16
            )

    row_tile = 2 * TILE

    def project(h, part):
        @pl.loop(part * part_rows // row_tile, (part + 1) * part_rows // row_tile)
        def _(r):
            span = pl.ds(pl.multiple_of(r * row_tile, row_tile), row_tile)
            left = jnp.concatenate([attn[h, p, span, :] for p in range(peers)], axis=1)
            right = jnp.concatenate([rows[p, head_columns(h), :] for p in range(peers)], axis=0)
            term = jnp.dot(left, right, preferred_element_type=F32)
            if h > 0:
                term = term + acc[span, :]
            if h == heads - 1:
                out_ref[span, :] = term.astype(out_ref.dtype)
            else:
                acc[span, :] = term

    exchange.prepare()
    pl.semaphore_wait(barrier, frames + peers - 2)
    exchange.begin()
    over_peers(lambda target: w_copy(target, me_p).start())
    exchange.follow()
    for h in range(heads):
        exchange.receive(h, (lambda: finish(h - 1)) if h > 0 else (lambda: None))
        for part in range(PARTS):
            attend(h, part)
            share(h, part)
    finish(heads - 1)
    exchange.drain()
    over_peers(lambda target: w_copy(target, me_p).wait_send())
    for h in range(heads):
        for part in range(PARTS):
            drain_attn(h, part)


def shards(queries, keys, values, block_ids, counts, w_out):
    frames = lax.axis_size("frames")
    peers = lax.axis_size("heads")
    here = lax.axis_index("frames")
    tokens, width = queries.shape
    blocks = tokens // TILE
    select = block_ids.shape[1]
    heads = width // DH
    requests = blocks * select
    capacity = max(2, (requests + frames - 1) // frames)
    features = w_out.shape[1] // peers
    slots = min(3, heads)

    ids = block_ids.reshape(frames, requests)
    owner = ids // blocks
    order = jnp.arange(requests, dtype=jnp.int32)
    same = (owner[:, :, None] == owner[:, None, :]) & (order[:, None] < order[None, :])
    slot = owner * capacity + jnp.sum(same.astype(jnp.int32), axis=1)
    hit = slot[:, None, :] == jnp.arange(frames * capacity, dtype=jnp.int32)[:, None]
    pick = jnp.sum(jnp.where(hit, (ids % blocks)[:, None, :], 0), axis=2).reshape(-1)
    my_slot = lax.dynamic_slice_in_dim(slot, here, 1, 0).reshape(requests)

    smem = pl.BlockSpec(memory_space=pltpu.SMEM)
    vmem = pl.BlockSpec(memory_space=pltpu.VMEM)
    tiles = (blocks, TILE, width)
    dma = pltpu.SemaphoreType.DMA
    bf16 = jnp.bfloat16
    common = [
        pltpu.VMEM((peers, width, features), bf16),
        pltpu.VMEM((heads, peers, tokens, DH), bf16),
        pltpu.VMEM((tokens, features), F32),
    ]
    common_sems = [
        dma((peers,)), dma((peers,)), dma((heads, PARTS, peers, peers)),
        dma((heads, PARTS, peers)), dma,
    ]
    recv = [pltpu.VMEM((frames * capacity, 2, TILE, DH), bf16)] * heads
    extra = [
        pltpu.VMEM((slots, frames, capacity, 2, TILE, DH), bf16),
        dma((heads, frames)),
        dma((heads, frames)),
    ]
    dims = (frames, peers, blocks, select, capacity, heads, slots)
    return pl.pallas_call(
        functools.partial(layer_kernel, dims),
        out_shape=jax.ShapeDtypeStruct((tokens, features), bf16),
        in_specs=[smem, smem, smem, vmem, vmem, vmem, pl.BlockSpec(memory_space=pl.ANY)],
        out_specs=vmem,
        scratch_shapes=common + common_sems + recv + extra,
        compiler_params=pltpu.CompilerParams(
            collective_id=0, has_side_effects=True, vmem_limit_bytes=VMEM_BYTES
        ),
    )(
        pick, my_slot, counts, queries.reshape(tiles), keys.reshape(tiles), values.reshape(tiles),
        w_out,
    )


def column_kernel(
    dims, ids_ref, own_count_ref, q_ref, k_ref, v_ref, w_ref, out_ref,
    rows, attn, acc, qall, count, osend, orecv, ssend, srecv, oself, sself, place, usable,
    w_send, w_recv, a_send, a_recv, own_sem, kv_send, kv_recv, q_send, q_recv,
    c_send, c_recv, o_send, o_recv, s_send, s_recv, *kv,
):
    frames, peers, blocks, select, heads = dims
    me_f, me_p = lax.axis_index("frames"), lax.axis_index("heads")
    line = frames // PAIR
    z, x = me_f // PAIR, me_f % PAIR
    half = z // (line // 2)
    mid, end = half + 1, (line - 1) * half
    across = line - 1 - mid
    is_mid = z == mid
    is_end = z == end
    other = 1 - x
    depth = heads * DH
    features = rows.shape[2]
    part_blocks = blocks // PARTS
    part_rows = part_blocks * TILE
    exponent = LOG2E / DH**0.5

    def at(zz, xx):
        return (zz * PAIR + xx, me_p)

    barrier = pltpu.get_barrier_semaphore()

    @pl.loop(1, frames)
    def _(step):
        pl.semaphore_signal(
            barrier, inc=1, device_id=(lax.rem(me_f + step, frames), me_p), device_id_type=MESH
        )

    @pl.loop(1, peers)
    def _(step):
        pl.semaphore_signal(
            barrier, inc=1, device_id=(me_f, lax.rem(me_p + step, peers)), device_id_type=MESH
        )

    def columns_of(peer):
        return pl.ds(pl.multiple_of(peer * features, features), features)

    own_rows = pltpu.make_async_copy(w_ref.at[:, columns_of(me_p)], rows.at[me_p], own_sem)
    own_rows.start()

    def send(source, target, send_sem, recv_sem, device):
        return pltpu.make_async_remote_copy(
            src_ref=source, dst_ref=target, send_sem=send_sem, recv_sem=recv_sem,
            device_id=device, device_id_type=MESH,
        )

    def kv_copy(h, flow, which):
        source = (k_ref, v_ref)[which].at[:, :, head_columns(h)]
        if flow == 2:
            source = kv[h].at[which, pl.ds(blocks, blocks)]
        return send(
            source, kv[h].at[which, pl.ds((flow + 1) * blocks, blocks)],
            kv_send.at[flow, h, which], kv_recv.at[flow, h, which],
            at(mid, x) if flow == 0 else at(across, x),
        )

    def q_copy(h, flow):
        source = q_ref.at[:, :, head_columns(h)] if flow < 2 else qall.at[h, 1]
        return send(
            source, qall.at[h, flow], q_send.at[flow, h], q_recv.at[flow, h],
            at(mid, x) if flow == 1 else at(z, other),
        )

    def c_copy(flow):
        device = (at(z, other), at(mid, x), at(mid, other))[flow]
        return send(
            own_count_ref, count.at[flow + 1], c_send.at[flow], c_recv.at[flow], device
        )

    def o_copies(h, part, slot):
        span = pl.ds(part * part_rows, part_rows)
        to_z = z + (end - z) * ((slot + 1) // 2)
        to_x = x + (other - x) * ((slot + 1) % 2)
        device = at(to_z, to_x)
        return (
            send(
                osend.at[h, slot, span], orecv.at[h, slot, span],
                o_send.at[h, part, slot], o_recv.at[h, part, slot], device,
            ),
            send(
                ssend.at[h, slot, part], srecv.at[h, slot, part],
                s_send.at[h, part, slot], s_recv.at[h, part, slot], device,
            ),
        )

    def w_copy(h, target, origin):
        span = pl.ds(h * DH, DH)
        return send(
            w_ref.at[span, columns_of(target)], rows.at[origin, span],
            w_send.at[h, target], w_recv.at[h, origin], (me_f, target),
        )

    def a_copy(h, part, target, origin):
        held = attn.at[h, origin, pl.ds(part * part_rows, part_rows)]
        return send(
            held, held, a_send.at[h, part, target, origin], a_recv.at[h, part, origin],
            (me_f, target),
        )

    twin = me_p + 1 - 2 * lax.rem(me_p, 2)

    def over_peers(action):
        @pl.loop(1, peers)
        def _(step):
            action(lax.rem(me_p + step, peers))

    def over_alike(action):
        @pl.loop(1, peers // 2)
        def _(step):
            action(lax.rem(me_p + 2 * step, peers))

    def over_twins(action):
        @pl.loop(0, peers // 2)
        def _(step):
            action(lax.rem(twin + 2 * step, peers))

    def share(h, part):
        over_alike(lambda target: a_copy(h, part, target, me_p).start())
        a_copy(h, part, twin, me_p).start()

    def finish(h):
        if h == 0:
            own_rows.wait()
        over_peers(lambda origin: w_copy(h, origin, origin).wait_recv())
        for part in range(PARTS):

            def relay(origin):
                a_copy(h, part, origin, origin).wait_recv()
                a_copy(h, part, twin, origin).start()

            over_alike(relay)
        for part in range(PARTS):
            over_twins(lambda origin: a_copy(h, part, origin, origin).wait_recv())
            project(h, part)

    def drain_attn(h, part):
        over_alike(lambda target: a_copy(h, part, target, me_p).wait_send())
        a_copy(h, part, twin, me_p).wait_send()
        over_alike(lambda origin: a_copy(h, part, twin, origin).wait_send())

    row_tile = 2 * TILE

    def project(h, part):
        @pl.loop(part * part_rows // row_tile, (part + 1) * part_rows // row_tile)
        def _(r):
            span = pl.ds(pl.multiple_of(r * row_tile, row_tile), row_tile)
            left = jnp.concatenate([attn[h, p, span, :] for p in range(peers)], axis=1)
            right = jnp.concatenate([rows[p, head_columns(h), :] for p in range(peers)], axis=0)
            term = jnp.dot(left, right, preferred_element_type=F32)
            if h > 0:
                term = term + acc[span, :]
            if h == heads - 1:
                out_ref[span, :] = term.astype(out_ref.dtype)
            else:
                acc[span, :] = term

    def fill_tables():
        for role in range(4):
            role_z = z if role < 2 else end
            role_x = x if role % 2 == 0 else other

            @pl.loop(0, blocks)
            def _(b):
                for s in range(select):
                    chosen = ids_ref[s, (role_z * PAIR + role_x) * blocks + b]
                    owner = lax.div(chosen, blocks)
                    owner_z, owner_x = lax.div(owner, PAIR), lax.rem(owner, PAIR)
                    here = owner_z == z
                    near = owner_z == end
                    source = jnp.where(
                        here, 0, jnp.where(near, 1, jnp.where(owner_z == across, 2, 3))
                    )
                    ours = here | is_mid
                    if role > 1:
                        ours = ours & jnp.logical_not(near)
                    ours = ours & (owner_x == x)
                    entry = (role * blocks + b) * select + s
                    index = source * blocks + lax.rem(chosen, blocks)
                    place[entry] = jnp.where(ours, index, 0)
                    usable[entry] = jnp.where(ours, 1, 0)

    def own_block(h):
        @pl.loop(0, blocks)
        def _(b):
            kv[h][0, b] = k_ref[b, :, head_columns(h)]
            kv[h][1, b] = v_ref[b, :, head_columns(h)]

    lane = lax.broadcasted_iota(jnp.int32, (TILE, TILE), 1)

    def partial(h, role, b, query, first_keys, first_values):
        entries = [(role * blocks + b) * select + s for s in range(select)]
        picks = [place[e] for e in entries]
        keyset = jnp.concatenate(first_keys + [kv[h][0, i] for i in picks], axis=0)
        valueset = jnp.concatenate(first_values + [kv[h][1, i] for i in picks], axis=0)
        scores = lax.dot_general(query, keyset, NT_DIMS, preferred_element_type=F32)
        used = count[role, pl.ds(b, 1), :]
        pieces = [scores[:, i * TILE : (i + 1) * TILE] for i in range(len(first_keys) + select)]
        for s in range(select):
            keep = jnp.broadcast_to(used * usable[entries[s]], (TILE, TILE)) > s
            at_piece = len(first_keys) + s
            pieces[at_piece] = jnp.where(keep, pieces[at_piece], -jnp.inf)
        top = jnp.max(functools.reduce(jnp.maximum, pieces), axis=1, keepdims=True)
        top = jnp.maximum(top, LOWEST)
        probs = [jnp.exp2((piece - top) * exponent) for piece in pieces]
        denom = jnp.sum(functools.reduce(jnp.add, probs), axis=1, keepdims=True)
        weights = jnp.concatenate([p.astype(jnp.bfloat16) for p in probs], axis=1)
        mixed = jnp.dot(weights, valueset, preferred_element_type=F32)
        level = top * exponent + jnp.log(denom) * LOG2E
        return mixed / jnp.maximum(denom, SMALLEST), level

    def rows_of(levels):
        tile = jnp.zeros((TILE, TILE), F32)
        for j, level in enumerate(levels):
            tile = jnp.where(lane == j, level, tile)
        return tile.T[:SUBLANES]

    others = 1 + 2 * is_mid.astype(jnp.int32)

    def attend_others(h):
        @pl.loop(0, PARTS * others)
        def _(step):
            part, turn = step // others, step % others
            role = others - turn
            levels = []
            for j in range(part_blocks):
                b = part * part_blocks + j
                mixed, level = partial(h, role, b, qall[h, role - 1, b], [], [])
                span = pl.ds(pl.multiple_of(b * TILE, TILE), TILE)
                osend[h, role - 1, span, :] = mixed.astype(jnp.bfloat16)
                levels.append(level)
            ssend[h, role - 1, part] = rows_of(levels)
            for copy in o_copies(h, part, role - 1):
                copy.start()
            if h + 1 < heads:

                @pl.when(is_mid & (step == others - 1))
                def _():
                    relay_on(h + 1)

    def attend_own(h):
        @pl.loop(0, PARTS)
        def _(part):
            levels = []
            for j in range(part_blocks):
                b = part * part_blocks + j
                mixed, level = partial(
                    h, 0, b, q_ref[b, :, head_columns(h)],
                    [k_ref[b, :, head_columns(h)]], [v_ref[b, :, head_columns(h)]],
                )
                oself[pl.ds(pl.multiple_of(b * TILE, TILE), TILE), :] = mixed
                levels.append(level)
            sself[part] = rows_of(levels)

    def merge(h, part, slots):
        levels = [sself[part]] + [srecv[h, slot, part] for slot in range(slots)]
        top = functools.reduce(jnp.maximum, levels)
        shares = [jnp.exp2(level - top) for level in levels]
        total = functools.reduce(jnp.add, shares)
        spare = TILE - SUBLANES * len(shares)
        tall = jnp.concatenate(
            [share / total for share in shares] + [jnp.zeros((spare, TILE), F32)], axis=0
        ).T
        for j in range(part_blocks):
            span = pl.ds((part * part_blocks + j) * TILE, TILE)
            value = oself[span, :] * tall[:, j : j + 1]
            for slot in range(slots):
                column = SUBLANES * (slot + 1) + j
                value = value + orecv[h, slot, span, :].astype(F32) * tall[:, column : column + 1]
            attn[h, me_p, span, :] = value.astype(jnp.bfloat16)

    def combine(h, part):
        for copy in o_copies(h, part, 0):
            copy.wait_recv()

        @pl.when(is_mid)
        def _():
            merge(h, part, 1)

        @pl.when(is_end)
        def _():
            for slot in (1, 2):
                for copy in o_copies(h, part, slot):
                    copy.wait_recv()
            merge(h, part, 3)

    def relay_on(h):
        for which in range(2):
            kv_copy(h, 0, which).wait_recv()
            kv_copy(h, 2, which).start()
        if h + 1 < heads:
            for which in range(2):
                kv_copy(h + 1, 1, which).start()
        q_copy(h, 1).wait_recv()
        q_copy(h, 2).start()

    def send_early(h):
        q_copy(h, 0).start()

        @pl.when(is_end)
        def _():
            for which in range(2):
                kv_copy(h, 0, which).start()
            q_copy(h, 1).start()

    def send_rows(h):
        over_peers(lambda target: w_copy(h, target, me_p).start())

    pl.semaphore_wait(barrier, frames + peers - 2)
    c_copy(0).start()

    @pl.when(is_end)
    def _():
        c_copy(1).start()
        c_copy(2).start()

    @pl.when(is_mid)
    def _():
        for which in range(2):
            kv_copy(0, 1, which).start()

    for h in range(min(EARLY, heads)):
        send_early(h)
        send_rows(h)
    count[0] = own_count_ref[...]
    fill_tables()
    own_block(0)
    c_copy(0).wait_recv()

    @pl.when(is_mid)
    def _():
        relay_on(0)
        c_copy(1).wait_recv()
        c_copy(2).wait_recv()

    for h in range(heads):
        if h + EARLY < heads:
            send_early(h + EARLY)
        if h > 0:
            own_block(h)
        q_copy(h, 0).wait_recv()

        @pl.when(is_mid)
        def _():
            for which in range(2):
                kv_copy(h, 1, which).wait_recv()
                kv_copy(h, 2, which).wait_recv()
            q_copy(h, 2).wait_recv()

        attend_others(h)
        attend_own(h)
        if h > 0:
            finish(h - 1)
        for part in range(PARTS):
            combine(h, part)
            share(h, part)
        if h + EARLY < heads:
            send_rows(h + EARLY)
    finish(heads - 1)

    c_copy(0).wait_send()

    @pl.when(is_end)
    def _():
        c_copy(1).wait_send()
        c_copy(2).wait_send()

    for h in range(heads):
        over_peers(lambda target: w_copy(h, target, me_p).wait_send())
        q_copy(h, 0).wait_send()

        @pl.when(is_end)
        def _():
            for which in range(2):
                kv_copy(h, 0, which).wait_send()
            q_copy(h, 1).wait_send()

        @pl.when(is_mid)
        def _():
            for which in range(2):
                kv_copy(h, 1, which).wait_send()
                kv_copy(h, 2, which).wait_send()
            q_copy(h, 2).wait_send()

        for part in range(PARTS):
            drain_attn(h, part)

            @pl.loop(0, others)
            def _(slot):
                for copy in o_copies(h, part, slot):
                    copy.wait_send()


def column_shards(queries, keys, values, block_ids, counts, w_out):
    frames = lax.axis_size("frames")
    peers = lax.axis_size("heads")
    tokens, width = queries.shape
    blocks = tokens // TILE
    select = block_ids.shape[1]
    heads = width // DH
    features = w_out.shape[1] // peers
    smem = pl.BlockSpec(memory_space=pltpu.SMEM)
    vmem = pl.BlockSpec(memory_space=pltpu.VMEM)
    tiles = (blocks, TILE, width)
    dma = pltpu.SemaphoreType.DMA
    bf16 = jnp.bfloat16
    level_rows = (PARTS, SUBLANES, TILE)
    scratch = [
        pltpu.VMEM((peers, width, features), bf16),
        pltpu.VMEM((heads, peers, tokens, DH), bf16),
        pltpu.VMEM((tokens, features), F32),
        pltpu.VMEM((heads, 3, blocks, TILE, DH), bf16),
        pltpu.VMEM((4, blocks, TILE), jnp.int32),
        pltpu.VMEM((heads, 3, tokens, DH), bf16),
        pltpu.VMEM((heads, 3, tokens, DH), bf16),
        pltpu.VMEM((heads, 3) + level_rows, F32),
        pltpu.VMEM((heads, 3) + level_rows, F32),
        pltpu.VMEM((tokens, DH), F32),
        pltpu.VMEM(level_rows, F32),
        pltpu.SMEM((4 * blocks * select,), jnp.int32),
        pltpu.SMEM((4 * blocks * select,), jnp.int32),
        dma((heads, peers)), dma((heads, peers)), dma((heads, PARTS, peers, peers)),
        dma((heads, PARTS, peers)), dma,
        dma((3, heads, 2)), dma((3, heads, 2)), dma((3, heads)), dma((3, heads)),
        dma((3,)), dma((3,)),
        dma((heads, PARTS, 3)), dma((heads, PARTS, 3)),
        dma((heads, PARTS, 3)), dma((heads, PARTS, 3)),
    ] + [pltpu.VMEM((2, 4 * blocks, TILE, DH), bf16)] * heads
    dims = (frames, peers, blocks, select, heads)
    return pl.pallas_call(
        functools.partial(column_kernel, dims),
        out_shape=jax.ShapeDtypeStruct((tokens, features), bf16),
        in_specs=[smem, vmem, vmem, vmem, vmem, pl.BlockSpec(memory_space=pl.ANY)],
        out_specs=vmem,
        scratch_shapes=scratch,
        compiler_params=pltpu.CompilerParams(
            collective_id=0, has_side_effects=True, vmem_limit_bytes=VMEM_BYTES
        ),
    )(
        block_ids.T, jnp.broadcast_to(counts[:, None], (blocks, TILE)),
        queries.reshape(tiles), keys.reshape(tiles), values.reshape(tiles), w_out,
    )


def solution(mesh):
    placed = (
        P("frames", "heads"),
        P("frames", "heads"),
        P("frames", "heads"),
        P(),
        P("frames"),
        P("heads", None),
    )
    columns = mesh.shape["frames"] == PAIR * LINE and mesh.shape["heads"] % 2 == 0
    return jax.shard_map(
        column_shards if columns else shards, mesh=mesh, in_specs=placed, out_specs=P("frames", "heads"), check_vma=False
    )
```

```python
import functools
import math

import jax
import jax.numpy as jnp
from jax import lax
from jax.experimental import pallas as pl
from jax.experimental.pallas import tpu as pltpu
from jax.sharding import PartitionSpec as P

DH = 128
TILE = 128
MESH = pl.DeviceIdType.MESH
F32 = jnp.float32
PAIR = 2
LINE = 4
PARTS = 2
UNROLL = 2
EARLY = 3
LOG2E = math.log2(math.e)
LOWEST = -1e38
VMEM_BYTES = 67043328
NT_DIMS = (((1,), (1,)), ((), ()))


def head_columns(h):
    return slice(h * DH, (h + 1) * DH)


class direct_exchange:
    def __init__(self, dims, pick_ref, k_ref, v_ref, recv, send, kv_send, kv_recv):
        self.frames, _, _, _, self.capacity, self.heads, self.slots = dims
        self.pick_ref, self.k_ref, self.v_ref, self.recv = pick_ref, k_ref, v_ref, recv
        self.send, self.kv_send, self.kv_recv = send, kv_send, kv_recv
        self.me_f, self.me_p = lax.axis_index("frames"), lax.axis_index("heads")

    def copy(self, h, target, origin):
        return pltpu.make_async_remote_copy(
            src_ref=self.send.at[h % self.slots, target],
            dst_ref=self.recv[h].at[pl.ds(origin * self.capacity, self.capacity)],
            send_sem=self.kv_send.at[h, target],
            recv_sem=self.kv_recv.at[h, origin],
            device_id=(target, self.me_p),
            device_id_type=MESH,
        )

    def others(self, action):
        @pl.loop(1, self.frames)
        def _(step):
            action(lax.rem(self.me_f + step, self.frames))

    def pick(self, target, c):
        return self.pick_ref[(target * self.frames + self.me_f) * self.capacity + c]

    def build(self, h):
        if h >= self.slots:
            self.others(lambda target: self.copy(h - self.slots, target, self.me_f).wait_send())

        def fill(target):
            for c in range(self.capacity):
                index = self.pick(target, c)
                self.send[h % self.slots, target, c, 0] = self.k_ref[index, :, head_columns(h)]
                self.send[h % self.slots, target, c, 1] = self.v_ref[index, :, head_columns(h)]

        self.others(fill)
        for c in range(self.capacity):
            index = self.pick(self.me_f, c)
            self.recv[h][self.me_f * self.capacity + c, 0] = self.k_ref[index, :, head_columns(h)]
            self.recv[h][self.me_f * self.capacity + c, 1] = self.v_ref[index, :, head_columns(h)]

    def start(self, h):
        self.others(lambda target: self.copy(h, target, self.me_f).start())

    def prepare(self):
        self.build(0)

    def begin(self):
        self.start(0)

    def follow(self):
        if self.heads > 1:
            self.build(1)
            self.start(1)

    def receive(self, h, midway):
        if h + 2 < self.heads:
            self.build(h + 2)
        midway()
        self.others(lambda origin: self.copy(h, origin, origin).wait_recv())
        if h + 2 < self.heads:
            self.start(h + 2)

    def drain(self):
        for h in range(max(0, self.heads - self.slots), self.heads):
            self.others(lambda target: self.copy(h, target, self.me_f).wait_send())


def layer_kernel(
    dims, pick_ref, slot_ref, count_ref, q_ref, k_ref, v_ref, w_ref, out_ref,
    rows, attn, acc, w_send, w_recv, a_send, a_recv, own_sem, *kv_refs,
):
    frames, peers, blocks, select, capacity, heads, slots = dims
    recv, kv_refs = kv_refs[:heads], kv_refs[heads:]
    me_f, me_p = lax.axis_index("frames"), lax.axis_index("heads")
    depth = heads * DH
    features = rows.shape[2]

    barrier = pltpu.get_barrier_semaphore()

    @pl.loop(1, frames)
    def _(step):
        pl.semaphore_signal(
            barrier, inc=1, device_id=(lax.rem(me_f + step, frames), me_p), device_id_type=MESH
        )

    @pl.loop(1, peers)
    def _(step):
        pl.semaphore_signal(
            barrier, inc=1, device_id=(me_f, lax.rem(me_p + step, peers)), device_id_type=MESH
        )

    def columns_of(peer):
        return pl.ds(pl.multiple_of(peer * features, features), features)

    own_rows = pltpu.make_async_copy(w_ref.at[:, columns_of(me_p)], rows.at[me_p], own_sem)
    own_rows.start()

    exchange = direct_exchange(dims, pick_ref, k_ref, v_ref, recv, *kv_refs)

    def w_copy(target, origin):
        return pltpu.make_async_remote_copy(
            src_ref=w_ref.at[:, columns_of(target)],
            dst_ref=rows.at[origin],
            send_sem=w_send.at[target],
            recv_sem=w_recv.at[origin],
            device_id=(me_f, target),
            device_id_type=MESH,
        )

    part_blocks = blocks // PARTS
    part_rows = part_blocks * TILE

    def a_copy(h, part, target, origin):
        held = attn.at[h, origin, pl.ds(part * part_rows, part_rows)]
        return pltpu.make_async_remote_copy(
            src_ref=held,
            dst_ref=held,
            send_sem=a_send.at[h, part, target, origin],
            recv_sem=a_recv.at[h, part, origin],
            device_id=(me_f, target),
            device_id_type=MESH,
        )

    twin = me_p + 1 - 2 * lax.rem(me_p, 2)

    def over_alike(action):
        @pl.loop(1, peers // 2)
        def _(step):
            action(lax.rem(me_p + 2 * step, peers))

    def over_twins(action):
        @pl.loop(0, peers // 2)
        def _(step):
            action(lax.rem(twin + 2 * step, peers))

    def share(h, part):
        over_alike(lambda target: a_copy(h, part, target, me_p).start())
        a_copy(h, part, twin, me_p).start()

    def finish(h):
        if h == 0:
            own_rows.wait()
            over_peers(lambda origin: w_copy(origin, origin).wait_recv())
        for part in range(PARTS):

            def relay(origin):
                a_copy(h, part, origin, origin).wait_recv()
                a_copy(h, part, twin, origin).start()

            over_alike(relay)
        for part in range(PARTS):
            over_twins(lambda origin: a_copy(h, part, origin, origin).wait_recv())
            project(h, part)

    def drain_attn(h, part):
        over_alike(lambda target: a_copy(h, part, target, me_p).wait_send())
        a_copy(h, part, twin, me_p).wait_send()
        over_alike(lambda origin: a_copy(h, part, twin, origin).wait_send())

    def over_peers(action):
        @pl.loop(1, peers)
        def _(step):
            action(lax.rem(me_p + step, peers))

    def attend(h, part):
        @pl.loop(part * part_blocks, (part + 1) * part_blocks, unroll=UNROLL)
        def _(b):
            q = q_ref[b, :, head_columns(h)]
            picks = [slot_ref[b * select + s] for s in range(select)]
            keyset = jnp.concatenate(
                [k_ref[b, :, head_columns(h)]] + [recv[h][i, 0] for i in picks], axis=0
            )
            valueset = jnp.concatenate(
                [v_ref[b, :, head_columns(h)]] + [recv[h][i, 1] for i in picks], axis=0
            )
            scores = lax.dot_general(q, keyset, NT_DIMS, preferred_element_type=F32)
            scores = scores * (1.0 / DH**0.5)
            position = lax.broadcasted_iota(jnp.int32, scores.shape, 1)
            scores = jnp.where(position < (count_ref[b] + 1) * TILE, scores, -jnp.inf)
            top = jnp.max(scores, axis=1, keepdims=True)
            probs = jnp.exp(scores - top)
            denom = jnp.sum(probs, axis=1, keepdims=True)
            mixed = jnp.dot(probs.astype(jnp.bfloat16), valueset, preferred_element_type=F32)
            attn[h, me_p, pl.ds(pl.multiple_of(b * TILE, TILE), TILE), :] = (mixed / denom).astype(
                jnp.bfloat16
            )

    row_tile = 2 * TILE

    def project(h, part):
        @pl.loop(part * part_rows // row_tile, (part + 1) * part_rows // row_tile)
        def _(r):
            span = pl.ds(pl.multiple_of(r * row_tile, row_tile), row_tile)
            left = jnp.concatenate([attn[h, p, span, :] for p in range(peers)], axis=1)
            right = jnp.concatenate([rows[p, head_columns(h), :] for p in range(peers)], axis=0)
            term = jnp.dot(left, right, preferred_element_type=F32)
            if h > 0:
                term = term + acc[span, :]
            if h == heads - 1:
                out_ref[span, :] = term.astype(out_ref.dtype)
            else:
                acc[span, :] = term

    exchange.prepare()
    pl.semaphore_wait(barrier, frames + peers - 2)
    exchange.begin()
    over_peers(lambda target: w_copy(target, me_p).start())
    exchange.follow()
    for h in range(heads):
        exchange.receive(h, (lambda: finish(h - 1)) if h > 0 else (lambda: None))
        for part in range(PARTS):
            attend(h, part)
            share(h, part)
    finish(heads - 1)
    exchange.drain()
    over_peers(lambda target: w_copy(target, me_p).wait_send())
    for h in range(heads):
        for part in range(PARTS):
            drain_attn(h, part)


def shards(queries, keys, values, block_ids, counts, w_out):
    frames = lax.axis_size("frames")
    peers = lax.axis_size("heads")
    here = lax.axis_index("frames")
    tokens, width = queries.shape
    blocks = tokens // TILE
    select = block_ids.shape[1]
    heads = width // DH
    requests = blocks * select
    capacity = max(2, (requests + frames - 1) // frames)
    features = w_out.shape[1] // peers
    slots = min(3, heads)

    ids = block_ids.reshape(frames, requests)
    owner = ids // blocks
    order = jnp.arange(requests, dtype=jnp.int32)
    same = (owner[:, :, None] == owner[:, None, :]) & (order[:, None] < order[None, :])
    slot = owner * capacity + jnp.sum(same.astype(jnp.int32), axis=1)
    hit = slot[:, None, :] == jnp.arange(frames * capacity, dtype=jnp.int32)[:, None]
    pick = jnp.sum(jnp.where(hit, (ids % blocks)[:, None, :], 0), axis=2).reshape(-1)
    my_slot = lax.dynamic_slice_in_dim(slot, here, 1, 0).reshape(requests)

    smem = pl.BlockSpec(memory_space=pltpu.SMEM)
    vmem = pl.BlockSpec(memory_space=pltpu.VMEM)
    tiles = (blocks, TILE, width)
    dma = pltpu.SemaphoreType.DMA
    bf16 = jnp.bfloat16
    common = [
        pltpu.VMEM((peers, width, features), bf16),
        pltpu.VMEM((heads, peers, tokens, DH), bf16),
        pltpu.VMEM((tokens, features), F32),
    ]
    common_sems = [
        dma((peers,)), dma((peers,)), dma((heads, PARTS, peers, peers)),
        dma((heads, PARTS, peers)), dma,
    ]
    recv = [pltpu.VMEM((frames * capacity, 2, TILE, DH), bf16)] * heads
    extra = [
        pltpu.VMEM((slots, frames, capacity, 2, TILE, DH), bf16),
        dma((heads, frames)),
        dma((heads, frames)),
    ]
    dims = (frames, peers, blocks, select, capacity, heads, slots)
    return pl.pallas_call(
        functools.partial(layer_kernel, dims),
        out_shape=jax.ShapeDtypeStruct((tokens, features), bf16),
        in_specs=[smem, smem, smem, vmem, vmem, vmem, pl.BlockSpec(memory_space=pl.ANY)],
        out_specs=vmem,
        scratch_shapes=common + common_sems + recv + extra,
        compiler_params=pltpu.CompilerParams(
            collective_id=0, has_side_effects=True, vmem_limit_bytes=VMEM_BYTES
        ),
    )(
        pick, my_slot, counts, queries.reshape(tiles), keys.reshape(tiles), values.reshape(tiles),
        w_out,
    )


def column_kernel(
    dims, ids_ref, own_count_ref, q_hbm, k_hbm, v_hbm, w_ref, out_ref,
    q_ref, k_ref, v_ref, rows, attn, acc, qall, count, osend, orecv, ssend, srecv, oself, sself, weights, finished, place, usable,
    w_send, w_recv, a_send, a_recv, own_sem, load_sem, turn_sem, out_sem,
    kv_send, kv_recv, q_send, q_recv, c_send, c_recv, o_send, o_recv, s_send, s_recv, *kv,
):
    frames, peers, blocks, select, heads = dims
    keys, values = kv[:heads], kv[heads:]
    me_f, me_p = lax.axis_index("frames"), lax.axis_index("heads")
    line = frames // PAIR
    z, x = me_f // PAIR, me_f % PAIR
    half = z // (line // 2)
    mid, end = half + 1, (line - 1) * half
    across = line - 1 - mid
    is_mid = z == mid
    is_end = z == end
    other = 1 - x
    depth = heads * DH
    features = rows.shape[2]
    part_blocks = blocks // PARTS
    part_rows = part_blocks * TILE
    exponent = LOG2E / DH**0.5

    def at(zz, xx):
        return (zz * PAIR + xx, me_p)

    loads = [
        pltpu.make_async_copy(source, held, load_sem.at[i])
        for i, (source, held) in enumerate(((k_hbm, k_ref), (v_hbm, v_ref), (q_hbm, q_ref)))
    ]
    for load in loads:
        load.start()
    barrier = pltpu.get_barrier_semaphore()

    def greet(device):
        pl.semaphore_signal(barrier, inc=1, device_id=device, device_id_type=MESH)

    @pl.loop(1, peers)
    def _(step):
        greet((me_f, lax.rem(me_p + step, peers)))

    greet(at(z, other))
    greet(at(mid + end - z, x))
    greet(at(mid + end - z, other))

    @pl.when(is_mid)
    def _():
        greet(at(across, x))

    def columns_of(peer):
        return pl.ds(pl.multiple_of(peer * features, features), features)

    own_rows = pltpu.make_async_copy(w_ref.at[:, columns_of(me_p)], rows.at[me_p], own_sem)
    own_rows.start()

    @pl.loop(0, blocks)
    def _(b):
        count[0, pl.ds(b, 1), :] = jnp.full((1, TILE), own_count_ref[b], jnp.int32)

    def send(source, target, send_sem, recv_sem, device):
        return pltpu.make_async_remote_copy(
            src_ref=source, dst_ref=target, send_sem=send_sem, recv_sem=recv_sem,
            device_id=device, device_id_type=MESH,
        )

    def kv_copy(h, flow, which):
        held = (keys, values)[which][h]
        source = (k_ref, v_ref)[which].at[:, :, head_columns(h)]
        if flow == 2:
            source = held.at[pl.ds(blocks, blocks)]
        return send(
            source, held.at[pl.ds((flow + 1) * blocks, blocks)],
            kv_send.at[flow, h, which], kv_recv.at[flow, h, which],
            at(mid, x) if flow == 0 else at(across, x),
        )

    def q_copy(h, flow):
        source = q_ref.at[:, :, head_columns(h)] if flow < 2 else qall.at[h, 1]
        return send(
            source, qall.at[h, flow], q_send.at[flow, h], q_recv.at[flow, h],
            at(mid, x) if flow == 1 else at(z, other),
        )

    def c_copy(flow):
        device = (at(z, other), at(mid, x), at(mid, other))[flow]
        return send(
            count.at[0], count.at[flow + 1], c_send.at[flow], c_recv.at[flow], device
        )

    def partial_device(slot):
        to_z = z + (end - z) * ((slot + 1) // 2)
        to_x = x + (other - x) * ((slot + 1) % 2)
        return at(to_z, to_x)

    def o_copy(h, part, slot):
        span = pl.ds(part * part_rows, part_rows)
        return send(
            osend.at[h, slot, span], orecv.at[h, slot, span],
            o_send.at[h, part, slot], o_recv.at[h, part, slot], partial_device(slot),
        )

    def s_copy(h, slot):
        return send(
            ssend.at[h, slot], srecv.at[h, slot], s_send.at[h, slot], s_recv.at[h, slot],
            partial_device(slot),
        )

    def w_copy(h, target, origin):
        span = pl.ds(h * DH, DH)
        return send(
            w_ref.at[span, columns_of(target)], rows.at[origin, span],
            w_send.at[h, target], w_recv.at[h, origin], (me_f, target),
        )

    def a_copy(h, part, target, origin):
        held = attn.at[h, origin, pl.ds(part * part_rows, part_rows)]
        to_twin = lax.rem(target + me_p, 2)
        lane_of = target + to_twin * (origin - me_p)
        return send(
            held, held, a_send.at[h, part, lane_of], a_recv.at[h, part, origin],
            (me_f, target),
        )

    twin = me_p + 1 - 2 * lax.rem(me_p, 2)

    def over_peers(action):
        @pl.loop(1, peers)
        def _(step):
            action(lax.rem(me_p + step, peers))

    def over_alike(action):
        @pl.loop(1, peers // 2)
        def _(step):
            action(lax.rem(me_p + 2 * step, peers))

    def over_twins(action):
        @pl.loop(0, peers // 2)
        def _(step):
            action(lax.rem(twin + 2 * step, peers))

    def share(h, part):
        over_alike(lambda target: a_copy(h, part, target, me_p).start())
        a_copy(h, part, twin, me_p).start()

    def pass_on(h):
        for part in range(PARTS):

            def relay(origin):
                a_copy(h, part, origin, origin).wait_recv()
                a_copy(h, part, twin, origin).start()

            over_alike(relay)

    def finish(h):
        if h == 0:
            own_rows.wait()
        over_peers(lambda origin: w_copy(h, origin, origin).wait_recv())
        for part in range(PARTS):
            over_twins(lambda origin: a_copy(h, part, origin, origin).wait_recv())
            project(h, part)

    def drain_attn(h, part):
        over_alike(lambda target: a_copy(h, part, target, me_p).wait_send())
        a_copy(h, part, twin, me_p).wait_send()
        over_alike(lambda origin: a_copy(h, part, twin, origin).wait_send())

    row_tile = 2 * TILE

    def out_copy(r):
        span = pl.ds(pl.multiple_of(r * row_tile, row_tile), row_tile)
        return pltpu.make_async_copy(finished.at[span], out_ref.at[span], out_sem.at[r])

    def project(h, part):
        @pl.loop(part * part_rows // row_tile, (part + 1) * part_rows // row_tile)
        def _(r):
            span = pl.ds(pl.multiple_of(r * row_tile, row_tile), row_tile)
            left = jnp.concatenate([attn[h, p, span, :] for p in range(peers)], axis=1)
            right = jnp.concatenate([rows[p, head_columns(h), :] for p in range(peers)], axis=0)
            term = jnp.dot(left, right, preferred_element_type=F32)
            if h > 0:
                term = term + acc[span, :]
            if h == heads - 1:
                finished[span, :] = term.astype(out_ref.dtype)
                out_copy(r).start()
            else:
                acc[span, :] = term

    def fill_tables():
        for role in range(4):
            role_z = z if role < 2 else end
            role_x = x if role % 2 == 0 else other

            @pl.loop(0, blocks)
            def _(b):
                for s in range(select):
                    chosen = ids_ref[s, (role_z * PAIR + role_x) * blocks + b]
                    owner = lax.div(chosen, blocks)
                    owner_z, owner_x = lax.div(owner, PAIR), lax.rem(owner, PAIR)
                    here = owner_z == z
                    near = owner_z == end
                    source = jnp.where(
                        here, 0, jnp.where(near, 1, jnp.where(owner_z == across, 2, 3))
                    )
                    ours = here | is_mid
                    if role > 1:
                        ours = ours & jnp.logical_not(near)
                    ours = ours & (owner_x == x)
                    entry = (role * blocks + b) * select + s
                    index = source * blocks + lax.rem(chosen, blocks)
                    place[entry] = jnp.where(ours, index, 0)
                    usable[entry] = jnp.where(ours, 1, 0)

    def own_block(h):
        @pl.loop(0, blocks)
        def _(b):
            keys[h][b] = k_ref[b, :, head_columns(h)]
            values[h][b] = v_ref[b, :, head_columns(h)]

    lane = lax.broadcasted_iota(jnp.int32, (TILE, TILE), 1)

    def weigh(h, role, b, query, first_keys):
        entries = [(role * blocks + b) * select + s for s in range(select)]
        keyset = jnp.concatenate(first_keys + [keys[h][place[e]] for e in entries], axis=0)
        scores = lax.dot_general(query, keyset, NT_DIMS, preferred_element_type=F32)
        used = count[role, pl.ds(b, 1), :]
        lead = len(first_keys)
        pieces = [scores[:, i * TILE : (i + 1) * TILE] for i in range(lead + select)]
        for s in range(select):
            keep = jnp.broadcast_to(used * usable[entries[s]], (TILE, TILE)) > s
            pieces[lead + s] = jnp.where(keep, pieces[lead + s], -jnp.inf)
        top = jnp.max(functools.reduce(jnp.maximum, pieces), axis=1, keepdims=True)
        top = jnp.maximum(top, LOWEST)
        probs = [jnp.exp2((piece - top) * exponent) for piece in pieces]
        denom = jnp.sum(functools.reduce(jnp.add, probs), axis=1, keepdims=True)
        for i, piece in enumerate(probs):
            weights[role, b, :, i * TILE : (i + 1) * TILE] = piece.astype(jnp.bfloat16)
        return top * exponent, denom

    def mix(h, role, b, first_values):
        entries = [(role * blocks + b) * select + s for s in range(select)]
        valueset = jnp.concatenate(first_values + [values[h][place[e]] for e in entries], axis=0)
        held = weights[role, b, :, : (len(first_values) + select) * TILE]
        return jnp.dot(held, valueset, preferred_element_type=F32)

    def rows_of(levels):
        tile = jnp.zeros((TILE, TILE), F32)
        for j, (top, denom) in enumerate(levels):
            tile = jnp.where(lane == j, top, tile)
            tile = jnp.where(lane == part_blocks + j, denom, tile)
        return tile.T[: 2 * part_blocks]

    away = is_mid.astype(jnp.int32)

    def over_others(action):
        first = 2 * PARTS

        @pl.loop(first * (1 - away), first + PARTS)
        def _(step):
            late = step // first
            role = late + (1 - late) * (3 - step % 2)
            part = late * (step - first) + (1 - late) * (step // 2)
            action(step, role, part)

    def weigh_others(h):
        def action(step, role, part):
            levels = []
            for j in range(part_blocks):
                b = part * part_blocks + j
                levels.append(weigh(h, role, b, qall[h, role - 1, b], []))
            ssend[h, role - 1, part] = rows_of(levels)

            @pl.when(part == PARTS - 1)
            def _():
                s_copy(h, role - 1).start()

        over_others(action)

    def mix_others(h):
        def action(step, role, part):
            for j in range(part_blocks):
                b = part * part_blocks + j
                span = pl.ds(pl.multiple_of(b * TILE, TILE), TILE)
                osend[h, role - 1, span, :] = mix(h, role, b, []).astype(jnp.bfloat16)
            o_copy(h, part, role - 1).start()

        over_others(action)

    def weigh_own(h):
        @pl.loop(0, PARTS)
        def _(part):
            levels = []
            for j in range(part_blocks):
                b = part * part_blocks + j
                query = q_ref[b, :, head_columns(h)]
                levels.append(weigh(h, 0, b, query, [k_ref[b, :, head_columns(h)]]))
            sself[part] = rows_of(levels)

    def mix_own(h):
        @pl.loop(0, PARTS)
        def _(part):
            for j in range(part_blocks):
                b = part * part_blocks + j
                span = pl.ds(pl.multiple_of(b * TILE, TILE), TILE)
                oself[span, :] = mix(h, 0, b, [v_ref[b, :, head_columns(h)]])

    def merge(h, part, slots):
        levels = [sself[part]] + [srecv[h, slot, part] for slot in range(slots)]
        tops = [level[:part_blocks] for level in levels]
        denoms = [level[part_blocks:] for level in levels]
        top = functools.reduce(jnp.maximum, tops)
        shares = [jnp.exp2(one - top) for one in tops]
        total = functools.reduce(jnp.add, [share * d for share, d in zip(shares, denoms)])
        spare = TILE - part_blocks * len(shares)
        tall = jnp.concatenate(
            [share / total for share in shares] + [jnp.zeros((spare, TILE), F32)], axis=0
        ).T
        for j in range(part_blocks):
            span = pl.ds((part * part_blocks + j) * TILE, TILE)
            value = oself[span, :] * tall[:, j : j + 1]
            for slot in range(slots):
                column = part_blocks * (slot + 1) + j
                value = value + orecv[h, slot, span, :].astype(F32) * tall[:, column : column + 1]
            attn[h, me_p, span, :] = value.astype(jnp.bfloat16)

    def combine(h, part):
        o_copy(h, part, 0).wait_recv()

        @pl.when(is_mid)
        def _():
            merge(h, part, 1)

        @pl.when(is_end)
        def _():
            for slot in (1, 2):
                o_copy(h, part, slot).wait_recv()
            merge(h, part, 3)

    def relay_on(h):
        last = h == heads - 1
        for which in range(2):
            kv_copy(h, 0, which).wait_recv()
            kv_copy(h, 2, which).start()
            if last and h > 0 and which == 0:
                kv_copy(h, 1, 1).start()
        if not last:
            kv_copy(h + 1, 1, 0).start()
            if h + 1 < heads - 1:
                kv_copy(h + 1, 1, 1).start()
        q_copy(h, 1).wait_recv()
        q_copy(h, 2).start()

    def send_early(h):
        @pl.when(is_end)
        def _():
            for which in range(2):
                kv_copy(h, 0, which).start()
            q_copy(h, 1).start()

    def open_column():
        @pl.when(is_mid)
        def _():
            for which in range(2):
                kv_copy(0, 1, which).start()

        for h in range(early):
            send_early(h)

    early = min(EARLY, heads)
    leads = lax.rem(me_p, 2) == 1

    def send_rows(h):
        over_peers(lambda target: w_copy(h, target, me_p).start())

    pl.semaphore_wait(barrier, peers + 2 + away)
    for load in loads:
        load.wait()

    c_copy(0).start()

    @pl.when(is_end)
    def _():
        c_copy(1).start()
        c_copy(2).start()

    @pl.when(leads)
    def _():
        open_column()

    for h in range(early):
        q_copy(h, 0).start()
        send_rows(h)
    fill_tables()
    own_block(0)

    def first_sent(flow):
        for which in range(2):
            kv_copy(0, flow, which).wait_send()

    @pl.when(leads & is_end)
    def _():
        first_sent(0)

    @pl.when(leads & is_mid)
    def _():
        first_sent(1)

    @pl.when(leads)
    def _():
        pl.semaphore_signal(turn_sem, inc=1, device_id=(me_f, twin), device_id_type=MESH)

    @pl.when(jnp.logical_not(leads))
    def _():
        pl.semaphore_wait(turn_sem, 1)
        open_column()

    c_copy(0).wait_recv()

    @pl.when(is_mid)
    def _():
        relay_on(0)
        c_copy(1).wait_recv()
        c_copy(2).wait_recv()

    def drain_sends(h):
        over_peers(lambda target: w_copy(h, target, me_p).wait_send())
        q_copy(h, 0).wait_send()
        started_here = jnp.logical_not(leads) if h == 0 else h >= 0

        @pl.when(is_end & started_here)
        def _():
            for which in range(2):
                kv_copy(h, 0, which).wait_send()

        @pl.when(is_mid & started_here)
        def _():
            for which in range(2):
                kv_copy(h, 1, which).wait_send()

        @pl.when(is_end)
        def _():
            q_copy(h, 1).wait_send()

        @pl.when(is_mid)
        def _():
            for which in range(2):
                kv_copy(h, 2, which).wait_send()
            q_copy(h, 2).wait_send()

    def drain_partials(h):
        @pl.loop(0, 1 + 2 * away)
        def _(slot):
            s_copy(h, slot).wait_send()
            for part in range(PARTS):
                o_copy(h, part, slot).wait_send()

    def settle(h):
        if h >= 0:
            drain_sends(h)
            drain_partials(h)
            finish(h)
        if h >= 1:
            for part in range(PARTS):
                drain_attn(h - 1, part)

    for h in range(heads):
        if h + EARLY < heads:
            q_copy(h + EARLY, 0).start()
            send_early(h + EARLY)
        if h > 0:
            own_block(h)
        last = h == heads - 1

        def catch_up():
            settle(h - 2)
            if h > 0:
                pass_on(h - 1)

        if 0 < h < heads - 1:

            @pl.when(is_mid)
            def _():
                relay_on(h + 1)

        if last:
            catch_up()
            if h > 0:

                @pl.when(jnp.logical_not(leads))
                def _():
                    finish(h - 1)

        q_copy(h, 0).wait_recv()

        def arrived(which):
            kv_copy(h, 1, which).wait_recv()
            kv_copy(h, 2, which).wait_recv()

        @pl.when(is_mid)
        def _():
            q_copy(h, 2).wait_recv()
            arrived(0)

        weigh_others(h)
        weigh_own(h)

        @pl.when(is_mid)
        def _():
            arrived(1)

        mix_others(h)
        mix_own(h)
        if not last:
            if h == 0:

                @pl.when(is_mid)
                def _():
                    relay_on(h + 1)

            catch_up()
        s_copy(h, 0).wait_recv()

        @pl.when(is_end)
        def _():
            for slot in (1, 2):
                s_copy(h, slot).wait_recv()

        for part in range(PARTS):
            combine(h, part)
            share(h, part)
        if h + EARLY < heads:
            send_rows(h + EARLY)
    c_copy(0).wait_send()

    @pl.when(is_end)
    def _():
        c_copy(1).wait_send()
        c_copy(2).wait_send()

    if heads > 1:

        @pl.when(leads)
        def _():
            finish(heads - 2)

        drain_sends(heads - 2)
        drain_partials(heads - 2)
    drain_sends(heads - 1)
    pass_on(heads - 1)
    finish(heads - 1)
    drain_partials(heads - 1)
    for h in range(max(0, heads - 3), heads):
        for part in range(PARTS):
            drain_attn(h, part)
    for r in range(PARTS * part_rows // row_tile):
        out_copy(r).wait()


def column_shards(queries, keys, values, block_ids, counts, w_out):
    frames = lax.axis_size("frames")
    peers = lax.axis_size("heads")
    tokens, width = queries.shape
    blocks = tokens // TILE
    select = block_ids.shape[1]
    heads = width // DH
    features = w_out.shape[1] // peers
    smem = pl.BlockSpec(memory_space=pltpu.SMEM)
    tiles = (blocks, TILE, width)
    dma = pltpu.SemaphoreType.DMA
    bf16 = jnp.bfloat16
    level_rows = (PARTS, 2 * blocks // PARTS, TILE)
    scratch = [pltpu.VMEM(tiles, bf16)] * 3 + [
        pltpu.VMEM((peers, width, features), bf16),
        pltpu.VMEM((heads, peers, tokens, DH), bf16),
        pltpu.VMEM((tokens, features), F32),
        pltpu.VMEM((heads, 3, blocks, TILE, DH), bf16),
        pltpu.VMEM((4, blocks, TILE), jnp.int32),
        pltpu.VMEM((heads, 3, tokens, DH), bf16),
        pltpu.VMEM((heads, 3, tokens, DH), bf16),
        pltpu.VMEM((heads, 3) + level_rows, F32),
        pltpu.VMEM((heads, 3) + level_rows, F32),
        pltpu.VMEM((tokens, DH), F32),
        pltpu.VMEM(level_rows, F32),
        pltpu.VMEM((4, blocks, TILE, (select + 1) * TILE), bf16),
        pltpu.VMEM((tokens, features), bf16),
        pltpu.SMEM((4 * blocks * select,), jnp.int32),
        pltpu.SMEM((4 * blocks * select,), jnp.int32),
        dma((heads, peers)), dma((heads, peers)), dma((heads, PARTS, peers)),
        dma((heads, PARTS, peers)), dma, dma((3,)), pltpu.SemaphoreType.REGULAR,
        dma((tokens // (2 * TILE),)),
        dma((3, heads, 2)), dma((3, heads, 2)), dma((3, heads)), dma((3, heads)),
        dma((3,)), dma((3,)),
        dma((heads, PARTS, 3)), dma((heads, PARTS, 3)), dma((heads, 3)), dma((heads, 3)),
    ] + [pltpu.VMEM((4 * blocks, TILE, DH), bf16)] * (2 * heads)
    dims = (frames, peers, blocks, select, heads)
    hbm = pl.BlockSpec(memory_space=pltpu.HBM)
    return pl.pallas_call(
        functools.partial(column_kernel, dims),
        out_shape=jax.ShapeDtypeStruct((tokens, features), bf16),
        in_specs=[smem, smem, hbm, hbm, hbm, hbm],
        out_specs=hbm,
        scratch_shapes=scratch,
        compiler_params=pltpu.CompilerParams(
            collective_id=0, has_side_effects=True, vmem_limit_bytes=VMEM_BYTES
        ),
    )(
        block_ids.T, counts,
        queries.reshape(tiles), keys.reshape(tiles), values.reshape(tiles), w_out,
    )


def solution(mesh):
    placed = (
        P("frames", "heads"),
        P("frames", "heads"),
        P("frames", "heads"),
        P(),
        P("frames"),
        P("heads", None),
    )
    columns = mesh.shape["frames"] == PAIR * LINE and mesh.shape["heads"] % 2 == 0
    return jax.shard_map(
        column_shards if columns else shards, mesh=mesh, in_specs=placed, out_specs=P("frames", "heads"), check_vma=False
    )
```

```python
import functools
import math

import jax
import jax.numpy as jnp
from jax import lax
from jax.experimental import pallas as pl
from jax.experimental.pallas import tpu as pltpu
from jax.sharding import PartitionSpec as P

DH = 128
TILE = 128
MESH = pl.DeviceIdType.MESH
F32 = jnp.float32
PAIR = 2
LINE = 4
PARTS = 2
UNROLL = 2
EARLY = 3
LOG2E = math.log2(math.e)
LOWEST = -1e38
VMEM_BYTES = 67043328
NT_DIMS = (((1,), (1,)), ((), ()))


def head_columns(h):
    return slice(h * DH, (h + 1) * DH)


class direct_exchange:
    def __init__(self, dims, pick_ref, k_ref, v_ref, recv, send, kv_send, kv_recv):
        self.frames, _, _, _, self.capacity, self.heads, self.slots = dims
        self.pick_ref, self.k_ref, self.v_ref, self.recv = pick_ref, k_ref, v_ref, recv
        self.send, self.kv_send, self.kv_recv = send, kv_send, kv_recv
        self.me_f, self.me_p = lax.axis_index("frames"), lax.axis_index("heads")

    def copy(self, h, target, origin):
        return pltpu.make_async_remote_copy(
            src_ref=self.send.at[h % self.slots, target],
            dst_ref=self.recv[h].at[pl.ds(origin * self.capacity, self.capacity)],
            send_sem=self.kv_send.at[h, target],
            recv_sem=self.kv_recv.at[h, origin],
            device_id=(target, self.me_p),
            device_id_type=MESH,
        )

    def others(self, action):
        @pl.loop(1, self.frames)
        def _(step):
            action(lax.rem(self.me_f + step, self.frames))

    def pick(self, target, c):
        return self.pick_ref[(target * self.frames + self.me_f) * self.capacity + c]

    def build(self, h):
        if h >= self.slots:
            self.others(lambda target: self.copy(h - self.slots, target, self.me_f).wait_send())

        def fill(target):
            for c in range(self.capacity):
                index = self.pick(target, c)
                self.send[h % self.slots, target, c, 0] = self.k_ref[index, :, head_columns(h)]
                self.send[h % self.slots, target, c, 1] = self.v_ref[index, :, head_columns(h)]

        self.others(fill)
        for c in range(self.capacity):
            index = self.pick(self.me_f, c)
            self.recv[h][self.me_f * self.capacity + c, 0] = self.k_ref[index, :, head_columns(h)]
            self.recv[h][self.me_f * self.capacity + c, 1] = self.v_ref[index, :, head_columns(h)]

    def start(self, h):
        self.others(lambda target: self.copy(h, target, self.me_f).start())

    def prepare(self):
        self.build(0)

    def begin(self):
        self.start(0)

    def follow(self):
        if self.heads > 1:
            self.build(1)
            self.start(1)

    def receive(self, h, midway):
        if h + 2 < self.heads:
            self.build(h + 2)
        midway()
        self.others(lambda origin: self.copy(h, origin, origin).wait_recv())
        if h + 2 < self.heads:
            self.start(h + 2)

    def drain(self):
        for h in range(max(0, self.heads - self.slots), self.heads):
            self.others(lambda target: self.copy(h, target, self.me_f).wait_send())


def layer_kernel(
    dims, pick_ref, slot_ref, count_ref, q_ref, k_ref, v_ref, w_ref, out_ref,
    rows, attn, acc, w_send, w_recv, a_send, a_recv, own_sem, *kv_refs,
):
    frames, peers, blocks, select, capacity, heads, slots = dims
    recv, kv_refs = kv_refs[:heads], kv_refs[heads:]
    me_f, me_p = lax.axis_index("frames"), lax.axis_index("heads")
    depth = heads * DH
    features = rows.shape[2]

    barrier = pltpu.get_barrier_semaphore()

    @pl.loop(1, frames)
    def _(step):
        pl.semaphore_signal(
            barrier, inc=1, device_id=(lax.rem(me_f + step, frames), me_p), device_id_type=MESH
        )

    @pl.loop(1, peers)
    def _(step):
        pl.semaphore_signal(
            barrier, inc=1, device_id=(me_f, lax.rem(me_p + step, peers)), device_id_type=MESH
        )

    def columns_of(peer):
        return pl.ds(pl.multiple_of(peer * features, features), features)

    own_rows = pltpu.make_async_copy(w_ref.at[:, columns_of(me_p)], rows.at[me_p], own_sem)
    own_rows.start()

    exchange = direct_exchange(dims, pick_ref, k_ref, v_ref, recv, *kv_refs)

    def w_copy(target, origin):
        return pltpu.make_async_remote_copy(
            src_ref=w_ref.at[:, columns_of(target)],
            dst_ref=rows.at[origin],
            send_sem=w_send.at[target],
            recv_sem=w_recv.at[origin],
            device_id=(me_f, target),
            device_id_type=MESH,
        )

    part_blocks = blocks // PARTS
    part_rows = part_blocks * TILE

    def a_copy(h, part, target, origin):
        held = attn.at[h, origin, pl.ds(part * part_rows, part_rows)]
        return pltpu.make_async_remote_copy(
            src_ref=held,
            dst_ref=held,
            send_sem=a_send.at[h, part, target, origin],
            recv_sem=a_recv.at[h, part, origin],
            device_id=(me_f, target),
            device_id_type=MESH,
        )

    twin = me_p + 1 - 2 * lax.rem(me_p, 2)

    def over_alike(action):
        @pl.loop(1, peers // 2)
        def _(step):
            action(lax.rem(me_p + 2 * step, peers))

    def over_twins(action):
        @pl.loop(0, peers // 2)
        def _(step):
            action(lax.rem(twin + 2 * step, peers))

    def share(h, part):
        over_alike(lambda target: a_copy(h, part, target, me_p).start())
        a_copy(h, part, twin, me_p).start()

    def finish(h):
        if h == 0:
            own_rows.wait()
            over_peers(lambda origin: w_copy(origin, origin).wait_recv())
        for part in range(PARTS):

            def relay(origin):
                a_copy(h, part, origin, origin).wait_recv()
                a_copy(h, part, twin, origin).start()

            over_alike(relay)
        for part in range(PARTS):
            over_twins(lambda origin: a_copy(h, part, origin, origin).wait_recv())
            project(h, part)

    def drain_attn(h, part):
        over_alike(lambda target: a_copy(h, part, target, me_p).wait_send())
        a_copy(h, part, twin, me_p).wait_send()
        over_alike(lambda origin: a_copy(h, part, twin, origin).wait_send())

    def over_peers(action):
        @pl.loop(1, peers)
        def _(step):
            action(lax.rem(me_p + step, peers))

    def attend(h, part):
        @pl.loop(part * part_blocks, (part + 1) * part_blocks, unroll=UNROLL)
        def _(b):
            q = q_ref[b, :, head_columns(h)]
            picks = [slot_ref[b * select + s] for s in range(select)]
            keyset = jnp.concatenate(
                [k_ref[b, :, head_columns(h)]] + [recv[h][i, 0] for i in picks], axis=0
            )
            valueset = jnp.concatenate(
                [v_ref[b, :, head_columns(h)]] + [recv[h][i, 1] for i in picks], axis=0
            )
            scores = lax.dot_general(q, keyset, NT_DIMS, preferred_element_type=F32)
            scores = scores * (1.0 / DH**0.5)
            position = lax.broadcasted_iota(jnp.int32, scores.shape, 1)
            scores = jnp.where(position < (count_ref[b] + 1) * TILE, scores, -jnp.inf)
            top = jnp.max(scores, axis=1, keepdims=True)
            probs = jnp.exp(scores - top)
            denom = jnp.sum(probs, axis=1, keepdims=True)
            mixed = jnp.dot(probs.astype(jnp.bfloat16), valueset, preferred_element_type=F32)
            attn[h, me_p, pl.ds(pl.multiple_of(b * TILE, TILE), TILE), :] = (mixed / denom).astype(
                jnp.bfloat16
            )

    row_tile = 2 * TILE

    def project(h, part):
        @pl.loop(part * part_rows // row_tile, (part + 1) * part_rows // row_tile)
        def _(r):
            span = pl.ds(pl.multiple_of(r * row_tile, row_tile), row_tile)
            left = jnp.concatenate([attn[h, p, span, :] for p in range(peers)], axis=1)
            right = jnp.concatenate([rows[p, head_columns(h), :] for p in range(peers)], axis=0)
            term = jnp.dot(left, right, preferred_element_type=F32)
            if h > 0:
                term = term + acc[span, :]
            if h == heads - 1:
                out_ref[span, :] = term.astype(out_ref.dtype)
            else:
                acc[span, :] = term

    exchange.prepare()
    pl.semaphore_wait(barrier, frames + peers - 2)
    exchange.begin()
    over_peers(lambda target: w_copy(target, me_p).start())
    exchange.follow()
    for h in range(heads):
        exchange.receive(h, (lambda: finish(h - 1)) if h > 0 else (lambda: None))
        for part in range(PARTS):
            attend(h, part)
            share(h, part)
    finish(heads - 1)
    exchange.drain()
    over_peers(lambda target: w_copy(target, me_p).wait_send())
    for h in range(heads):
        for part in range(PARTS):
            drain_attn(h, part)


def shards(queries, keys, values, block_ids, counts, w_out):
    frames = lax.axis_size("frames")
    peers = lax.axis_size("heads")
    here = lax.axis_index("frames")
    tokens, width = queries.shape
    blocks = tokens // TILE
    select = block_ids.shape[1]
    heads = width // DH
    requests = blocks * select
    capacity = max(2, (requests + frames - 1) // frames)
    features = w_out.shape[1] // peers
    slots = min(3, heads)

    ids = block_ids.reshape(frames, requests)
    owner = ids // blocks
    order = jnp.arange(requests, dtype=jnp.int32)
    same = (owner[:, :, None] == owner[:, None, :]) & (order[:, None] < order[None, :])
    slot = owner * capacity + jnp.sum(same.astype(jnp.int32), axis=1)
    hit = slot[:, None, :] == jnp.arange(frames * capacity, dtype=jnp.int32)[:, None]
    pick = jnp.sum(jnp.where(hit, (ids % blocks)[:, None, :], 0), axis=2).reshape(-1)
    my_slot = lax.dynamic_slice_in_dim(slot, here, 1, 0).reshape(requests)

    smem = pl.BlockSpec(memory_space=pltpu.SMEM)
    vmem = pl.BlockSpec(memory_space=pltpu.VMEM)
    tiles = (blocks, TILE, width)
    dma = pltpu.SemaphoreType.DMA
    bf16 = jnp.bfloat16
    common = [
        pltpu.VMEM((peers, width, features), bf16),
        pltpu.VMEM((heads, peers, tokens, DH), bf16),
        pltpu.VMEM((tokens, features), F32),
    ]
    common_sems = [
        dma((peers,)), dma((peers,)), dma((heads, PARTS, peers, peers)),
        dma((heads, PARTS, peers)), dma,
    ]
    recv = [pltpu.VMEM((frames * capacity, 2, TILE, DH), bf16)] * heads
    extra = [
        pltpu.VMEM((slots, frames, capacity, 2, TILE, DH), bf16),
        dma((heads, frames)),
        dma((heads, frames)),
    ]
    dims = (frames, peers, blocks, select, capacity, heads, slots)
    return pl.pallas_call(
        functools.partial(layer_kernel, dims),
        out_shape=jax.ShapeDtypeStruct((tokens, features), bf16),
        in_specs=[smem, smem, smem, vmem, vmem, vmem, pl.BlockSpec(memory_space=pl.ANY)],
        out_specs=vmem,
        scratch_shapes=common + common_sems + recv + extra,
        compiler_params=pltpu.CompilerParams(
            collective_id=0, has_side_effects=True, vmem_limit_bytes=VMEM_BYTES
        ),
    )(
        pick, my_slot, counts, queries.reshape(tiles), keys.reshape(tiles), values.reshape(tiles),
        w_out,
    )


def column_kernel(
    dims, ids_ref, own_count_ref, q_hbm, k_hbm, v_hbm, w_ref, out_ref,
    q_ref, k_ref, v_ref, rows, attn, acc, qall, count, osend, orecv, ssend, srecv, oself, sself, weights, finished, place, usable,
    w_send, w_recv, a_send, a_recv, own_sem, load_sem, turn_sem, out_sem,
    kv_send, kv_recv, q_send, q_recv, c_send, c_recv, o_send, o_recv, s_send, s_recv, *kv,
):
    frames, peers, blocks, select, heads = dims
    keys, values = kv[:heads], kv[heads:]
    me_f, me_p = lax.axis_index("frames"), lax.axis_index("heads")
    line = frames // PAIR
    z, x = me_f // PAIR, me_f % PAIR
    half = z // (line // 2)
    mid, end = half + 1, (line - 1) * half
    across = line - 1 - mid
    is_mid = z == mid
    is_end = z == end
    other = 1 - x
    depth = heads * DH
    features = rows.shape[2]
    part_blocks = blocks // PARTS
    part_rows = part_blocks * TILE
    exponent = LOG2E / DH**0.5

    def at(zz, xx):
        return (zz * PAIR + xx, me_p)

    loads = [
        pltpu.make_async_copy(source, held, load_sem.at[i])
        for i, (source, held) in enumerate(((k_hbm, k_ref), (v_hbm, v_ref), (q_hbm, q_ref)))
    ]
    for load in loads:
        load.start()
    barrier = pltpu.get_barrier_semaphore()

    def greet(device):
        pl.semaphore_signal(barrier, inc=1, device_id=device, device_id_type=MESH)

    @pl.loop(1, peers)
    def _(step):
        greet((me_f, lax.rem(me_p + step, peers)))

    greet(at(z, other))
    greet(at(mid + end - z, x))
    greet(at(mid + end - z, other))

    @pl.when(is_mid)
    def _():
        greet(at(across, x))

    def columns_of(peer):
        return pl.ds(pl.multiple_of(peer * features, features), features)

    own_rows = pltpu.make_async_copy(w_ref.at[:, columns_of(me_p)], rows.at[me_p], own_sem)
    own_rows.start()

    @pl.loop(0, blocks)
    def _(b):
        count[0, pl.ds(b, 1), :] = jnp.full((1, TILE), own_count_ref[b], jnp.int32)

    def send(source, target, send_sem, recv_sem, device):
        return pltpu.make_async_remote_copy(
            src_ref=source, dst_ref=target, send_sem=send_sem, recv_sem=recv_sem,
            device_id=device, device_id_type=MESH,
        )

    def kv_copy(h, flow, which):
        held = (keys, values)[which][h]
        source = (k_ref, v_ref)[which].at[:, :, head_columns(h)]
        if flow == 2:
            source = held.at[pl.ds(blocks, blocks)]
        return send(
            source, held.at[pl.ds((flow + 1) * blocks, blocks)],
            kv_send.at[flow, which, int(h > 0)], kv_recv.at[flow, h, which],
            at(mid, x) if flow == 0 else at(across, x),
        )

    def q_copy(h, flow):
        source = q_ref.at[:, :, head_columns(h)] if flow < 2 else qall.at[h, 1]
        return send(
            source, qall.at[h, flow], q_send.at[flow], q_recv.at[flow, h],
            at(mid, x) if flow == 1 else at(z, other),
        )

    def c_copy(flow):
        device = (at(z, other), at(mid, x), at(mid, other))[flow]
        return send(
            count.at[0], count.at[flow + 1], c_send.at[flow], c_recv.at[flow], device
        )

    def partial_device(slot):
        to_z = z + (end - z) * ((slot + 1) // 2)
        to_x = x + (other - x) * ((slot + 1) % 2)
        return at(to_z, to_x)

    def o_copy(h, part, slot):
        span = pl.ds(part * part_rows, part_rows)
        return send(
            osend.at[h, slot, span], orecv.at[h, slot, span],
            o_send.at[slot], o_recv.at[h, part, slot], partial_device(slot),
        )

    def s_copy(h, slot):
        return send(
            ssend.at[h, slot], srecv.at[h, slot], s_send.at[slot], s_recv.at[h, slot],
            partial_device(slot),
        )

    def w_copy(h, target, origin):
        span = pl.ds(h * DH, DH)
        return send(
            w_ref.at[span, columns_of(target)], rows.at[origin, span],
            w_send.at[target], w_recv.at[h, origin], (me_f, target),
        )

    def a_copy(h, part, target, origin):
        held = attn.at[h, origin, pl.ds(part * part_rows, part_rows)]
        to_twin = lax.rem(target + me_p, 2)
        lane_of = target + to_twin * (origin - me_p)
        return send(
            held, held, a_send.at[lane_of], a_recv.at[h, part, origin],
            (me_f, target),
        )

    twin = me_p + 1 - 2 * lax.rem(me_p, 2)

    def over_peers(action):
        @pl.loop(1, peers)
        def _(step):
            action(lax.rem(me_p + step, peers))

    def over_alike(action):
        @pl.loop(1, peers // 2)
        def _(step):
            action(lax.rem(me_p + 2 * step, peers))

    def over_twins(action):
        @pl.loop(0, peers // 2)
        def _(step):
            action(lax.rem(twin + 2 * step, peers))

    def share(h, part):
        over_alike(lambda target: a_copy(h, part, target, me_p).start())
        a_copy(h, part, twin, me_p).start()

    def pass_on(h):
        for part in range(PARTS):

            def relay(origin):
                a_copy(h, part, origin, origin).wait_recv()
                a_copy(h, part, twin, origin).start()

            over_alike(relay)

    def finish(h):
        if h == 0:
            own_rows.wait()
        over_peers(lambda origin: w_copy(h, origin, origin).wait_recv())
        for part in range(PARTS):
            over_twins(lambda origin: a_copy(h, part, origin, origin).wait_recv())
            project(h, part)

    row_tile = 2 * TILE

    def out_copy(r):
        span = pl.ds(pl.multiple_of(r * row_tile, row_tile), row_tile)
        return pltpu.make_async_copy(finished.at[span], out_ref.at[span], out_sem.at[r])

    def project(h, part):
        @pl.loop(part * part_rows // row_tile, (part + 1) * part_rows // row_tile)
        def _(r):
            span = pl.ds(pl.multiple_of(r * row_tile, row_tile), row_tile)
            left = jnp.concatenate([attn[h, p, span, :] for p in range(peers)], axis=1)
            right = jnp.concatenate([rows[p, head_columns(h), :] for p in range(peers)], axis=0)
            term = jnp.dot(left, right, preferred_element_type=F32)
            if h > 0:
                term = term + acc[span, :]
            if h == heads - 1:
                finished[span, :] = term.astype(out_ref.dtype)
                out_copy(r).start()
            else:
                acc[span, :] = term

    def fill_tables():
        for role in range(4):
            role_z = z if role < 2 else end
            role_x = x if role % 2 == 0 else other

            @pl.loop(0, blocks)
            def _(b):
                for s in range(select):
                    chosen = ids_ref[s, (role_z * PAIR + role_x) * blocks + b]
                    owner = lax.div(chosen, blocks)
                    owner_z, owner_x = lax.div(owner, PAIR), lax.rem(owner, PAIR)
                    here = owner_z == z
                    near = owner_z == end
                    source = jnp.where(
                        here, 0, jnp.where(near, 1, jnp.where(owner_z == across, 2, 3))
                    )
                    ours = here | is_mid
                    if role > 1:
                        ours = ours & jnp.logical_not(near)
                    ours = ours & (owner_x == x)
                    entry = (role * blocks + b) * select + s
                    index = source * blocks + lax.rem(chosen, blocks)
                    place[entry] = jnp.where(ours, index, 0)
                    usable[entry] = jnp.where(ours, 1, 0)

    def own_block(h):
        @pl.loop(0, blocks)
        def _(b):
            keys[h][b] = k_ref[b, :, head_columns(h)]
            values[h][b] = v_ref[b, :, head_columns(h)]

    lane = lax.broadcasted_iota(jnp.int32, (TILE, TILE), 1)

    def weigh(h, role, b, query, first_keys):
        entries = [(role * blocks + b) * select + s for s in range(select)]
        keyset = jnp.concatenate(first_keys + [keys[h][place[e]] for e in entries], axis=0)
        scores = lax.dot_general(query, keyset, NT_DIMS, preferred_element_type=F32)
        used = count[role, pl.ds(b, 1), :]
        lead = len(first_keys)
        pieces = [scores[:, i * TILE : (i + 1) * TILE] for i in range(lead + select)]
        for s in range(select):
            keep = jnp.broadcast_to(used * usable[entries[s]], (TILE, TILE)) > s
            pieces[lead + s] = jnp.where(keep, pieces[lead + s], -jnp.inf)
        top = jnp.max(functools.reduce(jnp.maximum, pieces), axis=1, keepdims=True)
        top = jnp.maximum(top, LOWEST)
        probs = [jnp.exp2((piece - top) * exponent) for piece in pieces]
        denom = jnp.sum(functools.reduce(jnp.add, probs), axis=1, keepdims=True)
        for i, piece in enumerate(probs):
            weights[role, b, :, i * TILE : (i + 1) * TILE] = piece.astype(jnp.bfloat16)
        return top * exponent, denom

    def mix(h, role, b, first_values):
        entries = [(role * blocks + b) * select + s for s in range(select)]
        valueset = jnp.concatenate(first_values + [values[h][place[e]] for e in entries], axis=0)
        held = weights[role, b, :, : (len(first_values) + select) * TILE]
        return jnp.dot(held, valueset, preferred_element_type=F32)

    def rows_of(levels):
        tile = jnp.zeros((TILE, TILE), F32)
        for j, (top, denom) in enumerate(levels):
            tile = jnp.where(lane == j, top, tile)
            tile = jnp.where(lane == part_blocks + j, denom, tile)
        return tile.T[: 2 * part_blocks]

    away = is_mid.astype(jnp.int32)

    def over_others(action):
        first = 2 * PARTS

        @pl.loop(first * (1 - away), first + PARTS)
        def _(step):
            late = step // first
            role = late + (1 - late) * (3 - step % 2)
            part = late * (step - first) + (1 - late) * (step // 2)
            action(step, role, part)

    def weigh_others(h):
        def action(step, role, part):
            levels = []
            for j in range(part_blocks):
                b = part * part_blocks + j
                levels.append(weigh(h, role, b, qall[h, role - 1, b], []))
            ssend[h, role - 1, part] = rows_of(levels)

            @pl.when(part == PARTS - 1)
            def _():
                s_copy(h, role - 1).start()

        over_others(action)

    def mix_others(h):
        def action(step, role, part):
            for j in range(part_blocks):
                b = part * part_blocks + j
                span = pl.ds(pl.multiple_of(b * TILE, TILE), TILE)
                osend[h, role - 1, span, :] = mix(h, role, b, []).astype(jnp.bfloat16)
            o_copy(h, part, role - 1).start()

        over_others(action)

    def weigh_own(h):
        @pl.loop(0, PARTS)
        def _(part):
            levels = []
            for j in range(part_blocks):
                b = part * part_blocks + j
                query = q_ref[b, :, head_columns(h)]
                levels.append(weigh(h, 0, b, query, [k_ref[b, :, head_columns(h)]]))
            sself[part] = rows_of(levels)

    def mix_own(h):
        @pl.loop(0, PARTS)
        def _(part):
            for j in range(part_blocks):
                b = part * part_blocks + j
                span = pl.ds(pl.multiple_of(b * TILE, TILE), TILE)
                oself[span, :] = mix(h, 0, b, [v_ref[b, :, head_columns(h)]])

    def merge(h, part, slots):
        levels = [sself[part]] + [srecv[h, slot, part] for slot in range(slots)]
        tops = [level[:part_blocks] for level in levels]
        denoms = [level[part_blocks:] for level in levels]
        top = functools.reduce(jnp.maximum, tops)
        shares = [jnp.exp2(one - top) for one in tops]
        total = functools.reduce(jnp.add, [share * d for share, d in zip(shares, denoms)])
        spare = TILE - part_blocks * len(shares)
        tall = jnp.concatenate(
            [share / total for share in shares] + [jnp.zeros((spare, TILE), F32)], axis=0
        ).T
        for j in range(part_blocks):
            span = pl.ds((part * part_blocks + j) * TILE, TILE)
            value = oself[span, :] * tall[:, j : j + 1]
            for slot in range(slots):
                column = part_blocks * (slot + 1) + j
                value = value + orecv[h, slot, span, :].astype(F32) * tall[:, column : column + 1]
            attn[h, me_p, span, :] = value.astype(jnp.bfloat16)

    def combine(h, part):
        o_copy(h, part, 0).wait_recv()

        @pl.when(is_mid)
        def _():
            merge(h, part, 1)

        @pl.when(is_end)
        def _():
            for slot in (1, 2):
                o_copy(h, part, slot).wait_recv()
            merge(h, part, 3)

    def relay_on(h):
        last = h == heads - 1
        for which in range(2):
            kv_copy(h, 0, which).wait_recv()
            kv_copy(h, 2, which).start()
            if last and h > 0 and which == 0:
                kv_copy(h, 1, 1).start()
        if not last:
            kv_copy(h + 1, 1, 0).start()
            if h + 1 < heads - 1:
                kv_copy(h + 1, 1, 1).start()
        q_copy(h, 1).wait_recv()
        q_copy(h, 2).start()

    def send_early(h):
        @pl.when(is_end)
        def _():
            for which in range(2):
                kv_copy(h, 0, which).start()
            q_copy(h, 1).start()

    def open_column():
        @pl.when(is_mid)
        def _():
            for which in range(2):
                kv_copy(0, 1, which).start()

        for h in range(early):
            send_early(h)

    early = min(EARLY, heads)
    leads = lax.rem(me_p, 2) == 1

    def send_rows(h):
        over_peers(lambda target: w_copy(h, target, me_p).start())

    pl.semaphore_wait(barrier, peers + 2 + away)
    for load in loads:
        load.wait()

    c_copy(0).start()

    @pl.when(is_end)
    def _():
        c_copy(1).start()
        c_copy(2).start()

    @pl.when(leads)
    def _():
        open_column()

    for h in range(early):
        q_copy(h, 0).start()
        send_rows(h)
    fill_tables()
    own_block(0)

    def first_sent(flow):
        for which in range(2):
            kv_copy(0, flow, which).wait_send()

    @pl.when(leads & is_end)
    def _():
        first_sent(0)

    @pl.when(leads & is_mid)
    def _():
        first_sent(1)

    @pl.when(leads)
    def _():
        pl.semaphore_signal(turn_sem, inc=1, device_id=(me_f, twin), device_id_type=MESH)

    @pl.when(jnp.logical_not(leads))
    def _():
        pl.semaphore_wait(turn_sem, 1)
        open_column()

    c_copy(0).wait_recv()

    @pl.when(is_mid)
    def _():
        relay_on(0)
        c_copy(1).wait_recv()
        c_copy(2).wait_recv()

    def all_sent(source, semaphore):
        pltpu.make_async_remote_copy(
            src_ref=source, dst_ref=source, send_sem=semaphore, recv_sem=semaphore,
            device_id=(me_f, twin), device_id_type=MESH,
        ).wait_send()

    def drain_early():
        rest = pl.ds(DH, depth - DH)

        def kv_sent(flow):
            for which in range(2):
                if heads > 1:
                    all_sent(k_ref.at[:, :, rest], kv_send.at[flow, which, 1])

                @pl.when(jnp.logical_not(leads) | (flow == 2))
                def _():
                    all_sent(k_ref.at[:, :, pl.ds(0, DH)], kv_send.at[flow, which, 0])

        c_copy(0).wait_send()
        all_sent(q_ref, q_send.at[0])
        over_peers(lambda target: all_sent(w_ref.at[:, columns_of(target)], w_send.at[target]))

        @pl.when(is_end)
        def _():
            c_copy(1).wait_send()
            c_copy(2).wait_send()
            all_sent(q_ref, q_send.at[1])
            kv_sent(0)

        @pl.when(is_mid)
        def _():
            all_sent(q_ref, q_send.at[2])
            kv_sent(1)
            kv_sent(2)

    def drain_late():
        @pl.loop(0, 1 + 2 * away)
        def _(slot):
            all_sent(ssend.at[:, slot], s_send.at[slot])
            all_sent(osend.at[:, slot], o_send.at[slot])

        over_alike(lambda target: all_sent(attn.at[:, me_p], a_send.at[target]))
        over_twins(lambda origin: all_sent(attn.at[:, me_p], a_send.at[origin]))

    def settle(h):
        if h >= 0:
            finish(h)

    for h in range(heads):
        if h + EARLY < heads:
            q_copy(h + EARLY, 0).start()
            send_early(h + EARLY)
        if h > 0:
            own_block(h)
        last = h == heads - 1

        def catch_up():
            settle(h - 2)
            if h > 0:
                pass_on(h - 1)

        if 0 < h < heads - 1:

            @pl.when(is_mid)
            def _():
                relay_on(h + 1)

        if last:

            @pl.when(jnp.logical_not(leads))
            def _():
                settle(h - 2)

        q_copy(h, 0).wait_recv()

        def arrived(which):
            kv_copy(h, 1, which).wait_recv()
            kv_copy(h, 2, which).wait_recv()

        @pl.when(is_mid)
        def _():
            q_copy(h, 2).wait_recv()
            arrived(0)

        weigh_others(h)
        weigh_own(h)
        if last and h > 0:
            pass_on(h - 1)

        @pl.when(is_mid)
        def _():
            arrived(1)

        mix_others(h)
        mix_own(h)
        if not last:
            if h == 0:

                @pl.when(is_mid)
                def _():
                    relay_on(h + 1)

            catch_up()
        elif h > 0:

            @pl.when(jnp.logical_not(leads))
            def _():
                finish(h - 1)

        s_copy(h, 0).wait_recv()

        @pl.when(is_end)
        def _():
            for slot in (1, 2):
                s_copy(h, slot).wait_recv()

        for part in range(PARTS):
            combine(h, part)
            share(h, part)
        if h + EARLY < heads:
            send_rows(h + EARLY)
    @pl.when(leads)
    def _():
        settle(heads - 3)
        settle(heads - 2)

    drain_early()
    pass_on(heads - 1)
    finish(heads - 1)
    drain_late()
    for r in range(PARTS * part_rows // row_tile):
        out_copy(r).wait()


def column_shards(queries, keys, values, block_ids, counts, w_out):
    frames = lax.axis_size("frames")
    peers = lax.axis_size("heads")
    tokens, width = queries.shape
    blocks = tokens // TILE
    select = block_ids.shape[1]
    heads = width // DH
    features = w_out.shape[1] // peers
    smem = pl.BlockSpec(memory_space=pltpu.SMEM)
    tiles = (blocks, TILE, width)
    dma = pltpu.SemaphoreType.DMA
    bf16 = jnp.bfloat16
    level_rows = (PARTS, 2 * blocks // PARTS, TILE)
    scratch = [pltpu.VMEM(tiles, bf16)] * 3 + [
        pltpu.VMEM((peers, width, features), bf16),
        pltpu.VMEM((heads, peers, tokens, DH), bf16),
        pltpu.VMEM((tokens, features), F32),
        pltpu.VMEM((heads, 3, blocks, TILE, DH), bf16),
        pltpu.VMEM((4, blocks, TILE), jnp.int32),
        pltpu.VMEM((heads, 3, tokens, DH), bf16),
        pltpu.VMEM((heads, 3, tokens, DH), bf16),
        pltpu.VMEM((heads, 3) + level_rows, F32),
        pltpu.VMEM((heads, 3) + level_rows, F32),
        pltpu.VMEM((tokens, DH), F32),
        pltpu.VMEM(level_rows, F32),
        pltpu.VMEM((4, blocks, TILE, (select + 1) * TILE), bf16),
        pltpu.VMEM((tokens, features), bf16),
        pltpu.SMEM((4 * blocks * select,), jnp.int32),
        pltpu.SMEM((4 * blocks * select,), jnp.int32),
        dma((peers,)), dma((heads, peers)), dma((peers,)),
        dma((heads, PARTS, peers)), dma, dma((3,)), pltpu.SemaphoreType.REGULAR,
        dma((tokens // (2 * TILE),)),
        dma((3, 2, 2)), dma((3, heads, 2)), dma((3,)), dma((3, heads)),
        dma((3,)), dma((3,)),
        dma((3,)), dma((heads, PARTS, 3)), dma((3,)), dma((heads, 3)),
    ] + [pltpu.VMEM((4 * blocks, TILE, DH), bf16)] * (2 * heads)
    dims = (frames, peers, blocks, select, heads)
    hbm = pl.BlockSpec(memory_space=pltpu.HBM)
    return pl.pallas_call(
        functools.partial(column_kernel, dims),
        out_shape=jax.ShapeDtypeStruct((tokens, features), bf16),
        in_specs=[smem, smem, hbm, hbm, hbm, hbm],
        out_specs=hbm,
        scratch_shapes=scratch,
        compiler_params=pltpu.CompilerParams(
            collective_id=0, has_side_effects=True, vmem_limit_bytes=VMEM_BYTES
        ),
    )(
        block_ids.T, counts,
        queries.reshape(tiles), keys.reshape(tiles), values.reshape(tiles), w_out,
    )


def solution(mesh):
    placed = (
        P("frames", "heads"),
        P("frames", "heads"),
        P("frames", "heads"),
        P(),
        P("frames"),
        P("heads", None),
    )
    columns = mesh.shape["frames"] == PAIR * LINE and mesh.shape["heads"] % 2 == 0
    return jax.shard_map(
        column_shards if columns else shards, mesh=mesh, in_specs=placed, out_specs=P("frames", "heads"), check_vma=False
    )
```

```python
import functools
import math

import jax
import jax.numpy as jnp
from jax import lax
from jax.experimental import pallas as pl
from jax.experimental.pallas import tpu as pltpu
from jax.sharding import PartitionSpec as P

DH = 128
TILE = 128
MESH = pl.DeviceIdType.MESH
F32 = jnp.float32
PAIR = 2
LINE = 4
PARTS = 2
LAST_PARTS = 4
COPY_TILES = 8
UNROLL = 2
EARLY = 3
LOG2E = math.log2(math.e)
LOWEST = -1e38
VMEM_BYTES = 67043328
NT_DIMS = (((1,), (1,)), ((), ()))


def head_columns(h):
    return slice(h * DH, (h + 1) * DH)


class direct_exchange:
    def __init__(self, dims, pick_ref, k_ref, v_ref, recv, send, kv_send, kv_recv):
        self.frames, _, _, _, self.capacity, self.heads, self.slots = dims
        self.pick_ref, self.k_ref, self.v_ref, self.recv = pick_ref, k_ref, v_ref, recv
        self.send, self.kv_send, self.kv_recv = send, kv_send, kv_recv
        self.me_f, self.me_p = lax.axis_index("frames"), lax.axis_index("heads")

    def copy(self, h, target, origin):
        return pltpu.make_async_remote_copy(
            src_ref=self.send.at[h % self.slots, target],
            dst_ref=self.recv[h].at[pl.ds(origin * self.capacity, self.capacity)],
            send_sem=self.kv_send.at[h, target],
            recv_sem=self.kv_recv.at[h, origin],
            device_id=(target, self.me_p),
            device_id_type=MESH,
        )

    def others(self, action):
        @pl.loop(1, self.frames)
        def _(step):
            action(lax.rem(self.me_f + step, self.frames))

    def pick(self, target, c):
        return self.pick_ref[(target * self.frames + self.me_f) * self.capacity + c]

    def build(self, h):
        if h >= self.slots:
            self.others(lambda target: self.copy(h - self.slots, target, self.me_f).wait_send())

        def fill(target):
            for c in range(self.capacity):
                index = self.pick(target, c)
                self.send[h % self.slots, target, c, 0] = self.k_ref[index, :, head_columns(h)]
                self.send[h % self.slots, target, c, 1] = self.v_ref[index, :, head_columns(h)]

        self.others(fill)
        for c in range(self.capacity):
            index = self.pick(self.me_f, c)
            self.recv[h][self.me_f * self.capacity + c, 0] = self.k_ref[index, :, head_columns(h)]
            self.recv[h][self.me_f * self.capacity + c, 1] = self.v_ref[index, :, head_columns(h)]

    def start(self, h):
        self.others(lambda target: self.copy(h, target, self.me_f).start())

    def prepare(self):
        self.build(0)

    def begin(self):
        self.start(0)

    def follow(self):
        if self.heads > 1:
            self.build(1)
            self.start(1)

    def receive(self, h, midway):
        if h + 2 < self.heads:
            self.build(h + 2)
        midway()
        self.others(lambda origin: self.copy(h, origin, origin).wait_recv())
        if h + 2 < self.heads:
            self.start(h + 2)

    def drain(self):
        for h in range(max(0, self.heads - self.slots), self.heads):
            self.others(lambda target: self.copy(h, target, self.me_f).wait_send())


def layer_kernel(
    dims, pick_ref, slot_ref, count_ref, q_ref, k_ref, v_ref, w_ref, out_ref,
    rows, attn, acc, w_send, w_recv, a_send, a_recv, own_sem, *kv_refs,
):
    frames, peers, blocks, select, capacity, heads, slots = dims
    recv, kv_refs = kv_refs[:heads], kv_refs[heads:]
    me_f, me_p = lax.axis_index("frames"), lax.axis_index("heads")
    depth = heads * DH
    features = rows.shape[2]

    barrier = pltpu.get_barrier_semaphore()

    @pl.loop(1, frames)
    def _(step):
        pl.semaphore_signal(
            barrier, inc=1, device_id=(lax.rem(me_f + step, frames), me_p), device_id_type=MESH
        )

    @pl.loop(1, peers)
    def _(step):
        pl.semaphore_signal(
            barrier, inc=1, device_id=(me_f, lax.rem(me_p + step, peers)), device_id_type=MESH
        )

    def columns_of(peer):
        return pl.ds(pl.multiple_of(peer * features, features), features)

    own_rows = pltpu.make_async_copy(w_ref.at[:, columns_of(me_p)], rows.at[me_p], own_sem)
    own_rows.start()

    exchange = direct_exchange(dims, pick_ref, k_ref, v_ref, recv, *kv_refs)

    def w_copy(target, origin):
        return pltpu.make_async_remote_copy(
            src_ref=w_ref.at[:, columns_of(target)],
            dst_ref=rows.at[origin],
            send_sem=w_send.at[target],
            recv_sem=w_recv.at[origin],
            device_id=(me_f, target),
            device_id_type=MESH,
        )

    part_blocks = blocks // PARTS
    part_rows = part_blocks * TILE

    def a_copy(h, part, target, origin):
        held = attn.at[h, origin, pl.ds(part * part_rows, part_rows)]
        return pltpu.make_async_remote_copy(
            src_ref=held,
            dst_ref=held,
            send_sem=a_send.at[h, part, target, origin],
            recv_sem=a_recv.at[h, part, origin],
            device_id=(me_f, target),
            device_id_type=MESH,
        )

    twin = me_p + 1 - 2 * lax.rem(me_p, 2)

    def over_alike(action):
        @pl.loop(1, peers // 2)
        def _(step):
            action(lax.rem(me_p + 2 * step, peers))

    def over_twins(action):
        @pl.loop(0, peers // 2)
        def _(step):
            action(lax.rem(twin + 2 * step, peers))

    def share(h, part):
        over_alike(lambda target: a_copy(h, part, target, me_p).start())
        a_copy(h, part, twin, me_p).start()

    def finish(h):
        if h == 0:
            own_rows.wait()
            over_peers(lambda origin: w_copy(origin, origin).wait_recv())
        for part in range(PARTS):

            def relay(origin):
                a_copy(h, part, origin, origin).wait_recv()
                a_copy(h, part, twin, origin).start()

            over_alike(relay)
        for part in range(PARTS):
            over_twins(lambda origin: a_copy(h, part, origin, origin).wait_recv())
            project(h, part)

    def drain_attn(h, part):
        over_alike(lambda target: a_copy(h, part, target, me_p).wait_send())
        a_copy(h, part, twin, me_p).wait_send()
        over_alike(lambda origin: a_copy(h, part, twin, origin).wait_send())

    def over_peers(action):
        @pl.loop(1, peers)
        def _(step):
            action(lax.rem(me_p + step, peers))

    def attend(h, part):
        @pl.loop(part * part_blocks, (part + 1) * part_blocks, unroll=UNROLL)
        def _(b):
            q = q_ref[b, :, head_columns(h)]
            picks = [slot_ref[b * select + s] for s in range(select)]
            keyset = jnp.concatenate(
                [k_ref[b, :, head_columns(h)]] + [recv[h][i, 0] for i in picks], axis=0
            )
            valueset = jnp.concatenate(
                [v_ref[b, :, head_columns(h)]] + [recv[h][i, 1] for i in picks], axis=0
            )
            scores = lax.dot_general(q, keyset, NT_DIMS, preferred_element_type=F32)
            scores = scores * (1.0 / DH**0.5)
            position = lax.broadcasted_iota(jnp.int32, scores.shape, 1)
            scores = jnp.where(position < (count_ref[b] + 1) * TILE, scores, -jnp.inf)
            top = jnp.max(scores, axis=1, keepdims=True)
            probs = jnp.exp(scores - top)
            denom = jnp.sum(probs, axis=1, keepdims=True)
            mixed = jnp.dot(probs.astype(jnp.bfloat16), valueset, preferred_element_type=F32)
            attn[h, me_p, pl.ds(pl.multiple_of(b * TILE, TILE), TILE), :] = (mixed / denom).astype(
                jnp.bfloat16
            )

    row_tile = 2 * TILE

    def project(h, part):
        @pl.loop(part * part_rows // row_tile, (part + 1) * part_rows // row_tile)
        def _(r):
            span = pl.ds(pl.multiple_of(r * row_tile, row_tile), row_tile)
            left = jnp.concatenate([attn[h, p, span, :] for p in range(peers)], axis=1)
            right = jnp.concatenate([rows[p, head_columns(h), :] for p in range(peers)], axis=0)
            term = jnp.dot(left, right, preferred_element_type=F32)
            if h > 0:
                term = term + acc[span, :]
            if h == heads - 1:
                out_ref[span, :] = term.astype(out_ref.dtype)
            else:
                acc[span, :] = term

    exchange.prepare()
    pl.semaphore_wait(barrier, frames + peers - 2)
    exchange.begin()
    over_peers(lambda target: w_copy(target, me_p).start())
    exchange.follow()
    for h in range(heads):
        exchange.receive(h, (lambda: finish(h - 1)) if h > 0 else (lambda: None))
        for part in range(PARTS):
            attend(h, part)
            share(h, part)
    finish(heads - 1)
    exchange.drain()
    over_peers(lambda target: w_copy(target, me_p).wait_send())
    for h in range(heads):
        for part in range(PARTS):
            drain_attn(h, part)


def shards(queries, keys, values, block_ids, counts, w_out):
    frames = lax.axis_size("frames")
    peers = lax.axis_size("heads")
    here = lax.axis_index("frames")
    tokens, width = queries.shape
    blocks = tokens // TILE
    select = block_ids.shape[1]
    heads = width // DH
    requests = blocks * select
    capacity = max(2, (requests + frames - 1) // frames)
    features = w_out.shape[1] // peers
    slots = min(3, heads)

    ids = block_ids.reshape(frames, requests)
    owner = ids // blocks
    order = jnp.arange(requests, dtype=jnp.int32)
    same = (owner[:, :, None] == owner[:, None, :]) & (order[:, None] < order[None, :])
    slot = owner * capacity + jnp.sum(same.astype(jnp.int32), axis=1)
    hit = slot[:, None, :] == jnp.arange(frames * capacity, dtype=jnp.int32)[:, None]
    pick = jnp.sum(jnp.where(hit, (ids % blocks)[:, None, :], 0), axis=2).reshape(-1)
    my_slot = lax.dynamic_slice_in_dim(slot, here, 1, 0).reshape(requests)

    smem = pl.BlockSpec(memory_space=pltpu.SMEM)
    vmem = pl.BlockSpec(memory_space=pltpu.VMEM)
    tiles = (blocks, TILE, width)
    dma = pltpu.SemaphoreType.DMA
    bf16 = jnp.bfloat16
    common = [
        pltpu.VMEM((peers, width, features), bf16),
        pltpu.VMEM((heads, peers, tokens, DH), bf16),
        pltpu.VMEM((tokens, features), F32),
    ]
    common_sems = [
        dma((peers,)), dma((peers,)), dma((heads, PARTS, peers, peers)),
        dma((heads, PARTS, peers)), dma,
    ]
    recv = [pltpu.VMEM((frames * capacity, 2, TILE, DH), bf16)] * heads
    extra = [
        pltpu.VMEM((slots, frames, capacity, 2, TILE, DH), bf16),
        dma((heads, frames)),
        dma((heads, frames)),
    ]
    dims = (frames, peers, blocks, select, capacity, heads, slots)
    return pl.pallas_call(
        functools.partial(layer_kernel, dims),
        out_shape=jax.ShapeDtypeStruct((tokens, features), bf16),
        in_specs=[smem, smem, smem, vmem, vmem, vmem, pl.BlockSpec(memory_space=pl.ANY)],
        out_specs=vmem,
        scratch_shapes=common + common_sems + recv + extra,
        compiler_params=pltpu.CompilerParams(
            collective_id=0, has_side_effects=True, vmem_limit_bytes=VMEM_BYTES
        ),
    )(
        pick, my_slot, counts, queries.reshape(tiles), keys.reshape(tiles), values.reshape(tiles),
        w_out,
    )


def column_kernel(
    dims, ids_ref, own_count_ref, q_hbm, k_hbm, v_hbm, w_ref, out_ref,
    q_ref, k_ref, v_ref, rows, attn, acc, qall, count, osend, orecv, ssend, srecv, oself, sself, weights, finished, place, usable,
    w_send, w_recv, a_send, a_recv, own_sem, load_sem, turn_sem, out_sem,
    kv_send, kv_recv, q_send, q_recv, c_send, c_recv, o_send, o_recv, s_send, s_recv, *kv,
):
    frames, peers, blocks, select, heads = dims
    keys, values = kv[:heads], kv[heads:]
    me_f, me_p = lax.axis_index("frames"), lax.axis_index("heads")
    line = frames // PAIR
    z, x = me_f // PAIR, me_f % PAIR
    half = z // (line // 2)
    mid, end = half + 1, (line - 1) * half
    across = line - 1 - mid
    is_mid = z == mid
    is_end = z == end
    other = 1 - x
    depth = heads * DH
    features = rows.shape[2]
    group_blocks = blocks // PARTS
    exponent = LOG2E / DH**0.5

    def at(zz, xx):
        return (zz * PAIR + xx, me_p)

    def parts_of(h):
        return LAST_PARTS if h == heads - 1 else PARTS

    def rows_in(h):
        return blocks // parts_of(h) * TILE

    def rows_span(h, part):
        return pl.ds(part * rows_in(h), rows_in(h))

    loads = [
        pltpu.make_async_copy(source, held, load_sem.at[i])
        for i, (source, held) in enumerate(((k_hbm, k_ref), (v_hbm, v_ref), (q_hbm, q_ref)))
    ]
    for load in loads:
        load.start()
    barrier = pltpu.get_barrier_semaphore()

    def greet(device):
        pl.semaphore_signal(barrier, inc=1, device_id=device, device_id_type=MESH)

    @pl.loop(1, peers)
    def _(step):
        greet((me_f, lax.rem(me_p + step, peers)))

    greet(at(z, other))
    greet(at(mid + end - z, x))
    greet(at(mid + end - z, other))

    @pl.when(is_mid)
    def _():
        greet(at(across, x))

    def columns_of(peer):
        return pl.ds(pl.multiple_of(peer * features, features), features)

    own_rows = pltpu.make_async_copy(w_ref.at[:, columns_of(me_p)], rows.at[me_p], own_sem)
    own_rows.start()

    @pl.loop(0, blocks)
    def _(b):
        count[0, pl.ds(b, 1), :] = jnp.full((1, TILE), own_count_ref[b], jnp.int32)

    def send(source, target, send_sem, recv_sem, device):
        return pltpu.make_async_remote_copy(
            src_ref=source, dst_ref=target, send_sem=send_sem, recv_sem=recv_sem,
            device_id=device, device_id_type=MESH,
        )

    def kv_copy(h, flow, which):
        held = (keys, values)[which][h]
        source = (k_ref, v_ref)[which].at[:, :, head_columns(h)]
        if flow == 2:
            source = held.at[pl.ds(blocks, blocks)]
        return send(
            source, held.at[pl.ds((flow + 1) * blocks, blocks)],
            kv_send.at[flow, which, int(h > 0)], kv_recv.at[flow, h, which],
            at(mid, x) if flow == 0 else at(across, x),
        )

    def q_copy(h, flow):
        source = q_ref.at[:, :, head_columns(h)] if flow < 2 else qall.at[h, 1]
        return send(
            source, qall.at[h, flow], q_send.at[flow], q_recv.at[flow, h],
            at(mid, x) if flow == 1 else at(z, other),
        )

    def c_copy(flow):
        device = (at(z, other), at(mid, x), at(mid, other))[flow]
        return send(
            count.at[0], count.at[flow + 1], c_send.at[flow], c_recv.at[flow], device
        )

    def partial_device(slot):
        to_z = z + (end - z) * ((slot + 1) // 2)
        to_x = x + (other - x) * ((slot + 1) % 2)
        return at(to_z, to_x)

    def o_copy(h, part, slot):
        span = rows_span(h, part)
        return send(
            osend.at[h, slot, span], orecv.at[h, slot, span],
            o_send.at[slot], o_recv.at[h * PARTS + part, slot], partial_device(slot),
        )

    def s_copy(h, slot):
        return send(
            ssend.at[h, slot], srecv.at[h, slot], s_send.at[slot], s_recv.at[h, slot],
            partial_device(slot),
        )

    def w_copy(h, target, origin):
        span = pl.ds(h * DH, DH)
        return send(
            w_ref.at[span, columns_of(target)], rows.at[origin, span],
            w_send.at[target], w_recv.at[h, origin], (me_f, target),
        )

    def a_copy(h, part, target, origin):
        held = attn.at[h, origin, rows_span(h, part)]
        to_twin = lax.rem(target + me_p, 2)
        lane_of = target + to_twin * (origin - me_p)
        return send(
            held, held, a_send.at[lane_of], a_recv.at[h * PARTS + part, origin],
            (me_f, target),
        )

    twin = me_p + 1 - 2 * lax.rem(me_p, 2)

    def over_peers(action):
        @pl.loop(1, peers)
        def _(step):
            action(lax.rem(me_p + step, peers))

    def over_alike(action):
        @pl.loop(1, peers // 2)
        def _(step):
            action(lax.rem(me_p + 2 * step, peers))

    def over_twins(action):
        @pl.loop(0, peers // 2)
        def _(step):
            action(lax.rem(twin + 2 * step, peers))

    def share(h, part):
        over_alike(lambda target: a_copy(h, part, target, me_p).start())
        a_copy(h, part, twin, me_p).start()

    def pass_on(h, part):
        def relay(origin):
            a_copy(h, part, origin, origin).wait_recv()
            a_copy(h, part, twin, origin).start()

        over_alike(relay)

    def finish(h, part):
        if part == 0:
            if h == 0:
                own_rows.wait()
            over_peers(lambda origin: w_copy(h, origin, origin).wait_recv())
        over_twins(lambda origin: a_copy(h, part, origin, origin).wait_recv())
        project(h, part)

    row_tile = 2 * TILE

    def out_copy(r):
        span = pl.ds(pl.multiple_of(r * row_tile, row_tile), row_tile)
        return pltpu.make_async_copy(finished.at[span], out_ref.at[span], out_sem.at[r])

    def project(h, part):
        tiles = rows_in(h) // row_tile

        @pl.loop(part * tiles, (part + 1) * tiles)
        def _(r):
            span = pl.ds(pl.multiple_of(r * row_tile, row_tile), row_tile)
            left = jnp.concatenate([attn[h, p, span, :] for p in range(peers)], axis=1)
            right = jnp.concatenate([rows[p, head_columns(h), :] for p in range(peers)], axis=0)
            term = jnp.dot(left, right, preferred_element_type=F32)
            if h > 0:
                term = term + acc[span, :]
            if h == heads - 1:
                finished[span, :] = term.astype(out_ref.dtype)
                out_copy(r).start()
            else:
                acc[span, :] = term

    def fill_tables():
        for role in range(4):
            role_z = z if role < 2 else end
            role_x = x if role % 2 == 0 else other

            @pl.loop(0, blocks)
            def _(b):
                for s in range(select):
                    chosen = ids_ref[s, (role_z * PAIR + role_x) * blocks + b]
                    owner = lax.div(chosen, blocks)
                    owner_z, owner_x = lax.div(owner, PAIR), lax.rem(owner, PAIR)
                    here = owner_z == z
                    near = owner_z == end
                    source = jnp.where(
                        here, 0, jnp.where(near, 1, jnp.where(owner_z == across, 2, 3))
                    )
                    ours = here | is_mid
                    if role > 1:
                        ours = ours & jnp.logical_not(near)
                    ours = ours & (owner_x == x)
                    entry = (role * blocks + b) * select + s
                    index = source * blocks + lax.rem(chosen, blocks)
                    place[entry] = jnp.where(ours, index, 0)
                    usable[entry] = jnp.where(ours, 1, 0)

    def own_block(h):
        @pl.loop(0, blocks)
        def _(b):
            keys[h][b] = k_ref[b, :, head_columns(h)]
            values[h][b] = v_ref[b, :, head_columns(h)]

    lane = lax.broadcasted_iota(jnp.int32, (TILE, TILE), 1)

    def weigh(h, role, b, query, first_keys):
        entries = [(role * blocks + b) * select + s for s in range(select)]
        keyset = jnp.concatenate(first_keys + [keys[h][place[e]] for e in entries], axis=0)
        scores = lax.dot_general(query, keyset, NT_DIMS, preferred_element_type=F32)
        used = count[role, pl.ds(b, 1), :]
        lead = len(first_keys)
        pieces = [scores[:, i * TILE : (i + 1) * TILE] for i in range(lead + select)]
        for s in range(select):
            keep = jnp.broadcast_to(used * usable[entries[s]], (TILE, TILE)) > s
            pieces[lead + s] = jnp.where(keep, pieces[lead + s], -jnp.inf)
        top = jnp.max(functools.reduce(jnp.maximum, pieces), axis=1, keepdims=True)
        top = jnp.maximum(top, LOWEST)
        probs = [jnp.exp2((piece - top) * exponent) for piece in pieces]
        denom = jnp.sum(functools.reduce(jnp.add, probs), axis=1, keepdims=True)
        for i, piece in enumerate(probs):
            weights[role, b, :, i * TILE : (i + 1) * TILE] = piece.astype(jnp.bfloat16)
        return top * exponent, denom

    def mix(h, role, b, first_values):
        entries = [(role * blocks + b) * select + s for s in range(select)]
        valueset = jnp.concatenate(first_values + [values[h][place[e]] for e in entries], axis=0)
        held = weights[role, b, :, : (len(first_values) + select) * TILE]
        return jnp.dot(held, valueset, preferred_element_type=F32)

    def rows_of(levels):
        tile = jnp.zeros((TILE, TILE), F32)
        for j, (top, denom) in enumerate(levels):
            tile = jnp.where(lane == j, top, tile)
            tile = jnp.where(lane == group_blocks + j, denom, tile)
        return tile.T[: 2 * group_blocks]

    away = is_mid.astype(jnp.int32)

    def over_others(parts, action):
        first = 2 * parts

        @pl.loop(first * (1 - away), first + parts)
        def _(step):
            late = step // first
            role = late + (1 - late) * (3 - step % 2)
            part = late * (step - first) + (1 - late) * (step // 2)
            action(step, role, part)

    def weigh_others(h):
        def action(step, role, part):
            levels = []
            for j in range(group_blocks):
                b = part * group_blocks + j
                levels.append(weigh(h, role, b, qall[h, role - 1, b], []))
            ssend[h, role - 1, part] = rows_of(levels)

            @pl.when(part == PARTS - 1)
            def _():
                s_copy(h, role - 1).start()

        over_others(PARTS, action)

    def mix_others(h):
        part_blocks = blocks // parts_of(h)

        def action(step, role, part):
            for j in range(part_blocks):
                b = part * part_blocks + j
                span = pl.ds(pl.multiple_of(b * TILE, TILE), TILE)
                osend[h, role - 1, span, :] = mix(h, role, b, []).astype(jnp.bfloat16)
            o_copy(h, part, role - 1).start()

        over_others(parts_of(h), action)

    def weigh_own(h):
        @pl.loop(0, PARTS)
        def _(part):
            levels = []
            for j in range(group_blocks):
                b = part * group_blocks + j
                query = q_ref[b, :, head_columns(h)]
                levels.append(weigh(h, 0, b, query, [k_ref[b, :, head_columns(h)]]))
            sself[part] = rows_of(levels)

    def mix_own(h):
        @pl.loop(0, PARTS)
        def _(part):
            for j in range(group_blocks):
                b = part * group_blocks + j
                span = pl.ds(pl.multiple_of(b * TILE, TILE), TILE)
                oself[span, :] = mix(h, 0, b, [v_ref[b, :, head_columns(h)]])

    def merge(h, part, slots):
        part_blocks = blocks // parts_of(h)
        group, first = divmod(part * part_blocks, group_blocks)
        levels = [sself[group]] + [srecv[h, slot, group] for slot in range(slots)]
        tops = [level[:group_blocks] for level in levels]
        denoms = [level[group_blocks:] for level in levels]
        top = functools.reduce(jnp.maximum, tops)
        shares = [jnp.exp2(one - top) for one in tops]
        total = functools.reduce(jnp.add, [share * d for share, d in zip(shares, denoms)])
        spare = TILE - group_blocks * len(shares)
        tall = jnp.concatenate(
            [share / total for share in shares] + [jnp.zeros((spare, TILE), F32)], axis=0
        ).T
        for j in range(part_blocks):
            span = pl.ds((part * part_blocks + j) * TILE, TILE)
            column = first + j
            value = oself[span, :] * tall[:, column : column + 1]
            for slot in range(slots):
                column = group_blocks * (slot + 1) + first + j
                value = value + orecv[h, slot, span, :].astype(F32) * tall[:, column : column + 1]
            attn[h, me_p, span, :] = value.astype(jnp.bfloat16)

    def combine(h, part):
        o_copy(h, part, 0).wait_recv()

        @pl.when(is_mid)
        def _():
            merge(h, part, 1)

        @pl.when(is_end)
        def _():
            for slot in (1, 2):
                o_copy(h, part, slot).wait_recv()
            merge(h, part, 3)

    def relay_on(h):
        last = h == heads - 1
        for which in range(2):
            kv_copy(h, 0, which).wait_recv()
            kv_copy(h, 2, which).start()
            if last and h > 0 and which == 0:
                kv_copy(h, 1, 1).start()
        if not last:
            kv_copy(h + 1, 1, 0).start()
            if h + 1 < heads - 1:
                kv_copy(h + 1, 1, 1).start()
        q_copy(h, 1).wait_recv()
        q_copy(h, 2).start()

    def send_early(h):
        @pl.when(is_end)
        def _():
            for which in range(2):
                kv_copy(h, 0, which).start()
            q_copy(h, 1).start()

    def open_column():
        @pl.when(is_mid)
        def _():
            for which in range(2):
                kv_copy(0, 1, which).start()

        for h in range(early):
            send_early(h)

    early = min(EARLY, heads)
    leads = lax.rem(me_p, 2) == 1

    def send_rows(h):
        over_peers(lambda target: w_copy(h, target, me_p).start())

    pl.semaphore_wait(barrier, peers + 2 + away)
    for load in loads:
        load.wait()

    c_copy(0).start()

    @pl.when(is_end)
    def _():
        c_copy(1).start()
        c_copy(2).start()

    @pl.when(leads)
    def _():
        open_column()

    for h in range(early):
        q_copy(h, 0).start()
        send_rows(h)
    fill_tables()
    own_block(0)

    def first_sent(flow):
        for which in range(2):
            kv_copy(0, flow, which).wait_send()

    @pl.when(leads & is_end)
    def _():
        first_sent(0)

    @pl.when(leads & is_mid)
    def _():
        first_sent(1)

    @pl.when(leads)
    def _():
        pl.semaphore_signal(turn_sem, inc=1, device_id=(me_f, twin), device_id_type=MESH)

    @pl.when(jnp.logical_not(leads))
    def _():
        pl.semaphore_wait(turn_sem, 1)
        open_column()

    c_copy(0).wait_recv()

    @pl.when(is_mid)
    def _():
        relay_on(0)
        c_copy(1).wait_recv()
        c_copy(2).wait_recv()

    def all_sent(source, semaphore):
        pltpu.make_async_remote_copy(
            src_ref=source, dst_ref=source, send_sem=semaphore, recv_sem=semaphore,
            device_id=(me_f, twin), device_id_type=MESH,
        ).wait_send()

    def drain_early():
        rest = pl.ds(DH, depth - DH)

        def kv_sent(flow):
            for which in range(2):
                if heads > 1:
                    all_sent(k_ref.at[:, :, rest], kv_send.at[flow, which, 1])

                @pl.when(jnp.logical_not(leads) | (flow == 2))
                def _():
                    all_sent(k_ref.at[:, :, pl.ds(0, DH)], kv_send.at[flow, which, 0])

        c_copy(0).wait_send()
        all_sent(q_ref, q_send.at[0])
        over_peers(lambda target: all_sent(w_ref.at[:, columns_of(target)], w_send.at[target]))

        @pl.when(is_end)
        def _():
            c_copy(1).wait_send()
            c_copy(2).wait_send()
            all_sent(q_ref, q_send.at[1])
            kv_sent(0)

        @pl.when(is_mid)
        def _():
            all_sent(q_ref, q_send.at[2])
            kv_sent(1)
            kv_sent(2)

    def drain_late():
        @pl.loop(0, 1 + 2 * away)
        def _(slot):
            all_sent(ssend.at[:, slot], s_send.at[slot])
            all_sent(osend.at[:, slot], o_send.at[slot])

        over_alike(lambda target: all_sent(attn.at[:, me_p], a_send.at[target]))
        over_twins(lambda origin: all_sent(attn.at[:, me_p], a_send.at[origin]))

    def settle(h):
        if h >= 0:
            for part in range(parts_of(h)):
                finish(h, part)

    for h in range(heads):
        if h + EARLY < heads:
            q_copy(h + EARLY, 0).start()
            send_early(h + EARLY)
        if h > 0:
            own_block(h)
        last = h == heads - 1

        def catch_up():
            settle(h - 2)
            if h > 0:
                for part in range(parts_of(h - 1)):
                    pass_on(h - 1, part)

        if 0 < h < heads - 1:

            @pl.when(is_mid)
            def _():
                relay_on(h + 1)

        if last:

            @pl.when(jnp.logical_not(leads))
            def _():
                settle(h - 2)

        q_copy(h, 0).wait_recv()

        def arrived(which):
            kv_copy(h, 1, which).wait_recv()
            kv_copy(h, 2, which).wait_recv()

        @pl.when(is_mid)
        def _():
            q_copy(h, 2).wait_recv()
            arrived(0)

        weigh_others(h)
        weigh_own(h)
        if last and h > 0:
            for part in range(parts_of(h - 1)):
                pass_on(h - 1, part)

        @pl.when(is_mid)
        def _():
            arrived(1)

        mix_others(h)
        mix_own(h)
        if not last:
            if h == 0:

                @pl.when(is_mid)
                def _():
                    relay_on(h + 1)

            catch_up()
        elif h > 0:

            @pl.when(jnp.logical_not(leads))
            def _():
                settle(h - 1)

        s_copy(h, 0).wait_recv()

        @pl.when(is_end)
        def _():
            for slot in (1, 2):
                s_copy(h, slot).wait_recv()

        for part in range(parts_of(h)):
            combine(h, part)
            share(h, part)
        if h + EARLY < heads:
            send_rows(h + EARLY)
    @pl.when(leads)
    def _():
        settle(heads - 3)
        settle(heads - 2)

    drain_early()
    for part in range(parts_of(heads - 1)):
        pass_on(heads - 1, part)
        if part > 0:
            finish(heads - 1, part - 1)
    finish(heads - 1, parts_of(heads - 1) - 1)
    drain_late()
    for r in range(blocks * TILE // row_tile):
        out_copy(r).wait()


def place_result(result):
    tokens, features = result.shape
    rows = tokens // COPY_TILES

    def kernel(source, target, held, read_sem, write_sem):
        spans = [pl.ds(i * rows, rows) for i in range(COPY_TILES)]
        reads = [
            pltpu.make_async_copy(source.at[span], held.at[span], read_sem.at[i])
            for i, span in enumerate(spans)
        ]
        writes = [
            pltpu.make_async_copy(held.at[span], target.at[span], write_sem.at[i])
            for i, span in enumerate(spans)
        ]
        for read in reads:
            read.start()
        for read, write in zip(reads, writes):
            read.wait()
            write.start()
        for write in writes:
            write.wait()

    hbm = pl.BlockSpec(memory_space=pltpu.HBM)
    return pl.pallas_call(
        kernel,
        out_shape=jax.ShapeDtypeStruct(result.shape, result.dtype),
        in_specs=[hbm],
        out_specs=hbm,
        scratch_shapes=[
            pltpu.VMEM(result.shape, result.dtype),
            pltpu.SemaphoreType.DMA((COPY_TILES,)),
            pltpu.SemaphoreType.DMA((COPY_TILES,)),
        ],
    )(result)


def column_shards(queries, keys, values, block_ids, counts, w_out):
    frames = lax.axis_size("frames")
    peers = lax.axis_size("heads")
    tokens, width = queries.shape
    blocks = tokens // TILE
    select = block_ids.shape[1]
    heads = width // DH
    features = w_out.shape[1] // peers
    smem = pl.BlockSpec(memory_space=pltpu.SMEM)
    tiles = (blocks, TILE, width)
    dma = pltpu.SemaphoreType.DMA
    bf16 = jnp.bfloat16
    pieces = (heads - 1) * PARTS + LAST_PARTS
    level_rows = (PARTS, 2 * blocks // PARTS, TILE)
    scratch = [pltpu.VMEM(tiles, bf16)] * 3 + [
        pltpu.VMEM((peers, width, features), bf16),
        pltpu.VMEM((heads, peers, tokens, DH), bf16),
        pltpu.VMEM((tokens, features), F32),
        pltpu.VMEM((heads, 3, blocks, TILE, DH), bf16),
        pltpu.VMEM((4, blocks, TILE), jnp.int32),
        pltpu.VMEM((heads, 3, tokens, DH), bf16),
        pltpu.VMEM((heads, 3, tokens, DH), bf16),
        pltpu.VMEM((heads, 3) + level_rows, F32),
        pltpu.VMEM((heads, 3) + level_rows, F32),
        pltpu.VMEM((tokens, DH), F32),
        pltpu.VMEM(level_rows, F32),
        pltpu.VMEM((4, blocks, TILE, (select + 1) * TILE), bf16),
        pltpu.VMEM((tokens, features), bf16),
        pltpu.SMEM((4 * blocks * select,), jnp.int32),
        pltpu.SMEM((4 * blocks * select,), jnp.int32),
        dma((peers,)), dma((heads, peers)), dma((peers,)),
        dma((pieces, peers)), dma, dma((3,)), pltpu.SemaphoreType.REGULAR,
        dma((tokens // (2 * TILE),)),
        dma((3, 2, 2)), dma((3, heads, 2)), dma((3,)), dma((3, heads)),
        dma((3,)), dma((3,)),
        dma((3,)), dma((pieces, 3)), dma((3,)), dma((heads, 3)),
    ] + [pltpu.VMEM((4 * blocks, TILE, DH), bf16)] * (2 * heads)
    dims = (frames, peers, blocks, select, heads)
    hbm = pl.BlockSpec(memory_space=pltpu.HBM)
    result = pl.pallas_call(
        functools.partial(column_kernel, dims),
        out_shape=jax.ShapeDtypeStruct((tokens, features), bf16),
        in_specs=[smem, smem, hbm, hbm, hbm, hbm],
        out_specs=hbm,
        scratch_shapes=scratch,
        compiler_params=pltpu.CompilerParams(
            collective_id=0, has_side_effects=True, vmem_limit_bytes=VMEM_BYTES
        ),
    )(
        block_ids.T, counts,
        queries.reshape(tiles), keys.reshape(tiles), values.reshape(tiles), w_out,
    )
    return place_result(result)


def solution(mesh):
    placed = (
        P("frames", "heads"),
        P("frames", "heads"),
        P("frames", "heads"),
        P(),
        P("frames"),
        P("heads", None),
    )
    columns = mesh.shape["frames"] == PAIR * LINE and mesh.shape["heads"] % 2 == 0
    return jax.shard_map(
        column_shards if columns else shards, mesh=mesh, in_specs=placed, out_specs=P("frames", "heads"), check_vma=False
    )
```

```python
import functools
import math

import jax
import jax.numpy as jnp
from jax import lax
from jax.experimental import pallas as pl
from jax.experimental.pallas import tpu as pltpu
from jax.sharding import PartitionSpec as P

DH = 128
TILE = 128
MESH = pl.DeviceIdType.MESH
F32 = jnp.float32
PAIR = 2
LINE = 4
PARTS = 2
LAST_PARTS = 4
COPY_TILES = 8
UNROLL = 2
EARLY = 3
LOG2E = math.log2(math.e)
LOWEST = -1e38
VMEM_BYTES = 67043328
NT_DIMS = (((1,), (1,)), ((), ()))


def head_columns(h):
    return slice(h * DH, (h + 1) * DH)


class direct_exchange:
    def __init__(self, dims, pick_ref, k_ref, v_ref, recv, send, kv_send, kv_recv):
        self.frames, _, _, _, self.capacity, self.heads, self.slots = dims
        self.pick_ref, self.k_ref, self.v_ref, self.recv = pick_ref, k_ref, v_ref, recv
        self.send, self.kv_send, self.kv_recv = send, kv_send, kv_recv
        self.me_f, self.me_p = lax.axis_index("frames"), lax.axis_index("heads")

    def copy(self, h, target, origin):
        return pltpu.make_async_remote_copy(
            src_ref=self.send.at[h % self.slots, target],
            dst_ref=self.recv[h].at[pl.ds(origin * self.capacity, self.capacity)],
            send_sem=self.kv_send.at[h, target],
            recv_sem=self.kv_recv.at[h, origin],
            device_id=(target, self.me_p),
            device_id_type=MESH,
        )

    def others(self, action):
        @pl.loop(1, self.frames)
        def _(step):
            action(lax.rem(self.me_f + step, self.frames))

    def pick(self, target, c):
        return self.pick_ref[(target * self.frames + self.me_f) * self.capacity + c]

    def build(self, h):
        if h >= self.slots:
            self.others(lambda target: self.copy(h - self.slots, target, self.me_f).wait_send())

        def fill(target):
            for c in range(self.capacity):
                index = self.pick(target, c)
                self.send[h % self.slots, target, c, 0] = self.k_ref[index, :, head_columns(h)]
                self.send[h % self.slots, target, c, 1] = self.v_ref[index, :, head_columns(h)]

        self.others(fill)
        for c in range(self.capacity):
            index = self.pick(self.me_f, c)
            self.recv[h][self.me_f * self.capacity + c, 0] = self.k_ref[index, :, head_columns(h)]
            self.recv[h][self.me_f * self.capacity + c, 1] = self.v_ref[index, :, head_columns(h)]

    def start(self, h):
        self.others(lambda target: self.copy(h, target, self.me_f).start())

    def prepare(self):
        self.build(0)

    def begin(self):
        self.start(0)

    def follow(self):
        if self.heads > 1:
            self.build(1)
            self.start(1)

    def receive(self, h, midway):
        if h + 2 < self.heads:
            self.build(h + 2)
        midway()
        self.others(lambda origin: self.copy(h, origin, origin).wait_recv())
        if h + 2 < self.heads:
            self.start(h + 2)

    def drain(self):
        for h in range(max(0, self.heads - self.slots), self.heads):
            self.others(lambda target: self.copy(h, target, self.me_f).wait_send())


def layer_kernel(
    dims, pick_ref, slot_ref, count_ref, q_ref, k_ref, v_ref, w_ref, out_ref,
    rows, attn, acc, w_send, w_recv, a_send, a_recv, own_sem, *kv_refs,
):
    frames, peers, blocks, select, capacity, heads, slots = dims
    recv, kv_refs = kv_refs[:heads], kv_refs[heads:]
    me_f, me_p = lax.axis_index("frames"), lax.axis_index("heads")
    depth = heads * DH
    features = rows.shape[2]

    barrier = pltpu.get_barrier_semaphore()

    @pl.loop(1, frames)
    def _(step):
        pl.semaphore_signal(
            barrier, inc=1, device_id=(lax.rem(me_f + step, frames), me_p), device_id_type=MESH
        )

    @pl.loop(1, peers)
    def _(step):
        pl.semaphore_signal(
            barrier, inc=1, device_id=(me_f, lax.rem(me_p + step, peers)), device_id_type=MESH
        )

    def columns_of(peer):
        return pl.ds(pl.multiple_of(peer * features, features), features)

    own_rows = pltpu.make_async_copy(w_ref.at[:, columns_of(me_p)], rows.at[me_p], own_sem)
    own_rows.start()

    exchange = direct_exchange(dims, pick_ref, k_ref, v_ref, recv, *kv_refs)

    def w_copy(target, origin):
        return pltpu.make_async_remote_copy(
            src_ref=w_ref.at[:, columns_of(target)],
            dst_ref=rows.at[origin],
            send_sem=w_send.at[target],
            recv_sem=w_recv.at[origin],
            device_id=(me_f, target),
            device_id_type=MESH,
        )

    part_blocks = blocks // PARTS
    part_rows = part_blocks * TILE

    def a_copy(h, part, target, origin):
        held = attn.at[h, origin, pl.ds(part * part_rows, part_rows)]
        return pltpu.make_async_remote_copy(
            src_ref=held,
            dst_ref=held,
            send_sem=a_send.at[h, part, target, origin],
            recv_sem=a_recv.at[h, part, origin],
            device_id=(me_f, target),
            device_id_type=MESH,
        )

    twin = me_p + 1 - 2 * lax.rem(me_p, 2)

    def over_alike(action):
        @pl.loop(1, peers // 2)
        def _(step):
            action(lax.rem(me_p + 2 * step, peers))

    def over_twins(action):
        @pl.loop(0, peers // 2)
        def _(step):
            action(lax.rem(twin + 2 * step, peers))

    def share(h, part):
        over_alike(lambda target: a_copy(h, part, target, me_p).start())
        a_copy(h, part, twin, me_p).start()

    def finish(h):
        if h == 0:
            own_rows.wait()
            over_peers(lambda origin: w_copy(origin, origin).wait_recv())
        for part in range(PARTS):

            def relay(origin):
                a_copy(h, part, origin, origin).wait_recv()
                a_copy(h, part, twin, origin).start()

            over_alike(relay)
        for part in range(PARTS):
            over_twins(lambda origin: a_copy(h, part, origin, origin).wait_recv())
            project(h, part)

    def drain_attn(h, part):
        over_alike(lambda target: a_copy(h, part, target, me_p).wait_send())
        a_copy(h, part, twin, me_p).wait_send()
        over_alike(lambda origin: a_copy(h, part, twin, origin).wait_send())

    def over_peers(action):
        @pl.loop(1, peers)
        def _(step):
            action(lax.rem(me_p + step, peers))

    def attend(h, part):
        @pl.loop(part * part_blocks, (part + 1) * part_blocks, unroll=UNROLL)
        def _(b):
            q = q_ref[b, :, head_columns(h)]
            picks = [slot_ref[b * select + s] for s in range(select)]
            keyset = jnp.concatenate(
                [k_ref[b, :, head_columns(h)]] + [recv[h][i, 0] for i in picks], axis=0
            )
            valueset = jnp.concatenate(
                [v_ref[b, :, head_columns(h)]] + [recv[h][i, 1] for i in picks], axis=0
            )
            scores = lax.dot_general(q, keyset, NT_DIMS, preferred_element_type=F32)
            scores = scores * (1.0 / DH**0.5)
            position = lax.broadcasted_iota(jnp.int32, scores.shape, 1)
            scores = jnp.where(position < (count_ref[b] + 1) * TILE, scores, -jnp.inf)
            top = jnp.max(scores, axis=1, keepdims=True)
            probs = jnp.exp(scores - top)
            denom = jnp.sum(probs, axis=1, keepdims=True)
            mixed = jnp.dot(probs.astype(jnp.bfloat16), valueset, preferred_element_type=F32)
            attn[h, me_p, pl.ds(pl.multiple_of(b * TILE, TILE), TILE), :] = (mixed / denom).astype(
                jnp.bfloat16
            )

    row_tile = 2 * TILE

    def project(h, part):
        @pl.loop(part * part_rows // row_tile, (part + 1) * part_rows // row_tile)
        def _(r):
            span = pl.ds(pl.multiple_of(r * row_tile, row_tile), row_tile)
            left = jnp.concatenate([attn[h, p, span, :] for p in range(peers)], axis=1)
            right = jnp.concatenate([rows[p, head_columns(h), :] for p in range(peers)], axis=0)
            term = jnp.dot(left, right, preferred_element_type=F32)
            if h > 0:
                term = term + acc[span, :]
            if h == heads - 1:
                out_ref[span, :] = term.astype(out_ref.dtype)
            else:
                acc[span, :] = term

    exchange.prepare()
    pl.semaphore_wait(barrier, frames + peers - 2)
    exchange.begin()
    over_peers(lambda target: w_copy(target, me_p).start())
    exchange.follow()
    for h in range(heads):
        exchange.receive(h, (lambda: finish(h - 1)) if h > 0 else (lambda: None))
        for part in range(PARTS):
            attend(h, part)
            share(h, part)
    finish(heads - 1)
    exchange.drain()
    over_peers(lambda target: w_copy(target, me_p).wait_send())
    for h in range(heads):
        for part in range(PARTS):
            drain_attn(h, part)


def shards(queries, keys, values, block_ids, counts, w_out):
    frames = lax.axis_size("frames")
    peers = lax.axis_size("heads")
    here = lax.axis_index("frames")
    tokens, width = queries.shape
    blocks = tokens // TILE
    select = block_ids.shape[1]
    heads = width // DH
    requests = blocks * select
    capacity = max(2, (requests + frames - 1) // frames)
    features = w_out.shape[1] // peers
    slots = min(3, heads)

    ids = block_ids.reshape(frames, requests)
    owner = ids // blocks
    order = jnp.arange(requests, dtype=jnp.int32)
    same = (owner[:, :, None] == owner[:, None, :]) & (order[:, None] < order[None, :])
    slot = owner * capacity + jnp.sum(same.astype(jnp.int32), axis=1)
    hit = slot[:, None, :] == jnp.arange(frames * capacity, dtype=jnp.int32)[:, None]
    pick = jnp.sum(jnp.where(hit, (ids % blocks)[:, None, :], 0), axis=2).reshape(-1)
    my_slot = lax.dynamic_slice_in_dim(slot, here, 1, 0).reshape(requests)

    smem = pl.BlockSpec(memory_space=pltpu.SMEM)
    vmem = pl.BlockSpec(memory_space=pltpu.VMEM)
    tiles = (blocks, TILE, width)
    dma = pltpu.SemaphoreType.DMA
    bf16 = jnp.bfloat16
    common = [
        pltpu.VMEM((peers, width, features), bf16),
        pltpu.VMEM((heads, peers, tokens, DH), bf16),
        pltpu.VMEM((tokens, features), F32),
    ]
    common_sems = [
        dma((peers,)), dma((peers,)), dma((heads, PARTS, peers, peers)),
        dma((heads, PARTS, peers)), dma,
    ]
    recv = [pltpu.VMEM((frames * capacity, 2, TILE, DH), bf16)] * heads
    extra = [
        pltpu.VMEM((slots, frames, capacity, 2, TILE, DH), bf16),
        dma((heads, frames)),
        dma((heads, frames)),
    ]
    dims = (frames, peers, blocks, select, capacity, heads, slots)
    return pl.pallas_call(
        functools.partial(layer_kernel, dims),
        out_shape=jax.ShapeDtypeStruct((tokens, features), bf16),
        in_specs=[smem, smem, smem, vmem, vmem, vmem, pl.BlockSpec(memory_space=pl.ANY)],
        out_specs=vmem,
        scratch_shapes=common + common_sems + recv + extra,
        compiler_params=pltpu.CompilerParams(
            collective_id=0, has_side_effects=True, vmem_limit_bytes=VMEM_BYTES
        ),
    )(
        pick, my_slot, counts, queries.reshape(tiles), keys.reshape(tiles), values.reshape(tiles),
        w_out,
    )


def column_kernel(
    dims, ids_ref, own_count_ref, q_hbm, k_hbm, v_hbm, w_ref, out_ref,
    q_ref, k_ref, v_ref, rows, attn, acc, qall, count, osend, orecv, ssend, srecv, oself, sself, weights, finished, place, usable,
    w_send, w_recv, a_send, a_recv, own_sem, load_sem, turn_sem, out_sem,
    kv_send, kv_recv, q_send, q_recv, c_send, c_recv, o_send, o_recv, s_send, s_recv, *kv,
):
    frames, peers, blocks, select, heads = dims
    keys, values = kv[:heads], kv[heads:]
    me_f, me_p = lax.axis_index("frames"), lax.axis_index("heads")
    line = frames // PAIR
    z, x = me_f // PAIR, me_f % PAIR
    half = z // (line // 2)
    mid, end = half + 1, (line - 1) * half
    across = line - 1 - mid
    is_mid = z == mid
    is_end = z == end
    other = 1 - x
    depth = heads * DH
    features = rows.shape[2]
    group_blocks = blocks // PARTS
    exponent = LOG2E / DH**0.5

    def at(zz, xx):
        return (zz * PAIR + xx, me_p)

    def parts_of(h):
        return LAST_PARTS if h == heads - 1 else PARTS

    def rows_in(h):
        return blocks // parts_of(h) * TILE

    def rows_span(h, part):
        return pl.ds(part * rows_in(h), rows_in(h))

    loads = [
        pltpu.make_async_copy(source, held, load_sem.at[i])
        for i, (source, held) in enumerate(((k_hbm, k_ref), (v_hbm, v_ref), (q_hbm, q_ref)))
    ]
    for load in loads:
        load.start()
    barrier = pltpu.get_barrier_semaphore()

    def greet(device):
        pl.semaphore_signal(barrier, inc=1, device_id=device, device_id_type=MESH)

    @pl.loop(1, peers)
    def _(step):
        greet((me_f, lax.rem(me_p + step, peers)))

    greet(at(z, other))
    greet(at(mid + end - z, x))
    greet(at(mid + end - z, other))

    @pl.when(is_mid)
    def _():
        greet(at(across, x))

    def columns_of(peer):
        return pl.ds(pl.multiple_of(peer * features, features), features)

    own_rows = pltpu.make_async_copy(w_ref.at[:, columns_of(me_p)], rows.at[me_p], own_sem)
    own_rows.start()

    @pl.loop(0, blocks)
    def _(b):
        count[0, pl.ds(b, 1), :] = jnp.full((1, TILE), own_count_ref[b], jnp.int32)

    def send(source, target, send_sem, recv_sem, device):
        return pltpu.make_async_remote_copy(
            src_ref=source, dst_ref=target, send_sem=send_sem, recv_sem=recv_sem,
            device_id=device, device_id_type=MESH,
        )

    def kv_copy(h, flow, which):
        held = (keys, values)[which][h]
        source = (k_ref, v_ref)[which].at[:, :, head_columns(h)]
        if flow == 2:
            source = held.at[pl.ds(blocks, blocks)]
        return send(
            source, held.at[pl.ds((flow + 1) * blocks, blocks)],
            kv_send.at[flow, which, int(h > 0)], kv_recv.at[flow, h, which],
            at(mid, x) if flow == 0 else at(across, x),
        )

    def q_copy(h, flow):
        source = q_ref.at[:, :, head_columns(h)] if flow < 2 else qall.at[h, 1]
        return send(
            source, qall.at[h, flow], q_send.at[flow], q_recv.at[flow, h],
            at(mid, x) if flow == 1 else at(z, other),
        )

    def c_copy(flow):
        device = (at(z, other), at(mid, x), at(mid, other))[flow]
        return send(
            count.at[0], count.at[flow + 1], c_send.at[flow], c_recv.at[flow], device
        )

    def partial_device(slot):
        to_z = z + (end - z) * ((slot + 1) // 2)
        to_x = x + (other - x) * ((slot + 1) % 2)
        return at(to_z, to_x)

    def o_copy(h, part, slot):
        span = rows_span(h, part)
        return send(
            osend.at[h, slot, span], orecv.at[h, slot, span],
            o_send.at[slot], o_recv.at[h * PARTS + part, slot], partial_device(slot),
        )

    def s_copy(h, slot):
        return send(
            ssend.at[h, slot], srecv.at[h, slot], s_send.at[slot], s_recv.at[h, slot],
            partial_device(slot),
        )

    def w_copy(h, target, origin):
        span = pl.ds(h * DH, DH)
        return send(
            w_ref.at[span, columns_of(target)], rows.at[origin, span],
            w_send.at[target], w_recv.at[h, origin], (me_f, target),
        )

    def a_copy(h, part, target, origin):
        held = attn.at[h, origin, rows_span(h, part)]
        to_twin = lax.rem(target + me_p, 2)
        lane_of = target + to_twin * (origin - me_p)
        return send(
            held, held, a_send.at[lane_of], a_recv.at[h * PARTS + part, origin],
            (me_f, target),
        )

    twin = me_p + 1 - 2 * lax.rem(me_p, 2)

    def over_peers(action):
        @pl.loop(1, peers)
        def _(step):
            action(lax.rem(me_p + step, peers))

    def over_alike(action):
        @pl.loop(1, peers // 2)
        def _(step):
            action(lax.rem(me_p + 2 * step, peers))

    def over_twins(action):
        @pl.loop(0, peers // 2)
        def _(step):
            action(lax.rem(twin + 2 * step, peers))

    def direct(h, part):
        return h == heads - 1 and part >= parts_of(h) // 2

    def share(h, part):
        over_alike(lambda target: a_copy(h, part, target, me_p).start())
        if direct(h, part):
            over_twins(lambda target: a_copy(h, part, target, me_p).start())
        else:
            a_copy(h, part, twin, me_p).start()

    def pass_on(h, part):
        def relay(origin):
            a_copy(h, part, origin, origin).wait_recv()
            a_copy(h, part, twin, origin).start()

        over_alike(relay)

    def finish(h, part):
        if part == 0:
            if h == 0:
                own_rows.wait()
            over_peers(lambda origin: w_copy(h, origin, origin).wait_recv())
        if direct(h, part):
            over_alike(lambda origin: a_copy(h, part, origin, origin).wait_recv())
        over_twins(lambda origin: a_copy(h, part, origin, origin).wait_recv())
        project(h, part)

    row_tile = 2 * TILE

    def out_copy(r):
        span = pl.ds(pl.multiple_of(r * row_tile, row_tile), row_tile)
        return pltpu.make_async_copy(finished.at[span], out_ref.at[span], out_sem.at[r])

    def project(h, part):
        tiles = rows_in(h) // row_tile

        @pl.loop(part * tiles, (part + 1) * tiles)
        def _(r):
            span = pl.ds(pl.multiple_of(r * row_tile, row_tile), row_tile)
            left = jnp.concatenate([attn[h, p, span, :] for p in range(peers)], axis=1)
            right = jnp.concatenate([rows[p, head_columns(h), :] for p in range(peers)], axis=0)
            term = jnp.dot(left, right, preferred_element_type=F32)
            if h > 0:
                term = term + acc[span, :]
            if h == heads - 1:
                finished[span, :] = term.astype(out_ref.dtype)
                out_copy(r).start()
            else:
                acc[span, :] = term

    def fill_tables():
        for role in range(4):
            role_z = z if role < 2 else end
            role_x = x if role % 2 == 0 else other

            @pl.loop(0, blocks)
            def _(b):
                for s in range(select):
                    chosen = ids_ref[s, (role_z * PAIR + role_x) * blocks + b]
                    owner = lax.div(chosen, blocks)
                    owner_z, owner_x = lax.div(owner, PAIR), lax.rem(owner, PAIR)
                    here = owner_z == z
                    near = owner_z == end
                    source = jnp.where(
                        here, 0, jnp.where(near, 1, jnp.where(owner_z == across, 2, 3))
                    )
                    ours = here | is_mid
                    if role > 1:
                        ours = ours & jnp.logical_not(near)
                    ours = ours & (owner_x == x)
                    entry = (role * blocks + b) * select + s
                    index = source * blocks + lax.rem(chosen, blocks)
                    place[entry] = jnp.where(ours, index, 0)
                    usable[entry] = jnp.where(ours, 1, 0)

    def own_block(h):
        @pl.loop(0, blocks)
        def _(b):
            keys[h][b] = k_ref[b, :, head_columns(h)]
            values[h][b] = v_ref[b, :, head_columns(h)]

    lane = lax.broadcasted_iota(jnp.int32, (TILE, TILE), 1)

    def weigh(h, role, b, query, first_keys):
        entries = [(role * blocks + b) * select + s for s in range(select)]
        keyset = jnp.concatenate(first_keys + [keys[h][place[e]] for e in entries], axis=0)
        scores = lax.dot_general(query, keyset, NT_DIMS, preferred_element_type=F32)
        used = count[role, pl.ds(b, 1), :]
        lead = len(first_keys)
        pieces = [scores[:, i * TILE : (i + 1) * TILE] for i in range(lead + select)]
        for s in range(select):
            keep = jnp.broadcast_to(used * usable[entries[s]], (TILE, TILE)) > s
            pieces[lead + s] = jnp.where(keep, pieces[lead + s], -jnp.inf)
        top = jnp.max(functools.reduce(jnp.maximum, pieces), axis=1, keepdims=True)
        top = jnp.maximum(top, LOWEST)
        probs = [jnp.exp2((piece - top) * exponent) for piece in pieces]
        denom = jnp.sum(functools.reduce(jnp.add, probs), axis=1, keepdims=True)
        for i, piece in enumerate(probs):
            weights[role, b, :, i * TILE : (i + 1) * TILE] = piece.astype(jnp.bfloat16)
        return top * exponent, denom

    def mix(h, role, b, first_values):
        entries = [(role * blocks + b) * select + s for s in range(select)]
        valueset = jnp.concatenate(first_values + [values[h][place[e]] for e in entries], axis=0)
        held = weights[role, b, :, : (len(first_values) + select) * TILE]
        return jnp.dot(held, valueset, preferred_element_type=F32)

    def rows_of(levels):
        tile = jnp.zeros((TILE, TILE), F32)
        for j, (top, denom) in enumerate(levels):
            tile = jnp.where(lane == j, top, tile)
            tile = jnp.where(lane == group_blocks + j, denom, tile)
        return tile.T[: 2 * group_blocks]

    away = is_mid.astype(jnp.int32)

    def over_others(parts, action):
        first = 2 * parts

        @pl.loop(first * (1 - away), first + parts)
        def _(step):
            late = step // first
            role = late + (1 - late) * (3 - step % 2)
            part = late * (step - first) + (1 - late) * (step // 2)
            action(step, role, part)

    def weigh_others(h):
        def action(step, role, part):
            levels = []
            for j in range(group_blocks):
                b = part * group_blocks + j
                levels.append(weigh(h, role, b, qall[h, role - 1, b], []))
            ssend[h, role - 1, part] = rows_of(levels)

            @pl.when(part == PARTS - 1)
            def _():
                s_copy(h, role - 1).start()

        over_others(PARTS, action)

    def mix_others(h):
        part_blocks = blocks // parts_of(h)

        def action(step, role, part):
            for j in range(part_blocks):
                b = part * part_blocks + j
                span = pl.ds(pl.multiple_of(b * TILE, TILE), TILE)
                osend[h, role - 1, span, :] = mix(h, role, b, []).astype(jnp.bfloat16)
            o_copy(h, part, role - 1).start()

        over_others(parts_of(h), action)

    def weigh_own(h):
        @pl.loop(0, PARTS)
        def _(part):
            levels = []
            for j in range(group_blocks):
                b = part * group_blocks + j
                query = q_ref[b, :, head_columns(h)]
                levels.append(weigh(h, 0, b, query, [k_ref[b, :, head_columns(h)]]))
            sself[part] = rows_of(levels)

    def mix_own(h):
        @pl.loop(0, PARTS)
        def _(part):
            for j in range(group_blocks):
                b = part * group_blocks + j
                span = pl.ds(pl.multiple_of(b * TILE, TILE), TILE)
                oself[span, :] = mix(h, 0, b, [v_ref[b, :, head_columns(h)]])

    def merge(h, part, slots):
        part_blocks = blocks // parts_of(h)
        group, first = divmod(part * part_blocks, group_blocks)
        levels = [sself[group]] + [srecv[h, slot, group] for slot in range(slots)]
        tops = [level[:group_blocks] for level in levels]
        denoms = [level[group_blocks:] for level in levels]
        top = functools.reduce(jnp.maximum, tops)
        shares = [jnp.exp2(one - top) for one in tops]
        total = functools.reduce(jnp.add, [share * d for share, d in zip(shares, denoms)])
        spare = TILE - group_blocks * len(shares)
        tall = jnp.concatenate(
            [share / total for share in shares] + [jnp.zeros((spare, TILE), F32)], axis=0
        ).T
        for j in range(part_blocks):
            span = pl.ds((part * part_blocks + j) * TILE, TILE)
            column = first + j
            value = oself[span, :] * tall[:, column : column + 1]
            for slot in range(slots):
                column = group_blocks * (slot + 1) + first + j
                value = value + orecv[h, slot, span, :].astype(F32) * tall[:, column : column + 1]
            attn[h, me_p, span, :] = value.astype(jnp.bfloat16)

    def combine(h, part):
        o_copy(h, part, 0).wait_recv()

        @pl.when(is_mid)
        def _():
            merge(h, part, 1)

        @pl.when(is_end)
        def _():
            for slot in (1, 2):
                o_copy(h, part, slot).wait_recv()
            merge(h, part, 3)

    def relay_on(h):
        last = h == heads - 1
        for which in range(2):
            kv_copy(h, 0, which).wait_recv()
            kv_copy(h, 2, which).start()
            if last and h > 0 and which == 0:
                kv_copy(h, 1, 1).start()
        if not last:
            kv_copy(h + 1, 1, 0).start()
            if h + 1 < heads - 1:
                kv_copy(h + 1, 1, 1).start()
        q_copy(h, 1).wait_recv()
        q_copy(h, 2).start()

    def send_early(h):
        @pl.when(is_end)
        def _():
            for which in range(2):
                kv_copy(h, 0, which).start()
            q_copy(h, 1).start()

    def open_column():
        @pl.when(is_mid)
        def _():
            for which in range(2):
                kv_copy(0, 1, which).start()

        for h in range(early):
            send_early(h)

    early = min(EARLY, heads)
    leads = lax.rem(me_p, 2) == 1

    def send_rows(h):
        over_peers(lambda target: w_copy(h, target, me_p).start())

    pl.semaphore_wait(barrier, peers + 2 + away)
    for load in loads:
        load.wait()

    c_copy(0).start()

    @pl.when(is_end)
    def _():
        c_copy(1).start()
        c_copy(2).start()

    @pl.when(leads)
    def _():
        open_column()

    for h in range(early):
        q_copy(h, 0).start()
        send_rows(h)
    fill_tables()
    own_block(0)

    def first_sent(flow):
        for which in range(2):
            kv_copy(0, flow, which).wait_send()

    @pl.when(leads & is_end)
    def _():
        first_sent(0)

    @pl.when(leads & is_mid)
    def _():
        first_sent(1)

    @pl.when(leads)
    def _():
        pl.semaphore_signal(turn_sem, inc=1, device_id=(me_f, twin), device_id_type=MESH)

    @pl.when(jnp.logical_not(leads))
    def _():
        pl.semaphore_wait(turn_sem, 1)
        open_column()

    c_copy(0).wait_recv()

    @pl.when(is_mid)
    def _():
        relay_on(0)
        c_copy(1).wait_recv()
        c_copy(2).wait_recv()

    def all_sent(source, semaphore):
        pltpu.make_async_remote_copy(
            src_ref=source, dst_ref=source, send_sem=semaphore, recv_sem=semaphore,
            device_id=(me_f, twin), device_id_type=MESH,
        ).wait_send()

    def drain_early():
        rest = pl.ds(DH, depth - DH)

        def kv_sent(flow):
            for which in range(2):
                if heads > 1:
                    all_sent(k_ref.at[:, :, rest], kv_send.at[flow, which, 1])

                @pl.when(jnp.logical_not(leads) | (flow == 2))
                def _():
                    all_sent(k_ref.at[:, :, pl.ds(0, DH)], kv_send.at[flow, which, 0])

        c_copy(0).wait_send()
        all_sent(q_ref, q_send.at[0])
        over_peers(lambda target: all_sent(w_ref.at[:, columns_of(target)], w_send.at[target]))

        @pl.when(is_end)
        def _():
            c_copy(1).wait_send()
            c_copy(2).wait_send()
            all_sent(q_ref, q_send.at[1])
            kv_sent(0)

        @pl.when(is_mid)
        def _():
            all_sent(q_ref, q_send.at[2])
            kv_sent(1)
            kv_sent(2)

    def drain_late():
        @pl.loop(0, 1 + 2 * away)
        def _(slot):
            all_sent(ssend.at[:, slot], s_send.at[slot])
            all_sent(osend.at[:, slot], o_send.at[slot])

        over_alike(lambda target: all_sent(attn.at[:, me_p], a_send.at[target]))
        over_twins(lambda origin: all_sent(attn.at[:, me_p], a_send.at[origin]))

    def settle(h):
        if h >= 0:
            for part in range(parts_of(h)):
                finish(h, part)

    for h in range(heads):
        if h + EARLY < heads:
            q_copy(h + EARLY, 0).start()
            send_early(h + EARLY)
        if h > 0:
            own_block(h)
        last = h == heads - 1

        def catch_up():
            settle(h - 2)
            if h > 0:
                for part in range(parts_of(h - 1)):
                    pass_on(h - 1, part)

        if 0 < h < heads - 1:

            @pl.when(is_mid)
            def _():
                relay_on(h + 1)

        if last:

            @pl.when(jnp.logical_not(leads))
            def _():
                settle(h - 2)

        q_copy(h, 0).wait_recv()

        def arrived(which):
            kv_copy(h, 1, which).wait_recv()
            kv_copy(h, 2, which).wait_recv()

        @pl.when(is_mid)
        def _():
            q_copy(h, 2).wait_recv()
            arrived(0)

        weigh_others(h)
        weigh_own(h)
        if last and h > 0:
            for part in range(parts_of(h - 1)):
                pass_on(h - 1, part)

        @pl.when(is_mid)
        def _():
            arrived(1)

        mix_others(h)
        mix_own(h)
        if not last:
            if h == 0:

                @pl.when(is_mid)
                def _():
                    relay_on(h + 1)

            catch_up()
        elif h > 0:

            @pl.when(jnp.logical_not(leads))
            def _():
                settle(h - 1)

        s_copy(h, 0).wait_recv()

        @pl.when(is_end)
        def _():
            for slot in (1, 2):
                s_copy(h, slot).wait_recv()

        for part in range(parts_of(h)):
            combine(h, part)
            share(h, part)
        if h + EARLY < heads:
            send_rows(h + EARLY)
    @pl.when(leads)
    def _():
        settle(heads - 3)
        settle(heads - 2)

    drain_early()
    for part in range(parts_of(heads - 1)):
        if not direct(heads - 1, part):
            pass_on(heads - 1, part)
    for part in range(parts_of(heads - 1)):
        finish(heads - 1, part)
    drain_late()
    for r in range(blocks * TILE // row_tile):
        out_copy(r).wait()


def place_result(result):
    tokens, features = result.shape
    rows = tokens // COPY_TILES

    def kernel(source, target, held, read_sem, write_sem):
        spans = [pl.ds(i * rows, rows) for i in range(COPY_TILES)]
        reads = [
            pltpu.make_async_copy(source.at[span], held.at[span], read_sem.at[i])
            for i, span in enumerate(spans)
        ]
        writes = [
            pltpu.make_async_copy(held.at[span], target.at[span], write_sem.at[i])
            for i, span in enumerate(spans)
        ]
        for read in reads:
            read.start()
        for read, write in zip(reads, writes):
            read.wait()
            write.start()
        for write in writes:
            write.wait()

    hbm = pl.BlockSpec(memory_space=pltpu.HBM)
    return pl.pallas_call(
        kernel,
        out_shape=jax.ShapeDtypeStruct(result.shape, result.dtype),
        in_specs=[hbm],
        out_specs=hbm,
        scratch_shapes=[
            pltpu.VMEM(result.shape, result.dtype),
            pltpu.SemaphoreType.DMA((COPY_TILES,)),
            pltpu.SemaphoreType.DMA((COPY_TILES,)),
        ],
    )(result)


def column_shards(queries, keys, values, block_ids, counts, w_out):
    frames = lax.axis_size("frames")
    peers = lax.axis_size("heads")
    tokens, width = queries.shape
    blocks = tokens // TILE
    select = block_ids.shape[1]
    heads = width // DH
    features = w_out.shape[1] // peers
    smem = pl.BlockSpec(memory_space=pltpu.SMEM)
    tiles = (blocks, TILE, width)
    dma = pltpu.SemaphoreType.DMA
    bf16 = jnp.bfloat16
    pieces = (heads - 1) * PARTS + LAST_PARTS
    level_rows = (PARTS, 2 * blocks // PARTS, TILE)
    scratch = [pltpu.VMEM(tiles, bf16)] * 3 + [
        pltpu.VMEM((peers, width, features), bf16),
        pltpu.VMEM((heads, peers, tokens, DH), bf16),
        pltpu.VMEM((tokens, features), F32),
        pltpu.VMEM((heads, 3, blocks, TILE, DH), bf16),
        pltpu.VMEM((4, blocks, TILE), jnp.int32),
        pltpu.VMEM((heads, 3, tokens, DH), bf16),
        pltpu.VMEM((heads, 3, tokens, DH), bf16),
        pltpu.VMEM((heads, 3) + level_rows, F32),
        pltpu.VMEM((heads, 3) + level_rows, F32),
        pltpu.VMEM((tokens, DH), F32),
        pltpu.VMEM(level_rows, F32),
        pltpu.VMEM((4, blocks, TILE, (select + 1) * TILE), bf16),
        pltpu.VMEM((tokens, features), bf16),
        pltpu.SMEM((4 * blocks * select,), jnp.int32),
        pltpu.SMEM((4 * blocks * select,), jnp.int32),
        dma((peers,)), dma((heads, peers)), dma((peers,)),
        dma((pieces, peers)), dma, dma((3,)), pltpu.SemaphoreType.REGULAR,
        dma((tokens // (2 * TILE),)),
        dma((3, 2, 2)), dma((3, heads, 2)), dma((3,)), dma((3, heads)),
        dma((3,)), dma((3,)),
        dma((3,)), dma((pieces, 3)), dma((3,)), dma((heads, 3)),
    ] + [pltpu.VMEM((4 * blocks, TILE, DH), bf16)] * (2 * heads)
    dims = (frames, peers, blocks, select, heads)
    hbm = pl.BlockSpec(memory_space=pltpu.HBM)
    result = pl.pallas_call(
        functools.partial(column_kernel, dims),
        out_shape=jax.ShapeDtypeStruct((tokens, features), bf16),
        in_specs=[smem, smem, hbm, hbm, hbm, hbm],
        out_specs=hbm,
        scratch_shapes=scratch,
        compiler_params=pltpu.CompilerParams(
            collective_id=0, has_side_effects=True, vmem_limit_bytes=VMEM_BYTES
        ),
    )(
        block_ids.T, counts,
        queries.reshape(tiles), keys.reshape(tiles), values.reshape(tiles), w_out,
    )
    return place_result(result)


def solution(mesh):
    placed = (
        P("frames", "heads"),
        P("frames", "heads"),
        P("frames", "heads"),
        P(),
        P("frames"),
        P("heads", None),
    )
    columns = mesh.shape["frames"] == PAIR * LINE and mesh.shape["heads"] % 2 == 0
    return jax.shard_map(
        column_shards if columns else shards, mesh=mesh, in_specs=placed, out_specs=P("frames", "heads"), check_vma=False
    )
```

```python
import functools
import math

import jax
import jax.numpy as jnp
from jax import lax
from jax.experimental import pallas as pl
from jax.experimental.pallas import tpu as pltpu
from jax.sharding import PartitionSpec as P

DH = 128
TILE = 128
MESH = pl.DeviceIdType.MESH
F32 = jnp.float32
PAIR = 2
LINE = 4
PARTS = 2
LAST_PARTS = 4
COPY_TILES = 8
UNROLL = 2
EARLY = 3
LOG2E = math.log2(math.e)
LOWEST = -1e38
VMEM_BYTES = 67043328
NT_DIMS = (((1,), (1,)), ((), ()))


def head_columns(h):
    return slice(h * DH, (h + 1) * DH)


class direct_exchange:
    def __init__(self, dims, pick_ref, k_ref, v_ref, recv, send, kv_send, kv_recv):
        self.frames, _, _, _, self.capacity, self.heads, self.slots = dims
        self.pick_ref, self.k_ref, self.v_ref, self.recv = pick_ref, k_ref, v_ref, recv
        self.send, self.kv_send, self.kv_recv = send, kv_send, kv_recv
        self.me_f, self.me_p = lax.axis_index("frames"), lax.axis_index("heads")

    def copy(self, h, target, origin):
        return pltpu.make_async_remote_copy(
            src_ref=self.send.at[h % self.slots, target],
            dst_ref=self.recv[h].at[pl.ds(origin * self.capacity, self.capacity)],
            send_sem=self.kv_send.at[h, target],
            recv_sem=self.kv_recv.at[h, origin],
            device_id=(target, self.me_p),
            device_id_type=MESH,
        )

    def others(self, action):
        @pl.loop(1, self.frames)
        def _(step):
            action(lax.rem(self.me_f + step, self.frames))

    def pick(self, target, c):
        return self.pick_ref[(target * self.frames + self.me_f) * self.capacity + c]

    def build(self, h):
        if h >= self.slots:
            self.others(lambda target: self.copy(h - self.slots, target, self.me_f).wait_send())

        def fill(target):
            for c in range(self.capacity):
                index = self.pick(target, c)
                self.send[h % self.slots, target, c, 0] = self.k_ref[index, :, head_columns(h)]
                self.send[h % self.slots, target, c, 1] = self.v_ref[index, :, head_columns(h)]

        self.others(fill)
        for c in range(self.capacity):
            index = self.pick(self.me_f, c)
            self.recv[h][self.me_f * self.capacity + c, 0] = self.k_ref[index, :, head_columns(h)]
            self.recv[h][self.me_f * self.capacity + c, 1] = self.v_ref[index, :, head_columns(h)]

    def start(self, h):
        self.others(lambda target: self.copy(h, target, self.me_f).start())

    def prepare(self):
        self.build(0)

    def begin(self):
        self.start(0)

    def follow(self):
        if self.heads > 1:
            self.build(1)
            self.start(1)

    def receive(self, h, midway):
        if h + 2 < self.heads:
            self.build(h + 2)
        midway()
        self.others(lambda origin: self.copy(h, origin, origin).wait_recv())
        if h + 2 < self.heads:
            self.start(h + 2)

    def drain(self):
        for h in range(max(0, self.heads - self.slots), self.heads):
            self.others(lambda target: self.copy(h, target, self.me_f).wait_send())


def layer_kernel(
    dims, pick_ref, slot_ref, count_ref, q_ref, k_ref, v_ref, w_ref, out_ref,
    rows, attn, acc, w_send, w_recv, a_send, a_recv, own_sem, *kv_refs,
):
    frames, peers, blocks, select, capacity, heads, slots = dims
    recv, kv_refs = kv_refs[:heads], kv_refs[heads:]
    me_f, me_p = lax.axis_index("frames"), lax.axis_index("heads")
    depth = heads * DH
    features = rows.shape[2]

    barrier = pltpu.get_barrier_semaphore()

    @pl.loop(1, frames)
    def _(step):
        pl.semaphore_signal(
            barrier, inc=1, device_id=(lax.rem(me_f + step, frames), me_p), device_id_type=MESH
        )

    @pl.loop(1, peers)
    def _(step):
        pl.semaphore_signal(
            barrier, inc=1, device_id=(me_f, lax.rem(me_p + step, peers)), device_id_type=MESH
        )

    def columns_of(peer):
        return pl.ds(pl.multiple_of(peer * features, features), features)

    own_rows = pltpu.make_async_copy(w_ref.at[:, columns_of(me_p)], rows.at[me_p], own_sem)
    own_rows.start()

    exchange = direct_exchange(dims, pick_ref, k_ref, v_ref, recv, *kv_refs)

    def w_copy(target, origin):
        return pltpu.make_async_remote_copy(
            src_ref=w_ref.at[:, columns_of(target)],
            dst_ref=rows.at[origin],
            send_sem=w_send.at[target],
            recv_sem=w_recv.at[origin],
            device_id=(me_f, target),
            device_id_type=MESH,
        )

    part_blocks = blocks // PARTS
    part_rows = part_blocks * TILE

    def a_copy(h, part, target, origin):
        held = attn.at[h, origin, pl.ds(part * part_rows, part_rows)]
        return pltpu.make_async_remote_copy(
            src_ref=held,
            dst_ref=held,
            send_sem=a_send.at[h, part, target, origin],
            recv_sem=a_recv.at[h, part, origin],
            device_id=(me_f, target),
            device_id_type=MESH,
        )

    twin = me_p + 1 - 2 * lax.rem(me_p, 2)

    def over_alike(action):
        @pl.loop(1, peers // 2)
        def _(step):
            action(lax.rem(me_p + 2 * step, peers))

    def over_twins(action):
        @pl.loop(0, peers // 2)
        def _(step):
            action(lax.rem(twin + 2 * step, peers))

    def share(h, part):
        over_alike(lambda target: a_copy(h, part, target, me_p).start())
        a_copy(h, part, twin, me_p).start()

    def finish(h):
        if h == 0:
            own_rows.wait()
            over_peers(lambda origin: w_copy(origin, origin).wait_recv())
        for part in range(PARTS):

            def relay(origin):
                a_copy(h, part, origin, origin).wait_recv()
                a_copy(h, part, twin, origin).start()

            over_alike(relay)
        for part in range(PARTS):
            over_twins(lambda origin: a_copy(h, part, origin, origin).wait_recv())
            project(h, part)

    def drain_attn(h, part):
        over_alike(lambda target: a_copy(h, part, target, me_p).wait_send())
        a_copy(h, part, twin, me_p).wait_send()
        over_alike(lambda origin: a_copy(h, part, twin, origin).wait_send())

    def over_peers(action):
        @pl.loop(1, peers)
        def _(step):
            action(lax.rem(me_p + step, peers))

    def attend(h, part):
        @pl.loop(part * part_blocks, (part + 1) * part_blocks, unroll=UNROLL)
        def _(b):
            q = q_ref[b, :, head_columns(h)]
            picks = [slot_ref[b * select + s] for s in range(select)]
            keyset = jnp.concatenate(
                [k_ref[b, :, head_columns(h)]] + [recv[h][i, 0] for i in picks], axis=0
            )
            valueset = jnp.concatenate(
                [v_ref[b, :, head_columns(h)]] + [recv[h][i, 1] for i in picks], axis=0
            )
            scores = lax.dot_general(q, keyset, NT_DIMS, preferred_element_type=F32)
            scores = scores * (1.0 / DH**0.5)
            position = lax.broadcasted_iota(jnp.int32, scores.shape, 1)
            scores = jnp.where(position < (count_ref[b] + 1) * TILE, scores, -jnp.inf)
            top = jnp.max(scores, axis=1, keepdims=True)
            probs = jnp.exp(scores - top)
            denom = jnp.sum(probs, axis=1, keepdims=True)
            mixed = jnp.dot(probs.astype(jnp.bfloat16), valueset, preferred_element_type=F32)
            attn[h, me_p, pl.ds(pl.multiple_of(b * TILE, TILE), TILE), :] = (mixed / denom).astype(
                jnp.bfloat16
            )

    row_tile = 2 * TILE

    def project(h, part):
        @pl.loop(part * part_rows // row_tile, (part + 1) * part_rows // row_tile)
        def _(r):
            span = pl.ds(pl.multiple_of(r * row_tile, row_tile), row_tile)
            left = jnp.concatenate([attn[h, p, span, :] for p in range(peers)], axis=1)
            right = jnp.concatenate([rows[p, head_columns(h), :] for p in range(peers)], axis=0)
            term = jnp.dot(left, right, preferred_element_type=F32)
            if h > 0:
                term = term + acc[span, :]
            if h == heads - 1:
                out_ref[span, :] = term.astype(out_ref.dtype)
            else:
                acc[span, :] = term

    exchange.prepare()
    pl.semaphore_wait(barrier, frames + peers - 2)
    exchange.begin()
    over_peers(lambda target: w_copy(target, me_p).start())
    exchange.follow()
    for h in range(heads):
        exchange.receive(h, (lambda: finish(h - 1)) if h > 0 else (lambda: None))
        for part in range(PARTS):
            attend(h, part)
            share(h, part)
    finish(heads - 1)
    exchange.drain()
    over_peers(lambda target: w_copy(target, me_p).wait_send())
    for h in range(heads):
        for part in range(PARTS):
            drain_attn(h, part)


def shards(queries, keys, values, block_ids, counts, w_out):
    frames = lax.axis_size("frames")
    peers = lax.axis_size("heads")
    here = lax.axis_index("frames")
    tokens, width = queries.shape
    blocks = tokens // TILE
    select = block_ids.shape[1]
    heads = width // DH
    requests = blocks * select
    capacity = max(2, (requests + frames - 1) // frames)
    features = w_out.shape[1] // peers
    slots = min(3, heads)

    ids = block_ids.reshape(frames, requests)
    owner = ids // blocks
    order = jnp.arange(requests, dtype=jnp.int32)
    same = (owner[:, :, None] == owner[:, None, :]) & (order[:, None] < order[None, :])
    slot = owner * capacity + jnp.sum(same.astype(jnp.int32), axis=1)
    hit = slot[:, None, :] == jnp.arange(frames * capacity, dtype=jnp.int32)[:, None]
    pick = jnp.sum(jnp.where(hit, (ids % blocks)[:, None, :], 0), axis=2).reshape(-1)
    my_slot = lax.dynamic_slice_in_dim(slot, here, 1, 0).reshape(requests)

    smem = pl.BlockSpec(memory_space=pltpu.SMEM)
    vmem = pl.BlockSpec(memory_space=pltpu.VMEM)
    tiles = (blocks, TILE, width)
    dma = pltpu.SemaphoreType.DMA
    bf16 = jnp.bfloat16
    common = [
        pltpu.VMEM((peers, width, features), bf16),
        pltpu.VMEM((heads, peers, tokens, DH), bf16),
        pltpu.VMEM((tokens, features), F32),
    ]
    common_sems = [
        dma((peers,)), dma((peers,)), dma((heads, PARTS, peers, peers)),
        dma((heads, PARTS, peers)), dma,
    ]
    recv = [pltpu.VMEM((frames * capacity, 2, TILE, DH), bf16)] * heads
    extra = [
        pltpu.VMEM((slots, frames, capacity, 2, TILE, DH), bf16),
        dma((heads, frames)),
        dma((heads, frames)),
    ]
    dims = (frames, peers, blocks, select, capacity, heads, slots)
    return pl.pallas_call(
        functools.partial(layer_kernel, dims),
        out_shape=jax.ShapeDtypeStruct((tokens, features), bf16),
        in_specs=[smem, smem, smem, vmem, vmem, vmem, pl.BlockSpec(memory_space=pl.ANY)],
        out_specs=vmem,
        scratch_shapes=common + common_sems + recv + extra,
        compiler_params=pltpu.CompilerParams(
            collective_id=0, has_side_effects=True, vmem_limit_bytes=VMEM_BYTES
        ),
    )(
        pick, my_slot, counts, queries.reshape(tiles), keys.reshape(tiles), values.reshape(tiles),
        w_out,
    )


def column_kernel(
    dims, ids_ref, own_count_ref, q_hbm, k_hbm, v_hbm, w_ref, out_ref,
    q_ref, k_ref, v_ref, rows, attn, acc, qall, count, osend, orecv, ssend, srecv, oself, sself, weights, finished, place, usable,
    w_send, w_recv, a_send, a_recv, own_sem, load_sem, turn_sem, out_sem,
    kv_send, kv_recv, q_send, q_recv, c_send, c_recv, o_send, o_recv, s_send, s_recv, *kv,
):
    frames, peers, blocks, select, heads = dims
    keys, values = kv[:heads], kv[heads:]
    me_f, me_p = lax.axis_index("frames"), lax.axis_index("heads")
    line = frames // PAIR
    z, x = me_f // PAIR, me_f % PAIR
    half = z // (line // 2)
    mid, end = half + 1, (line - 1) * half
    across = line - 1 - mid
    is_mid = z == mid
    is_end = z == end
    other = 1 - x
    depth = heads * DH
    features = rows.shape[2]
    group_blocks = blocks // PARTS
    exponent = LOG2E / DH**0.5

    def at(zz, xx):
        return (zz * PAIR + xx, me_p)

    def parts_of(h):
        return LAST_PARTS if h == heads - 1 else PARTS

    def rows_in(h):
        return blocks // parts_of(h) * TILE

    def rows_span(h, part):
        return pl.ds(part * rows_in(h), rows_in(h))

    loads = [
        pltpu.make_async_copy(source, held, load_sem.at[i])
        for i, (source, held) in enumerate(((k_hbm, k_ref), (v_hbm, v_ref), (q_hbm, q_ref)))
    ]
    for load in loads:
        load.start()
    barrier = pltpu.get_barrier_semaphore()

    def greet(device):
        pl.semaphore_signal(barrier, inc=1, device_id=device, device_id_type=MESH)

    @pl.loop(1, peers)
    def _(step):
        greet((me_f, lax.rem(me_p + step, peers)))

    greet(at(z, other))
    greet(at(mid + end - z, x))
    greet(at(mid + end - z, other))

    @pl.when(is_mid)
    def _():
        greet(at(across, x))

    def columns_of(peer):
        return pl.ds(pl.multiple_of(peer * features, features), features)

    own_rows = pltpu.make_async_copy(w_ref.at[:, columns_of(me_p)], rows.at[me_p], own_sem)
    own_rows.start()

    @pl.loop(0, blocks)
    def _(b):
        count[0, pl.ds(b, 1), :] = jnp.full((1, TILE), own_count_ref[b], jnp.int32)

    def send(source, target, send_sem, recv_sem, device):
        return pltpu.make_async_remote_copy(
            src_ref=source, dst_ref=target, send_sem=send_sem, recv_sem=recv_sem,
            device_id=device, device_id_type=MESH,
        )

    def kv_copy(h, flow, which):
        held = (keys, values)[which][h]
        source = (k_ref, v_ref)[which].at[:, :, head_columns(h)]
        if flow == 2:
            source = held.at[pl.ds(blocks, blocks)]
        return send(
            source, held.at[pl.ds((flow + 1) * blocks, blocks)],
            kv_send.at[flow, which, int(h > 0)], kv_recv.at[flow, h, which],
            at(mid, x) if flow == 0 else at(across, x),
        )

    def q_copy(h, flow):
        source = q_ref.at[:, :, head_columns(h)] if flow < 2 else qall.at[h, 1]
        return send(
            source, qall.at[h, flow], q_send.at[flow], q_recv.at[flow, h],
            at(mid, x) if flow == 1 else at(z, other),
        )

    def c_copy(flow):
        device = (at(z, other), at(mid, x), at(mid, other))[flow]
        return send(
            count.at[0], count.at[flow + 1], c_send.at[flow], c_recv.at[flow], device
        )

    def partial_device(slot):
        to_z = z + (end - z) * ((slot + 1) // 2)
        to_x = x + (other - x) * ((slot + 1) % 2)
        return at(to_z, to_x)

    def o_copy(h, part, slot):
        span = rows_span(h, part)
        return send(
            osend.at[h, slot, span], orecv.at[h, slot, span],
            o_send.at[slot], o_recv.at[h * PARTS + part, slot], partial_device(slot),
        )

    def s_copy(h, slot):
        return send(
            ssend.at[h, slot], srecv.at[h, slot], s_send.at[slot], s_recv.at[h, slot],
            partial_device(slot),
        )

    def w_copy(h, target, origin):
        span = pl.ds(h * DH, DH)
        return send(
            w_ref.at[span, columns_of(target)], rows.at[origin, span],
            w_send.at[target], w_recv.at[h, origin], (me_f, target),
        )

    def a_copy(h, part, target, origin):
        held = attn.at[h, origin, rows_span(h, part)]
        to_twin = lax.rem(target + me_p, 2)
        lane_of = target + to_twin * (origin - me_p)
        return send(
            held, held, a_send.at[lane_of], a_recv.at[h * PARTS + part, origin],
            (me_f, target),
        )

    twin = me_p + 1 - 2 * lax.rem(me_p, 2)

    def over_peers(action):
        @pl.loop(1, peers)
        def _(step):
            action(lax.rem(me_p + step, peers))

    def over_alike(action):
        @pl.loop(1, peers // 2)
        def _(step):
            action(lax.rem(me_p + 2 * step, peers))

    def over_twins(action):
        @pl.loop(0, peers // 2)
        def _(step):
            action(lax.rem(twin + 2 * step, peers))

    def direct(h, part):
        return h == heads - 1 and part >= parts_of(h) // 2

    def share(h, part):
        over_alike(lambda target: a_copy(h, part, target, me_p).start())
        if direct(h, part):
            over_twins(lambda target: a_copy(h, part, target, me_p).start())
        else:
            a_copy(h, part, twin, me_p).start()

    def pass_on(h, part):
        def relay(origin):
            a_copy(h, part, origin, origin).wait_recv()
            a_copy(h, part, twin, origin).start()

        over_alike(relay)

    def finish(h, part):
        if part == 0:
            if h == 0:
                own_rows.wait()
            over_peers(lambda origin: w_copy(h, origin, origin).wait_recv())
        if direct(h, part):
            over_alike(lambda origin: a_copy(h, part, origin, origin).wait_recv())
        over_twins(lambda origin: a_copy(h, part, origin, origin).wait_recv())
        project(h, part)

    row_tile = 2 * TILE

    def out_copy(r):
        span = pl.ds(pl.multiple_of(r * row_tile, row_tile), row_tile)
        return pltpu.make_async_copy(finished.at[span], out_ref.at[span], out_sem.at[r])

    def project(h, part):
        tiles = rows_in(h) // row_tile

        @pl.loop(part * tiles, (part + 1) * tiles)
        def _(r):
            span = pl.ds(pl.multiple_of(r * row_tile, row_tile), row_tile)
            left = jnp.concatenate([attn[h, p, span, :] for p in range(peers)], axis=1)
            right = jnp.concatenate([rows[p, head_columns(h), :] for p in range(peers)], axis=0)
            term = jnp.dot(left, right, preferred_element_type=F32)
            if h > 0:
                term = term + acc[span, :]
            if h == heads - 1:
                finished[span, :] = term.astype(out_ref.dtype)
                out_copy(r).start()
            else:
                acc[span, :] = term

    def fill_tables():
        for role in range(4):
            role_z = z if role < 2 else end
            role_x = x if role % 2 == 0 else other

            @pl.loop(0, blocks)
            def _(b):
                for s in range(select):
                    chosen = ids_ref[s, (role_z * PAIR + role_x) * blocks + b]
                    owner = lax.div(chosen, blocks)
                    owner_z, owner_x = lax.div(owner, PAIR), lax.rem(owner, PAIR)
                    here = owner_z == z
                    near = owner_z == end
                    source = jnp.where(
                        here, 0, jnp.where(near, 1, jnp.where(owner_z == across, 2, 3))
                    )
                    ours = here | is_mid
                    if role > 1:
                        ours = ours & jnp.logical_not(near)
                    ours = ours & (owner_x == x)
                    entry = (role * blocks + b) * select + s
                    index = source * blocks + lax.rem(chosen, blocks)
                    place[entry] = jnp.where(ours, index, 0)
                    usable[entry] = jnp.where(ours, 1, 0)

    def own_block(h):
        @pl.loop(0, blocks)
        def _(b):
            keys[h][b] = k_ref[b, :, head_columns(h)]
            values[h][b] = v_ref[b, :, head_columns(h)]

    lane = lax.broadcasted_iota(jnp.int32, (TILE, TILE), 1)

    def weigh(h, role, b, query, first_keys):
        entries = [(role * blocks + b) * select + s for s in range(select)]
        keyset = jnp.concatenate(first_keys + [keys[h][place[e]] for e in entries], axis=0)
        scores = lax.dot_general(query, keyset, NT_DIMS, preferred_element_type=F32)
        used = count[role, pl.ds(b, 1), :]
        lead = len(first_keys)
        pieces = [scores[:, i * TILE : (i + 1) * TILE] for i in range(lead + select)]
        for s in range(select):
            keep = jnp.broadcast_to(used * usable[entries[s]], (TILE, TILE)) > s
            pieces[lead + s] = jnp.where(keep, pieces[lead + s], -jnp.inf)
        top = jnp.max(functools.reduce(jnp.maximum, pieces), axis=1, keepdims=True)
        top = jnp.maximum(top, LOWEST)
        probs = [jnp.exp2((piece - top) * exponent) for piece in pieces]
        denom = jnp.sum(functools.reduce(jnp.add, probs), axis=1, keepdims=True)
        for i, piece in enumerate(probs):
            weights[role, b, :, i * TILE : (i + 1) * TILE] = piece.astype(jnp.bfloat16)
        return top * exponent, denom

    def mix(h, role, b, first_values):
        entries = [(role * blocks + b) * select + s for s in range(select)]
        valueset = jnp.concatenate(first_values + [values[h][place[e]] for e in entries], axis=0)
        held = weights[role, b, :, : (len(first_values) + select) * TILE]
        return jnp.dot(held, valueset, preferred_element_type=F32)

    def rows_of(levels):
        tile = jnp.zeros((TILE, TILE), F32)
        for j, (top, denom) in enumerate(levels):
            tile = jnp.where(lane == j, top, tile)
            tile = jnp.where(lane == group_blocks + j, denom, tile)
        return tile.T[: 2 * group_blocks]

    away = is_mid.astype(jnp.int32)

    def over_others(parts, action):
        first = 2 * parts

        @pl.loop(first * (1 - away), first + parts)
        def _(step):
            late = step // first
            role = late + (1 - late) * (3 - step % 2)
            part = late * (step - first) + (1 - late) * (step // 2)
            action(step, role, part)

    def weigh_others(h):
        def action(step, role, part):
            levels = []
            for j in range(group_blocks):
                b = part * group_blocks + j
                levels.append(weigh(h, role, b, qall[h, role - 1, b], []))
            ssend[h, role - 1, part] = rows_of(levels)

            @pl.when(part == PARTS - 1)
            def _():
                s_copy(h, role - 1).start()

        over_others(PARTS, action)

    def mix_others(h):
        part_blocks = blocks // parts_of(h)

        def action(step, role, part):
            for j in range(part_blocks):
                b = part * part_blocks + j
                span = pl.ds(pl.multiple_of(b * TILE, TILE), TILE)
                osend[h, role - 1, span, :] = mix(h, role, b, []).astype(jnp.bfloat16)
            o_copy(h, part, role - 1).start()

        over_others(parts_of(h), action)

    def weigh_own(h):
        @pl.loop(0, PARTS)
        def _(part):
            levels = []
            for j in range(group_blocks):
                b = part * group_blocks + j
                query = q_ref[b, :, head_columns(h)]
                levels.append(weigh(h, 0, b, query, [k_ref[b, :, head_columns(h)]]))
            sself[part] = rows_of(levels)

    def mix_own(h):
        @pl.loop(0, PARTS)
        def _(part):
            for j in range(group_blocks):
                b = part * group_blocks + j
                span = pl.ds(pl.multiple_of(b * TILE, TILE), TILE)
                oself[span, :] = mix(h, 0, b, [v_ref[b, :, head_columns(h)]])

    def merge(h, part, slots):
        part_blocks = blocks // parts_of(h)
        group, first = divmod(part * part_blocks, group_blocks)
        levels = [sself[group]] + [srecv[h, slot, group] for slot in range(slots)]
        tops = [level[:group_blocks] for level in levels]
        denoms = [level[group_blocks:] for level in levels]
        top = functools.reduce(jnp.maximum, tops)
        shares = [jnp.exp2(one - top) for one in tops]
        total = functools.reduce(jnp.add, [share * d for share, d in zip(shares, denoms)])
        spare = TILE - group_blocks * len(shares)
        tall = jnp.concatenate(
            [share / total for share in shares] + [jnp.zeros((spare, TILE), F32)], axis=0
        ).T
        for j in range(part_blocks):
            span = pl.ds((part * part_blocks + j) * TILE, TILE)
            column = first + j
            value = oself[span, :] * tall[:, column : column + 1]
            for slot in range(slots):
                column = group_blocks * (slot + 1) + first + j
                value = value + orecv[h, slot, span, :].astype(F32) * tall[:, column : column + 1]
            attn[h, me_p, span, :] = value.astype(jnp.bfloat16)

    def combine(h, part):
        o_copy(h, part, 0).wait_recv()

        @pl.when(is_mid)
        def _():
            merge(h, part, 1)

        @pl.when(is_end)
        def _():
            for slot in (1, 2):
                o_copy(h, part, slot).wait_recv()
            merge(h, part, 3)

    def relay_on(h):
        last = h == heads - 1
        for which in range(2):
            kv_copy(h, 0, which).wait_recv()
            kv_copy(h, 2, which).start()
            if last and h > 0 and which == 0:
                kv_copy(h, 1, 1).start()
        if not last:
            kv_copy(h + 1, 1, 0).start()
            if h + 1 < heads - 1:
                kv_copy(h + 1, 1, 1).start()
        q_copy(h, 1).wait_recv()
        q_copy(h, 2).start()

    def send_early(h):
        @pl.when(is_end)
        def _():
            for which in range(2):
                kv_copy(h, 0, which).start()
            q_copy(h, 1).start()

    def open_column():
        @pl.when(is_mid)
        def _():
            for which in range(2):
                kv_copy(0, 1, which).start()

        for h in range(early):
            send_early(h)

    early = min(EARLY, heads)
    leads = lax.rem(me_p, 2) == 1

    def send_rows(h):
        over_peers(lambda target: w_copy(h, target, me_p).start())

    pl.semaphore_wait(barrier, peers + 2 + away)
    for load in loads:
        load.wait()

    c_copy(0).start()

    @pl.when(is_end)
    def _():
        c_copy(1).start()
        c_copy(2).start()

    @pl.when(leads)
    def _():
        open_column()

    for h in range(early):
        q_copy(h, 0).start()
        send_rows(h)
    fill_tables()
    own_block(0)

    def first_sent(flow):
        for which in range(2):
            kv_copy(0, flow, which).wait_send()

    @pl.when(leads & is_end)
    def _():
        first_sent(0)

    @pl.when(leads & is_mid)
    def _():
        first_sent(1)

    @pl.when(leads)
    def _():
        pl.semaphore_signal(turn_sem, inc=1, device_id=(me_f, twin), device_id_type=MESH)

    @pl.when(jnp.logical_not(leads))
    def _():
        pl.semaphore_wait(turn_sem, 1)
        open_column()

    c_copy(0).wait_recv()

    @pl.when(is_mid)
    def _():
        relay_on(0)
        c_copy(1).wait_recv()
        c_copy(2).wait_recv()

    def all_sent(source, semaphore):
        pltpu.make_async_remote_copy(
            src_ref=source, dst_ref=source, send_sem=semaphore, recv_sem=semaphore,
            device_id=(me_f, twin), device_id_type=MESH,
        ).wait_send()

    def drain_early():
        rest = pl.ds(DH, depth - DH)

        def kv_sent(flow):
            for which in range(2):
                if heads > 1:
                    all_sent(k_ref.at[:, :, rest], kv_send.at[flow, which, 1])

                @pl.when(jnp.logical_not(leads) | (flow == 2))
                def _():
                    all_sent(k_ref.at[:, :, pl.ds(0, DH)], kv_send.at[flow, which, 0])

        c_copy(0).wait_send()
        all_sent(q_ref, q_send.at[0])
        over_peers(lambda target: all_sent(w_ref.at[:, columns_of(target)], w_send.at[target]))

        @pl.when(is_end)
        def _():
            c_copy(1).wait_send()
            c_copy(2).wait_send()
            all_sent(q_ref, q_send.at[1])
            kv_sent(0)

        @pl.when(is_mid)
        def _():
            all_sent(q_ref, q_send.at[2])
            kv_sent(1)
            kv_sent(2)

    def drain_late():
        @pl.loop(0, 1 + 2 * away)
        def _(slot):
            all_sent(ssend.at[:, slot], s_send.at[slot])
            all_sent(osend.at[:, slot], o_send.at[slot])

        over_alike(lambda target: all_sent(attn.at[:, me_p], a_send.at[target]))
        over_twins(lambda origin: all_sent(attn.at[:, me_p], a_send.at[origin]))

    def settle(h):
        if h >= 0:
            for part in range(parts_of(h)):
                finish(h, part)

    for h in range(heads):
        if h + EARLY < heads:
            q_copy(h + EARLY, 0).start()
            send_early(h + EARLY)
        if h > 0:
            own_block(h)
        last = h == heads - 1

        def catch_up():
            settle(h - 2)
            if h > 0:
                for part in range(parts_of(h - 1)):
                    pass_on(h - 1, part)

        if 0 < h < heads - 1:

            @pl.when(is_mid)
            def _():
                relay_on(h + 1)

        if last:

            @pl.when(jnp.logical_not(leads))
            def _():
                settle(h - 2)

        q_copy(h, 0).wait_recv()

        def arrived(which):
            kv_copy(h, 1, which).wait_recv()
            kv_copy(h, 2, which).wait_recv()

        @pl.when(is_mid)
        def _():
            q_copy(h, 2).wait_recv()
            arrived(0)

        weigh_others(h)
        weigh_own(h)
        if last and h > 0:
            for part in range(parts_of(h - 1)):
                pass_on(h - 1, part)

        @pl.when(is_mid)
        def _():
            arrived(1)

        mix_others(h)
        mix_own(h)
        if not last:
            if h == 0:

                @pl.when(is_mid)
                def _():
                    relay_on(h + 1)

            catch_up()
        elif h > 0:

            @pl.when(jnp.logical_not(leads) & is_end)
            def _():
                settle(h - 1)

        s_copy(h, 0).wait_recv()

        @pl.when(is_end)
        def _():
            for slot in (1, 2):
                s_copy(h, slot).wait_recv()

        for part in range(parts_of(h)):
            combine(h, part)
            share(h, part)
        if last and h > 0:

            @pl.when(jnp.logical_not(leads) & is_mid)
            def _():
                settle(h - 1)

        if h + EARLY < heads:
            send_rows(h + EARLY)
    @pl.when(leads)
    def _():
        settle(heads - 3)
        settle(heads - 2)

    drain_early()
    for part in range(parts_of(heads - 1)):
        if not direct(heads - 1, part):
            pass_on(heads - 1, part)
    for part in range(parts_of(heads - 1)):
        finish(heads - 1, part)
    drain_late()
    for r in range(blocks * TILE // row_tile):
        out_copy(r).wait()


def place_result(result):
    tokens, features = result.shape
    rows = tokens // COPY_TILES

    def kernel(source, target, held, read_sem, write_sem):
        spans = [pl.ds(i * rows, rows) for i in range(COPY_TILES)]
        reads = [
            pltpu.make_async_copy(source.at[span], held.at[span], read_sem.at[i])
            for i, span in enumerate(spans)
        ]
        writes = [
            pltpu.make_async_copy(held.at[span], target.at[span], write_sem.at[i])
            for i, span in enumerate(spans)
        ]
        for read in reads:
            read.start()
        for read, write in zip(reads, writes):
            read.wait()
            write.start()
        for write in writes:
            write.wait()

    hbm = pl.BlockSpec(memory_space=pltpu.HBM)
    return pl.pallas_call(
        kernel,
        out_shape=jax.ShapeDtypeStruct(result.shape, result.dtype),
        in_specs=[hbm],
        out_specs=hbm,
        scratch_shapes=[
            pltpu.VMEM(result.shape, result.dtype),
            pltpu.SemaphoreType.DMA((COPY_TILES,)),
            pltpu.SemaphoreType.DMA((COPY_TILES,)),
        ],
    )(result)


def column_shards(queries, keys, values, block_ids, counts, w_out):
    frames = lax.axis_size("frames")
    peers = lax.axis_size("heads")
    tokens, width = queries.shape
    blocks = tokens // TILE
    select = block_ids.shape[1]
    heads = width // DH
    features = w_out.shape[1] // peers
    smem = pl.BlockSpec(memory_space=pltpu.SMEM)
    tiles = (blocks, TILE, width)
    dma = pltpu.SemaphoreType.DMA
    bf16 = jnp.bfloat16
    pieces = (heads - 1) * PARTS + LAST_PARTS
    level_rows = (PARTS, 2 * blocks // PARTS, TILE)
    scratch = [pltpu.VMEM(tiles, bf16)] * 3 + [
        pltpu.VMEM((peers, width, features), bf16),
        pltpu.VMEM((heads, peers, tokens, DH), bf16),
        pltpu.VMEM((tokens, features), F32),
        pltpu.VMEM((heads, 3, blocks, TILE, DH), bf16),
        pltpu.VMEM((4, blocks, TILE), jnp.int32),
        pltpu.VMEM((heads, 3, tokens, DH), bf16),
        pltpu.VMEM((heads, 3, tokens, DH), bf16),
        pltpu.VMEM((heads, 3) + level_rows, F32),
        pltpu.VMEM((heads, 3) + level_rows, F32),
        pltpu.VMEM((tokens, DH), F32),
        pltpu.VMEM(level_rows, F32),
        pltpu.VMEM((4, blocks, TILE, (select + 1) * TILE), bf16),
        pltpu.VMEM((tokens, features), bf16),
        pltpu.SMEM((4 * blocks * select,), jnp.int32),
        pltpu.SMEM((4 * blocks * select,), jnp.int32),
        dma((peers,)), dma((heads, peers)), dma((peers,)),
        dma((pieces, peers)), dma, dma((3,)), pltpu.SemaphoreType.REGULAR,
        dma((tokens // (2 * TILE),)),
        dma((3, 2, 2)), dma((3, heads, 2)), dma((3,)), dma((3, heads)),
        dma((3,)), dma((3,)),
        dma((3,)), dma((pieces, 3)), dma((3,)), dma((heads, 3)),
    ] + [pltpu.VMEM((4 * blocks, TILE, DH), bf16)] * (2 * heads)
    dims = (frames, peers, blocks, select, heads)
    hbm = pl.BlockSpec(memory_space=pltpu.HBM)
    result = pl.pallas_call(
        functools.partial(column_kernel, dims),
        out_shape=jax.ShapeDtypeStruct((tokens, features), bf16),
        in_specs=[smem, smem, hbm, hbm, hbm, hbm],
        out_specs=hbm,
        scratch_shapes=scratch,
        compiler_params=pltpu.CompilerParams(
            collective_id=0, has_side_effects=True, vmem_limit_bytes=VMEM_BYTES
        ),
    )(
        block_ids.T, counts,
        queries.reshape(tiles), keys.reshape(tiles), values.reshape(tiles), w_out,
    )
    return place_result(result)


def solution(mesh):
    placed = (
        P("frames", "heads"),
        P("frames", "heads"),
        P("frames", "heads"),
        P(),
        P("frames"),
        P("heads", None),
    )
    columns = mesh.shape["frames"] == PAIR * LINE and mesh.shape["heads"] % 2 == 0
    return jax.shard_map(
        column_shards if columns else shards, mesh=mesh, in_specs=placed, out_specs=P("frames", "heads"), check_vma=False
    )
```
